8 devices in a mesh: dp: 1 (over z), hp: 2 (over y), cp: 4 (over x, core).
Axes of the slice: x: 2, y: 2, z: 1, core: 2. Of those that a mesh axis runs over, the one named last changes fastest.
Arguments:
- latent: bfloat16 [48, 2, 128, 512], P(('dp', 'cp'), 'hp')
- conv_w: bfloat16 [4, 3, 3, 3, 512, 512], replicated
- conv_b: float32 [4, 512], replicated
- gn_gamma: float32 [4, 512], replicated
- gn_beta: float32 [4, 512], replicated
Outputs:
- output: bfloat16 [48, 2, 128, 512], P(('dp', 'cp'), 'hp')
All inputs are finite; a program needn't handle non-finite values.
Results may differ from the reference program's by a relative error of at most 0.00887298.
Values are sent between devices in bfloat16 or wider.
A program may use at most 1 GiB of HBM per device.

```python
import jax
import jax.numpy as jnp
from jax import lax

FRAMES = 48
HEIGHT = 2
LAT_WIDTH = 128
CHANNELS = 512
GROUPS = 32
EPS = 1e-6


def setup_inputs(seed: int = 0, part: int = 0) -> dict:
    root_key = jax.random.key(seed)
    part_key = jax.random.fold_in(root_key, part)
    key_noise, key_fscale, key_fshift, key_rscale = jax.random.split(part_key, 4)
    key_kernel, key_bias, key_gamma, key_beta = jax.random.split(jax.random.key(seed + 1), 4)
    base_noise = jax.random.normal(key_noise, (FRAMES, HEIGHT, LAT_WIDTH, CHANNELS), jnp.float32)
    frame_scale = jnp.exp(0.5 * jax.random.normal(key_fscale, (FRAMES, 1, 1, 1), jnp.float32))
    frame_shift = 0.7 * jax.random.normal(key_fshift, (FRAMES, 1, 1, CHANNELS), jnp.float32)
    row_scale = jnp.exp(0.4 * jax.random.normal(key_rscale, (1, HEIGHT, 1, 1), jnp.float32))
    latent = ((base_noise + frame_shift) * frame_scale * row_scale).astype(jnp.bfloat16)
    fan_in = 27 * CHANNELS
    conv_w = (jax.random.normal(key_kernel, (4, 3, 3, 3, CHANNELS, CHANNELS), jnp.float32) * fan_in ** -0.5).astype(jnp.bfloat16)
    conv_b = 0.5 * jax.random.normal(key_bias, (4, CHANNELS), jnp.float32)
    gn_gamma = 1.0 + 0.3 * jax.random.normal(key_gamma, (4, CHANNELS), jnp.float32)
    gn_beta = 0.3 * jax.random.normal(key_beta, (4, CHANNELS), jnp.float32)
    return {"latent": latent, "conv_w": conv_w, "conv_b": conv_b, "gn_gamma": gn_gamma, "gn_beta": gn_beta}


def norm_silu(video, gamma, beta):
    per_group = CHANNELS // GROUPS
    grouped = video.reshape(FRAMES, HEIGHT, LAT_WIDTH, GROUPS, per_group).astype(jnp.float32)
    norm_count = FRAMES * HEIGHT * LAT_WIDTH * per_group
    mean_val = jnp.sum(grouped, axis=(0, 1, 2, 4)) / norm_count
    variance = jnp.sum(grouped * grouped, axis=(0, 1, 2, 4)) / norm_count - mean_val * mean_val
    inv_std = lax.rsqrt(variance + EPS)
    gamma_g = gamma.reshape(GROUPS, per_group)
    scale_c = (inv_std[:, None] * gamma_g).reshape(CHANNELS)
    shift_c = (beta.reshape(GROUPS, per_group) - (mean_val * inv_std)[:, None] * gamma_g).reshape(CHANNELS)
    return jax.nn.silu(video.astype(jnp.float32) * scale_c + shift_c).astype(jnp.bfloat16)


def causal_conv(video, kernel, bias_vec):
    padded = jnp.concatenate([video[:1], video[:1], video], axis=0)
    kernel_f = kernel.astype(jnp.float32)

    def one_frame(frame_idx):
        window = lax.dynamic_slice_in_dim(padded, frame_idx, 3, axis=0).astype(jnp.float32)
        conv_out = lax.conv_general_dilated(window[None], kernel_f, (1, 1, 1), ((0, 0), (1, 1), (1, 1)), dimension_numbers=("NDHWC", "DHWIO", "NDHWC"))
        return (conv_out[0, 0] + bias_vec).astype(jnp.bfloat16)

    return lax.map(one_frame, jnp.arange(FRAMES))


def reference(latent, conv_w, conv_b, gn_gamma, gn_beta):
    residual = latent
    for block_idx in range(2):
        hidden = residual
        for sub_idx in range(2):
            layer_idx = 2 * block_idx + sub_idx
            activated = norm_silu(hidden, gn_gamma[layer_idx], gn_beta[layer_idx])
            hidden = causal_conv(activated, conv_w[layer_idx], conv_b[layer_idx])
        residual = (residual.astype(jnp.float32) + hidden.astype(jnp.float32)).astype(jnp.bfloat16)
    return residual
```

```python
import functools

import jax
import jax.numpy as jnp
from jax import lax
from jax.experimental import pallas as pl
from jax.experimental.pallas import tpu as pltpu
from jax.sharding import PartitionSpec as P

GROUPS = 32
EPS = 1e-6
MESH = pl.DeviceIdType.MESH
F32 = jnp.float32
BF16 = jnp.bfloat16


def kernel(dims, lat, w_hbm, bias, gamma, beta, out, vid, act, acc, w_buf, x_in, halo, edge, ecol, s_acc, s_tot, s_send, s_recv,
           l_sem, w_sem, xs_sem, xr_sem, hs_sem, hr_sem, es_sem, er_sem, ei_sem, ss_sem, sr_sem, o_sem):
    n_cp, frames, half, chans, count = dims
    n_dev = 2 * n_cp
    n_pad = frames + 2
    h = lax.axis_index("hp")
    r = lax.axis_index("cp")
    other = 1 - h
    me = h * n_cp + r
    partner = {"hp": other, "cp": r}
    nxt = {"hp": h, "cp": lax.rem(r + 1, n_cp)}
    diag = {"hp": other, "cp": lax.rem(r + 1, n_cp)}
    not_last = r < n_cp - 1
    not_first = r > 0
    tail = pl.ds(frames - 2, 2)
    my_cols = pl.ds(pl.multiple_of(h * half, half), half)
    ot_cols = pl.ds(pl.multiple_of(other * half, half), half)

    def remote(src, dst, send, recv, dev):
        return pltpu.make_async_remote_copy(src_ref=src, dst_ref=dst, send_sem=send, recv_sem=recv, device_id=dev, device_id_type=MESH)

    def peer(step):
        t = lax.rem(me + step, n_dev)
        return {"hp": t // n_cp, "cp": lax.rem(t, n_cp)}

    load_x = pltpu.make_async_copy(lat, x_in, l_sem.at[0])
    load_own = pltpu.make_async_copy(lat.at[:, 0, my_cols, :], vid.at[0, h], l_sem.at[1])
    load_x.start()
    load_own.start()

    def w_copy(layer):
        slot = lax.rem(layer, 2)
        return pltpu.make_async_copy(w_hbm.at[layer], w_buf.at[slot], w_sem.at[slot])

    w_copy(0).start()
    w_copy(1).start()

    barrier = pltpu.get_barrier_semaphore()
    for step in range(1, n_dev):
        pl.semaphore_signal(barrier, inc=1, device_id=peer(step), device_id_type=MESH)
    pl.semaphore_wait(barrier, n_dev - 1)

    x_tail = remote(lat.at[tail, 0, ot_cols, :], vid.at[0, h, tail], xs_sem.at[0], xr_sem.at[0], partner)
    x_head = remote(lat.at[pl.ds(0, frames - 2), 0, ot_cols, :], vid.at[0, h, pl.ds(0, frames - 2)], xs_sem.at[1], xr_sem.at[1], partner)
    x_tail.start()
    x_head.start()
    x_halo = remote(lat.at[tail, 0, my_cols, :], halo.at[0, h], hs_sem.at[0], hr_sem.at[0, 0], nxt)

    @pl.when(not_last)
    def _():
        x_halo.start()

    s_acc[...] = jnp.zeros_like(s_acc)
    s_tot[...] = jnp.zeros_like(s_tot)
    load_x.wait()

    def fold(v):
        t = v[0:8]
        for k in range(1, v.shape[0] // 8):
            t = t + v[8 * k:8 * k + 8]
        return t

    def first_sums(f, carry):
        v = x_in[f, 0].astype(F32)
        s_acc[0] += fold(v)
        s_acc[1] += fold(v * v)
        lo, hi = v[half - 1:half], v[half:half + 1]
        ecol[h, f] = jnp.where(h == 0, lo, hi)
        edge[0, h, f + 2] = jnp.where(h == 0, hi, lo)
        return carry

    lax.fori_loop(0, frames, first_sums, 0)
    e_part = remote(ecol.at[h], edge.at[0, h, pl.ds(2, frames)], es_sem.at[0], ei_sem.at[0], partner)
    e_part.start()
    e_nxt = remote(edge.at[0, h, pl.ds(frames, 2)], edge.at[0, h, pl.ds(0, 2)], es_sem.at[1], ei_sem.at[1], nxt)
    e_diag = remote(ecol.at[h, tail], edge.at[0, h, pl.ds(0, 2)], es_sem.at[2], ei_sem.at[2], diag)

    @pl.when(not_last)
    def _():
        e_nxt.start()
        e_diag.start()

    def halo_send(slot, row, k):
        return remote(vid.at[slot, row, tail], halo.at[slot, row], hs_sem.at[k], hr_sem.at[slot, k], nxt)

    def edge_sends(slot):
        a = remote(ecol, edge.at[slot, :, pl.ds(2, frames)], es_sem.at[0], er_sem.at[slot, 0], partner)
        b = remote(ecol.at[:, tail], edge.at[slot, :, pl.ds(0, 2)], es_sem.at[1], er_sem.at[slot, 1], diag)
        return a, b

    def out_send():
        return remote(vid.at[0, other], out.at[:, 0, my_cols, :], o_sem.at[0], o_sem.at[1], partner)

    def out_local():
        return pltpu.make_async_copy(vid.at[0, h], out.at[:, 0, my_cols, :], o_sem.at[2])

    lane = lax.broadcasted_iota(jnp.int32, (8, chans), 1)
    rowid = lax.broadcasted_iota(jnp.int32, (half, chans), 0)
    n_group = chans // GROUPS

    def layer_body(layer, carry):
        slot = lax.rem(layer, 2)
        nslot = 1 - slot

        s_send[0:1] = jnp.sum(s_acc[0], axis=0, keepdims=True)
        s_send[1:2] = jnp.sum(s_acc[1], axis=0, keepdims=True)
        s_acc[...] = jnp.zeros_like(s_acc)
        sends = [remote(s_send, s_recv.at[slot, step], ss_sem.at[step], sr_sem.at[slot, step], peer(step)) for step in range(1, n_dev)]
        for c in sends:
            c.start()

        @pl.when(jnp.logical_and(layer >= 1, layer < 3))
        def _():
            w_copy(layer + 1).start()

        total = s_send[...]
        for c in sends:
            c.wait()
        for step in range(1, n_dev):
            total = total + s_recv[slot, step]
        s_tot[0:2] = total
        t = s_tot[...]
        shift_by = 1
        while shift_by < n_group:
            up = pltpu.roll(t, chans - shift_by, 1)
            down = pltpu.roll(t, shift_by, 1)
            t = t + jnp.where((lane & shift_by) == 0, up, down)
            shift_by *= 2
        t = t * (1.0 / count)
        mean = t[0:1]
        inv = lax.rsqrt(t[1:2] - mean * mean + EPS)
        scale = inv * gamma[layer]
        half_scale = 0.5 * scale
        half_shift = 0.5 * (beta[layer] - mean * scale)

        def silu(v):
            u = v * half_scale + half_shift
            return u + u * jnp.tanh(u)

        def norm_frame(v, e, row, f):
            y = silu(v.astype(F32))
            ye = silu(e)
            left = jnp.where(h == 0, 0.0, ye)
            right = jnp.where(h == 0, ye, 0.0)
            rows = pl.ds(pl.multiple_of(f * half, half), half)
            act[row, rows, 0:chans] = jnp.where(rowid == 0, left, pltpu.roll(y, 1, 0)).astype(BF16)
            act[row, rows, chans:2 * chans] = y.astype(BF16)
            act[row, rows, 2 * chans:3 * chans] = jnp.where(rowid == half - 1, right, pltpu.roll(y, half - 1, 0)).astype(BF16)

        def norm_row(row):
            @pl.when(r == 0)
            def _():
                for f in range(2):
                    halo[slot, row, f] = vid[slot, row, 0]
                    edge[slot, row, f] = edge[slot, row, 2]

            def past(f, c):
                norm_frame(halo[slot, row, f], edge[slot, row, f], row, f)
                return c

            def own(f, c):
                norm_frame(vid[slot, row, f], edge[slot, row, f + 2], row, f + 2)
                return c

            lax.fori_loop(0, 2, past, 0)
            lax.fori_loop(0, frames, own, 0)

        @pl.when(layer == 0)
        def _():
            load_own.wait()
            e_part.wait()

            @pl.when(not_last)
            def _():
                x_halo.wait_send()
                e_nxt.wait_send()
                e_diag.wait_send()

            @pl.when(not_first)
            def _():
                x_halo.wait_recv()
                e_nxt.wait_recv()
                e_diag.wait_recv()

            x_tail.wait()

            @pl.when(not_last)
            def _():
                halo_send(0, other, 1).start()

        @pl.when(layer > 0)
        def _():
            a, b = edge_sends(slot)
            a.wait()

            @pl.when(not_last)
            def _():
                b.wait_send()
                halo_send(slot, other, 0).wait_send()
                halo_send(slot, h, 1).wait_send()

            @pl.when(not_first)
            def _():
                b.wait_recv()
                halo_send(slot, other, 0).wait_recv()
                halo_send(slot, h, 1).wait_recv()

        def step_body(s, c):
            is0 = layer == 0
            hi = s // 2
            lo = lax.rem(s, 2)
            a_idx = jnp.where(is0, lo, hi)
            j_idx = jnp.where(is0, hi, lo)
            i_row = jnp.where(a_idx == 0, other, h)
            j_row = jnp.where(j_idx == 0, h, other)
            di = j_row - i_row + 1

            @pl.when(jnp.logical_and(is0, s == 2))
            def _():
                x_head.wait()

                @pl.when(not_last)
                def _():
                    halo_send(0, other, 1).wait_send()

                @pl.when(not_first)
                def _():
                    halo_send(0, other, 1).wait_recv()

            @pl.when(jnp.logical_or(s == 0, s == jnp.where(is0, 2, 1)))
            def _():
                norm_row(j_row)

            @pl.when(s == 0)
            def _():
                w_copy(layer).wait()

            d = jnp.where(j_idx == 0, 0.0, acc[i_row])
            p = None
            for k in range(3):
                q = jnp.dot(act[j_row, k * half:(k + frames) * half, :], w_buf[slot, k, di], preferred_element_type=F32)
                p = q if p is None else p + q
            acc[i_row] = d + p

            @pl.when(j_idx == 1)
            def _():
                def finish(f, c2):
                    rows = pl.ds(pl.multiple_of(f * half, half), half)
                    v = (acc[i_row, rows, :] + bias[layer]).astype(BF16).astype(F32)
                    res = vid[0, i_row, f].astype(F32)
                    vb = jnp.where(slot == 1, res + v, v).astype(BF16)
                    vid[nslot, i_row, f] = vb
                    v = vb.astype(F32)
                    s_acc[0] += fold(v)
                    s_acc[1] += fold(v * v)
                    ecol[i_row, f] = jnp.where(h == 0, v[half - 1:half], v[0:1])
                    return c2

                lax.fori_loop(0, frames, finish, 0)

                @pl.when(jnp.logical_and(layer < 3, not_last))
                def _():
                    remote(vid.at[nslot, i_row, tail], halo.at[nslot, i_row], hs_sem.at[a_idx], hr_sem.at[nslot, a_idx], nxt).start()

                @pl.when(jnp.logical_and(layer < 3, a_idx == 1))
                def _():
                    a, b = edge_sends(nslot)
                    a.start()

                    @pl.when(not_last)
                    def _():
                        b.start()

                @pl.when(jnp.logical_and(layer == 3, a_idx == 0))
                def _():
                    out_send().start()

                @pl.when(jnp.logical_and(layer == 3, a_idx == 1))
                def _():
                    out_local().start()

            return c

        lax.fori_loop(0, 4, step_body, 0)
        return carry

    lax.fori_loop(0, 4, layer_body, 0)
    out_local().wait()
    out_send().wait()


def solution(mesh):
    n_cp = mesh.shape["cp"]

    def local_decode(lat, conv_w, conv_b, gn_gamma, gn_beta):
        frames, _, width, chans = lat.shape
        half = width // 2
        n_dev = 2 * n_cp
        count = frames * n_cp * 2 * width * (chans // GROUPS)
        dma = pltpu.SemaphoreType.DMA
        any_spec = pl.BlockSpec(memory_space=pl.ANY)
        vmem = pl.BlockSpec(memory_space=pltpu.VMEM)
        return pl.pallas_call(
            functools.partial(kernel, (n_cp, frames, half, chans, count)),
            out_shape=jax.ShapeDtypeStruct(lat.shape, BF16),
            in_specs=[any_spec, any_spec, vmem, vmem, vmem],
            out_specs=any_spec,
            scratch_shapes=[
                pltpu.VMEM((2, 2, frames, half, chans), BF16),
                pltpu.VMEM((2, (frames + 2) * half, 3 * chans), BF16),
                pltpu.VMEM((2, frames * half, chans), F32),
                pltpu.VMEM((2, 3, 3, 3 * chans, chans), BF16),
                pltpu.VMEM(lat.shape, BF16),
                pltpu.VMEM((2, 2, 2, half, chans), BF16),
                pltpu.VMEM((2, 2, frames + 2, 1, chans), F32),
                pltpu.VMEM((2, frames, 1, chans), F32),
                pltpu.VMEM((2, 8, chans), F32),
                pltpu.VMEM((8, chans), F32),
                pltpu.VMEM((2, chans), F32),
                pltpu.VMEM((2, n_dev, 2, chans), F32),
                dma((2,)),
                dma((2,)),
                dma((2,)),
                dma((2,)),
                dma((2,)),
                dma((2, 2)),
                dma((3,)),
                dma((2, 2)),
                dma((3,)),
                dma((n_dev,)),
                dma((2, n_dev)),
                dma((3,)),
            ],
            compiler_params=pltpu.CompilerParams(collective_id=0, has_side_effects=True, vmem_limit_bytes=60 * 1024 * 1024),
            name="decode",
        )(
            lat,
            conv_w.reshape(4, 3, 3, 3 * chans, chans),
            conv_b.reshape(4, 1, chans),
            gn_gamma.reshape(4, 1, chans),
            gn_beta.reshape(4, 1, chans),
        )

    spec = P(("dp", "cp"), "hp", None, None)
    return jax.shard_map(local_decode, mesh=mesh, in_specs=(spec, P(), P(), P(), P()), out_specs=spec, check_vma=False)
```

```python
import functools

import jax
import jax.numpy as jnp
from jax import lax
from jax.experimental import pallas as pl
from jax.experimental.pallas import tpu as pltpu
from jax.sharding import PartitionSpec as P

GROUPS = 32
EPS = 1e-6
MESH = pl.DeviceIdType.MESH
F32 = jnp.float32
BF16 = jnp.bfloat16
OWN, OTH = 0, 1


def kernel(dims, lat, w_hbm, bias, gamma, beta, out, vid, act, acc, w_buf, x_in, halo, edge, ecol, s_acc, s_tot, s_send, s_recv,
           l_sem, w_sem, xs_sem, xr_sem, hs_sem, hr_sem, es_sem, er_sem, ss_sem, sr_sem, o_sem, os_sem, or_sem):
    n_cp, frames, half, chans, count = dims
    n_dev = 2 * n_cp
    per = frames // 4
    h = lax.axis_index("hp")
    r = lax.axis_index("cp")
    me = h * n_cp + r
    partner = {"hp": 1 - h, "cp": r}
    nxt = {"hp": h, "cp": lax.rem(r + 1, n_cp)}
    diag = {"hp": 1 - h, "cp": lax.rem(r + 1, n_cp)}
    not_last = r < n_cp - 1
    not_first = r > 0
    tail = pl.ds(frames - 2, 2)
    my_cols = pl.ds(pl.multiple_of(h * half, half), half)
    ot_cols = pl.ds(pl.multiple_of((1 - h) * half, half), half)

    def remote(src, dst, send, recv, dev):
        return pltpu.make_async_remote_copy(src_ref=src, dst_ref=dst, send_sem=send, recv_sem=recv, device_id=dev, device_id_type=MESH)

    def peer(step):
        t = lax.rem(me + step, n_dev)
        return {"hp": t // n_cp, "cp": lax.rem(t, n_cp)}

    load_x = pltpu.make_async_copy(lat, x_in, l_sem.at[0])
    load_own = pltpu.make_async_copy(lat.at[:, 0, my_cols, :], vid.at[0, OWN], l_sem.at[1])
    load_x.start()
    load_own.start()

    def w_copy(layer):
        slot = lax.rem(layer, 2)
        return pltpu.make_async_copy(w_hbm.at[layer], w_buf.at[slot], w_sem.at[slot])

    w_copy(0).start()

    barrier = pltpu.get_barrier_semaphore()
    for step in range(1, n_dev):
        pl.semaphore_signal(barrier, inc=1, device_id=peer(step), device_id_type=MESH)

    def fold(v):
        t = v[0:8]
        for k in range(1, v.shape[0] // 8):
            t = t + v[8 * k:8 * k + 8]
        return t

    s_acc[...] = jnp.zeros_like(s_acc)
    s_tot[...] = jnp.zeros_like(s_tot)
    load_x.wait()

    def first_sums(f, carry):
        v = x_in[f, 0].astype(F32)
        s_acc[0] += fold(v)
        s_acc[1] += fold(v * v)
        lo, hi = v[half - 1:half], v[half:half + 1]
        ecol[OWN, f] = jnp.where(h == 0, lo, hi)
        edge[0, OWN, f + 2] = jnp.where(h == 0, hi, lo)
        return carry

    lax.fori_loop(0, frames, first_sums, 0)
    pl.semaphore_wait(barrier, n_dev - 1)

    lane = lax.broadcasted_iota(jnp.int32, (8, chans), 1)
    rowid = lax.broadcasted_iota(jnp.int32, (half, chans), 0)
    n_group = chans // GROUPS

    def sum_sends(slot):
        return [remote(s_send, s_recv.at[slot, step], ss_sem.at[step], sr_sem.at[slot, step], peer(step)) for step in range(1, n_dev)]

    def sums_start(slot):
        s_send[0:1] = jnp.sum(s_acc[0], axis=0, keepdims=True)
        s_send[1:2] = jnp.sum(s_acc[1], axis=0, keepdims=True)
        s_acc[...] = jnp.zeros_like(s_acc)
        for c in sum_sends(slot):
            c.start()

    def sums_finish(slot, layer):
        total = s_send[...]
        for c in sum_sends(slot):
            c.wait()
        for step in range(1, n_dev):
            total = total + s_recv[slot, step]
        s_tot[0:2] = total
        t = s_tot[...]
        shift_by = 1
        while shift_by < n_group:
            up = pltpu.roll(t, chans - shift_by, 1)
            down = pltpu.roll(t, shift_by, 1)
            t = t + jnp.where((lane & shift_by) == 0, up, down)
            shift_by *= 2
        t = t * (1.0 / count)
        mean = t[0:1]
        inv = lax.rsqrt(t[1:2] - mean * mean + EPS)
        scale = inv * gamma[pl.ds(layer, 1), :]
        return 0.5 * scale, 0.5 * (beta[pl.ds(layer, 1), :] - mean * scale)

    def norm(coef, slot, row, p):
        def silu(v):
            u = v * coef[0] + coef[1]
            return u + u * jnp.tanh(u)

        v = halo[slot, row, p] if p < 2 else vid[slot, row, p - 2]
        y = silu(v.astype(F32))
        ye = silu(edge[slot, row, p])
        left = jnp.where(h == 0, 0.0, ye)
        right = jnp.where(h == 0, ye, 0.0)
        rows = pl.ds(p * half, half)
        act[row, rows, 0:chans] = jnp.where(rowid == 0, left, pltpu.roll(y, 1, 0)).astype(BF16)
        act[row, rows, chans:2 * chans] = y.astype(BF16)
        act[row, rows, 2 * chans:3 * chans] = jnp.where(rowid == half - 1, right, pltpu.roll(y, half - 1, 0)).astype(BF16)

    def dots(slot, i, js, lo, rows):
        total = None
        for j in js:
            di = 1 if i == j else (2 - 2 * h if i == OWN else 2 * h)
            for k in range(3):
                q = jnp.dot(act[j, pl.ds(lo + k * half, rows), :], w_buf[slot, k, di], preferred_element_type=F32)
                total = q if total is None else total + q
        return total

    def finish(layer, nslot, i, f0, p):
        b = bias[pl.ds(layer, 1), :]
        t1 = t2 = None
        for f in range(p.shape[0] // half):
            v = (p[f * half:(f + 1) * half] + b).astype(BF16).astype(F32)
            if isinstance(layer, int):
                vb = v.astype(BF16)
            else:
                res = vid[0, i, f0 + f].astype(F32)
                vb = jnp.where(nslot == 0, res + v, v).astype(BF16)
            vid[nslot, i, f0 + f] = vb
            v = vb.astype(F32)
            t1 = fold(v) if t1 is None else t1 + fold(v)
            t2 = fold(v * v) if t2 is None else t2 + fold(v * v)
            ecol[i, f0 + f] = jnp.where(h == 0, v[half - 1:half], v[0:1])
        s_acc[0] += t1
        s_acc[1] += t2

    def halo_send(slot, row):
        return remote(vid.at[slot, row, tail], halo.at[slot, row], hs_sem.at[row], hr_sem.at[slot, row], nxt)

    def edge_send(slot, row):
        return remote(ecol.at[row], edge.at[slot, 1 - row, pl.ds(2, frames)], es_sem.at[row, 0], er_sem.at[slot, 1 - row, 0], partner)

    def edge_diag(slot, row):
        return remote(ecol.at[row, tail], edge.at[slot, 1 - row, pl.ds(0, 2)], es_sem.at[row, 1], er_sem.at[slot, 1 - row, 1], diag)

    def edge_recv(slot, row):
        return edge_send(slot, 1 - row)

    def edge_diag_recv(slot, row):
        return edge_diag(slot, 1 - row)

    def repeat_first(slot, row):
        @pl.when(r == 0)
        def _():
            for f in range(2):
                halo[slot, row, f] = vid[slot, row, 0]
                edge[slot, row, f] = edge[slot, row, 2]

    pieces = [(0, 1), (1, per), (1 + per, per), (1 + 2 * per, frames - 1 - 2 * per)]

    def x_piece(g):
        f0, n = pieces[g]
        return remote(lat.at[pl.ds(f0, n), 0, ot_cols, :], vid.at[0, OTH, pl.ds(f0, n)], xs_sem.at[g], xr_sem.at[g], partner)

    sums_start(0)
    edge_send(0, OWN).start()
    x_halo = remote(lat.at[tail, 0, my_cols, :], halo.at[0, OWN], hs_sem.at[OWN], hr_sem.at[0, OWN], nxt)
    e_nxt = remote(edge.at[0, OWN, pl.ds(frames, 2)], edge.at[0, OWN, pl.ds(0, 2)], es_sem.at[OTH, 1], er_sem.at[0, OWN, 1], nxt)

    @pl.when(not_last)
    def _():
        edge_diag(0, OWN).start()
        e_nxt.start()
        x_halo.start()

    for g in (3, 2, 1, 0):
        x_piece(g).start()
    w_copy(1).start()
    load_own.wait()
    coef = sums_finish(0, 0)
    for p in range(2, frames + 2):
        norm(coef, 0, OWN, p)

    @pl.when(not_last)
    def _():
        x_halo.wait_send()
        e_nxt.wait_send()

    @pl.when(not_first)
    def _():
        x_halo.wait_recv()
        e_nxt.wait_recv()

    repeat_first(0, OWN)
    for p in range(2):
        norm(coef, 0, OWN, p)
    w_copy(0).wait()
    for i in (OTH, OWN):
        @pl.loop(0, 2)
        def _(c):
            lo = pl.multiple_of(c * (frames // 2) * half, half)
            acc[i, pl.ds(lo, frames // 2 * half), :] = dots(0, i, (OWN,), lo, frames // 2 * half)

    edge_send(0, OWN).wait_send()
    edge_recv(0, OTH).wait_recv()

    @pl.when(not_last)
    def _():
        edge_diag(0, OWN).wait_send()

    @pl.when(not_first)
    def _():
        edge_diag_recv(0, OTH).wait_recv()

    for g in (3, 2, 1, 0):
        x_piece(g).wait()
        if g == 3:
            @pl.when(not_last)
            def _():
                halo_send(0, OTH).start()
        if g == 0:
            @pl.when(not_first)
            def _():
                halo_send(0, OTH).wait_recv()

            repeat_first(0, OTH)
        for p in range(g * per, frames + 2 if g == 3 else (g + 1) * per):
            norm(coef, 0, OTH, p)
        rows = pl.ds(g * per * half, per * half)
        for i in (OTH, OWN):
            finish(0, 1, i, g * per, acc[i, rows, :] + dots(0, i, (OTH,), g * per * half, per * half))
        if g == 1:
            @pl.when(not_last)
            def _():
                halo_send(0, OTH).wait_send()
                halo_send(1, OTH).start()

    edge_send(1, OTH).start()

    @pl.when(not_last)
    def _():
        edge_diag(1, OTH).start()

    out_pieces = [(3 * per, per), (2 * per, per), (0, 2 * per)]

    def out_send(k):
        f0, n = out_pieces[k]
        return remote(vid.at[0, OTH, pl.ds(f0, n)], out.at[pl.ds(f0, n), 0, my_cols, :], os_sem.at[k], or_sem.at[k], partner)

    def out_local():
        return pltpu.make_async_copy(vid.at[0, OWN], out.at[:, 0, my_cols, :], o_sem.at[0])

    def layer_body(layer, carry):
        slot = lax.rem(layer, 2)
        nslot = 1 - slot
        last = layer == 3

        sums_start(slot)
        edge_send(slot, OWN).start()

        @pl.when(not_last)
        def _():
            edge_diag(slot, OWN).start()
            halo_send(slot, OWN).start()

        @pl.when(layer < 3)
        def _():
            w_copy(layer + 1).start()

        coef = sums_finish(slot, layer)
        edge_send(slot, OTH).wait_send()
        edge_recv(slot, OWN).wait_recv()
        edge_recv(slot, OTH).wait_recv()

        @pl.when(not_last)
        def _():
            edge_diag(slot, OTH).wait_send()
            halo_send(slot, OTH).wait_send()

        w_copy(layer).wait()

        def chunk(i, g):
            return dots(slot, i, (OWN, OTH), g * per * half, per * half)

        def norms(lo, hi):
            for p in range(lo, hi):
                for row in (OWN, OTH):
                    norm(coef, slot, row, p)

        norms(3 * per, frames + 2)
        p = chunk(OTH, 3)
        norms(2 * per, 3 * per)
        finish(layer, nslot, OTH, 3 * per, p)

        @pl.when(last)
        def _():
            out_send(0).start()

        p = chunk(OTH, 2)
        norms(per, 2 * per)
        finish(layer, nslot, OTH, 2 * per, p)

        @pl.when(last)
        def _():
            out_send(1).start()

        edge_send(slot, OWN).wait_send()

        @pl.when(not_last)
        def _():
            edge_diag(slot, OWN).wait_send()
            halo_send(slot, OWN).wait_send()

        @pl.when(not_first)
        def _():
            for row in (OWN, OTH):
                edge_diag_recv(slot, row).wait_recv()
                halo_send(slot, row).wait_recv()

        repeat_first(slot, OWN)
        repeat_first(slot, OTH)

        p = chunk(OTH, 1)
        norms(0, per)
        finish(layer, nslot, OTH, per, p)
        p = chunk(OTH, 0)
        finish(layer, nslot, OTH, 0, p)

        @pl.when(last)
        def _():
            out_send(2).start()

        @pl.when(jnp.logical_not(last))
        def _():
            edge_send(nslot, OTH).start()

            @pl.when(not_last)
            def _():
                edge_diag(nslot, OTH).start()
                halo_send(nslot, OTH).start()

        for g in (3, 2, 1, 0):
            p = chunk(OWN, g)
            finish(layer, nslot, OWN, g * per, p)
        return carry

    lax.fori_loop(1, 4, layer_body, 0)
    out_local().start()
    out_local().wait()
    for k in range(3):
        out_send(k).wait()


def solution(mesh):
    n_cp = mesh.shape["cp"]

    def local_decode(lat, conv_w, conv_b, gn_gamma, gn_beta):
        frames, _, width, chans = lat.shape
        half = width // 2
        n_dev = 2 * n_cp
        count = frames * n_cp * 2 * width * (chans // GROUPS)
        dma = pltpu.SemaphoreType.DMA
        any_spec = pl.BlockSpec(memory_space=pl.ANY)
        vmem = pl.BlockSpec(memory_space=pltpu.VMEM)
        return pl.pallas_call(
            functools.partial(kernel, (n_cp, frames, half, chans, count)),
            out_shape=jax.ShapeDtypeStruct(lat.shape, BF16),
            in_specs=[any_spec, any_spec, vmem, vmem, vmem],
            out_specs=any_spec,
            scratch_shapes=[
                pltpu.VMEM((2, 2, frames, half, chans), BF16),
                pltpu.VMEM((2, (frames + 2) * half, 3 * chans), BF16),
                pltpu.VMEM((2, frames * half, chans), F32),
                pltpu.VMEM((2, 3, 3, 3 * chans, chans), BF16),
                pltpu.VMEM(lat.shape, BF16),
                pltpu.VMEM((2, 2, 2, half, chans), BF16),
                pltpu.VMEM((2, 2, frames + 2, 1, chans), F32),
                pltpu.VMEM((2, frames, 1, chans), F32),
                pltpu.VMEM((2, 8, chans), F32),
                pltpu.VMEM((8, chans), F32),
                pltpu.VMEM((2, chans), F32),
                pltpu.VMEM((2, n_dev, 2, chans), F32),
                dma((2,)),
                dma((2,)),
                dma((4,)),
                dma((4,)),
                dma((2,)),
                dma((2, 2)),
                dma((2, 2)),
                dma((2, 2, 2)),
                dma((n_dev,)),
                dma((2, n_dev)),
                dma((1,)),
                dma((3,)),
                dma((3,)),
            ],
            compiler_params=pltpu.CompilerParams(collective_id=0, has_side_effects=True, vmem_limit_bytes=60 * 1024 * 1024),
            name="decode",
        )(lat, conv_w.reshape(4, 3, 3, 3 * chans, chans), conv_b, gn_gamma, gn_beta)

    spec = P(("dp", "cp"), "hp", None, None)
    return jax.shard_map(local_decode, mesh=mesh, in_specs=(spec, P(), P(), P(), P()), out_specs=spec, check_vma=False)
```

```python
import functools

import jax
import jax.numpy as jnp
from jax import lax
from jax.experimental import pallas as pl
from jax.experimental.pallas import tpu as pltpu
from jax.sharding import PartitionSpec as P

GROUPS = 32
EPS = 1e-6
MESH = pl.DeviceIdType.MESH
F32 = jnp.float32
BF16 = jnp.bfloat16
OWN, OTH = 0, 1


def kernel(dims, lat, w_hbm, bias, gamma, beta, out, vid, act, acc, w_buf, x_in, halo, edge, ecol, ext, xact, edge2, ecol2, xres,
           s_acc, s_tot, s_send, s_recv, l_sem, w_sem, xs_sem, xr_sem, hs_sem, hr_sem, es_sem, er_sem, ts_sem, tr_sem, cs_sem, cr_sem,
           rs_sem, ss_sem, sr_sem, o_sem, os_sem, or_sem):
    n_cp, frames, half, strip, chans, count = dims
    n_dev = 2 * n_cp
    per = frames // 4
    h = lax.axis_index("hp")
    r = lax.axis_index("cp")
    me = h * n_cp + r
    partner = {"hp": 1 - h, "cp": r}
    nxt = {"hp": h, "cp": lax.rem(r + 1, n_cp)}
    diag = {"hp": 1 - h, "cp": lax.rem(r + 1, n_cp)}
    not_last = r < n_cp - 1
    not_first = r > 0
    tail = pl.ds(frames - 2, 2)
    my_cols = pl.ds(pl.multiple_of(h * half, half), half)
    ot_cols = pl.ds(pl.multiple_of((1 - h) * half, half), half)
    part = half - strip
    part_cols = pl.ds(pl.multiple_of(h * strip, strip), part)
    edge_strip = pl.ds(pl.multiple_of((1 - h) * part, strip), strip)

    def remote(src, dst, send, recv, dev):
        return pltpu.make_async_remote_copy(src_ref=src, dst_ref=dst, send_sem=send, recv_sem=recv, device_id=dev, device_id_type=MESH)

    def peer(step):
        t = lax.rem(me + step, n_dev)
        return {"hp": t // n_cp, "cp": lax.rem(t, n_cp)}

    load_x = pltpu.make_async_copy(lat, x_in, l_sem.at[0])
    load_own = pltpu.make_async_copy(lat.at[:, 0, my_cols, :], vid.at[0, OWN], l_sem.at[1])
    load_x.start()
    load_own.start()

    def w_copy(layer):
        slot = lax.rem(layer, 2)
        return pltpu.make_async_copy(w_hbm.at[layer], w_buf.at[slot], w_sem.at[slot])

    w_copy(0).start()

    barrier = pltpu.get_barrier_semaphore()
    for step in range(1, n_dev):
        pl.semaphore_signal(barrier, inc=1, device_id=peer(step), device_id_type=MESH)

    def fold(v):
        t = v[0:8]
        for k in range(1, v.shape[0] // 8):
            t = t + v[8 * k:8 * k + 8]
        return t

    s_acc[...] = jnp.zeros_like(s_acc)
    s_tot[...] = jnp.zeros_like(s_tot)
    load_x.wait()

    def first_sums(f, carry):
        v = x_in[f, 0].astype(F32)
        s_acc[0] += fold(v)
        s_acc[1] += fold(v * v)
        lo, hi = v[half - 1:half], v[half:half + 1]
        ecol[OWN, f] = jnp.where(h == 0, lo, hi)
        edge[0, OWN, f + 2] = jnp.where(h == 0, hi, lo)
        return carry

    lax.fori_loop(0, frames, first_sums, 0)
    pl.semaphore_wait(barrier, n_dev - 1)

    lane = lax.broadcasted_iota(jnp.int32, (8, chans), 1)
    n_group = chans // GROUPS

    def sum_sends(slot):
        return [remote(s_send, s_recv.at[slot, step], ss_sem.at[step], sr_sem.at[slot, step], peer(step)) for step in range(1, n_dev)]

    def sums_start(slot):
        s_send[0:1] = jnp.sum(s_acc[0], axis=0, keepdims=True)
        s_send[1:2] = jnp.sum(s_acc[1], axis=0, keepdims=True)
        s_acc[...] = jnp.zeros_like(s_acc)
        for c in sum_sends(slot):
            c.start()

    def sums_finish(slot, layer):
        total = s_send[...]
        for c in sum_sends(slot):
            c.wait()
        for step in range(1, n_dev):
            total = total + s_recv[slot, step]
        s_tot[0:2] = total
        t = s_tot[...]
        shift_by = 1
        while shift_by < n_group:
            up = pltpu.roll(t, chans - shift_by, 1)
            down = pltpu.roll(t, shift_by, 1)
            t = t + jnp.where((lane & shift_by) == 0, up, down)
            shift_by *= 2
        t = t * (1.0 / count)
        mean = t[0:1]
        inv = lax.rsqrt(t[1:2] - mean * mean + EPS)
        scale = inv * gamma[pl.ds(layer, 1), :]
        return 0.5 * scale, 0.5 * (beta[pl.ds(layer, 1), :] - mean * scale)

    def silu(coef, v):
        u = v * coef[0] + coef[1]
        return u + u * jnp.tanh(u)

    def put_shifted(dst, row, p, y, left, right):
        n = y.shape[0]
        at = lax.broadcasted_iota(jnp.int32, y.shape, 0)
        dst[row, p, :, 0:chans] = jnp.where(at == 0, left, pltpu.roll(y, 1, 0)).astype(BF16)
        dst[row, p, :, chans:2 * chans] = y.astype(BF16)
        dst[row, p, :, 2 * chans:3 * chans] = jnp.where(at == n - 1, right, pltpu.roll(y, n - 1, 0)).astype(BF16)

    def norm(coef, slot, row, p):
        v = halo[slot, row, p] if p < 2 else vid[slot, row, p - 2]
        y = silu(coef, v.astype(F32))
        ye = silu(coef, edge[slot, row, p])
        put_shifted(act, row, p, y, jnp.where(h == 0, 0.0, ye), jnp.where(h == 0, ye, 0.0))

    def norm_ext(coef, row, p):
        mine = silu(coef, (halo[1, row, p] if p < 2 else vid[1, row, p - 2]).astype(F32))
        y = silu(coef, ext[row, p].astype(F32))
        far = silu(coef, edge2[row, p])
        put_shifted(xact, row, p, y, jnp.where(h == 0, mine[half - 1:half], far), jnp.where(h == 0, far, mine[0:1]))

    def dots(slot, i, js, lhs):
        total = None
        for j in js:
            if isinstance(i, int):
                di = 1 if i == j else (2 - 2 * h if i == OWN else 2 * h)
            else:
                di = jnp.where(i == OWN, 1, 2 * h)
            for k in range(3):
                v = lhs(j, k)
                v = v.reshape(v.shape[0] * v.shape[1], v.shape[2])
                q = jnp.dot(v, w_buf[slot, k, di], preferred_element_type=F32)
                total = q if total is None else total + q
        return total

    def frames_of(f0, n):
        return lambda j, k: act[j, pl.ds(f0 + k, n)]

    def finish(layer, nslot, i, f0, p):
        b = bias[pl.ds(layer, 1), :]
        t1 = t2 = None
        for f in range(p.shape[0] // half):
            v = (p[f * half:(f + 1) * half] + b).astype(BF16).astype(F32)
            if isinstance(layer, int):
                vb = v.astype(BF16)
            else:
                res = vid[0, i, f0 + f].astype(F32)
                vb = jnp.where(nslot == 0, res + v, v).astype(BF16)
            vid[nslot, i, f0 + f] = vb
            v = vb.astype(F32)
            t1 = fold(v) if t1 is None else t1 + fold(v)
            t2 = fold(v * v) if t2 is None else t2 + fold(v * v)
            ecol[i, f0 + f] = jnp.where(h == 0, v[half - 1:half], v[0:1])
        s_acc[0] += t1
        s_acc[1] += t2

    def halo_send(slot, row):
        return remote(vid.at[slot, row, tail], halo.at[slot, row], hs_sem.at[row], hr_sem.at[slot, row], nxt)

    def edge_send(slot, row):
        return remote(ecol.at[row], edge.at[slot, 1 - row, pl.ds(2, frames)], es_sem.at[row, 0], er_sem.at[slot, 1 - row, 0], partner)

    def edge_diag(slot, row):
        return remote(ecol.at[row, tail], edge.at[slot, 1 - row, pl.ds(0, 2)], es_sem.at[row, 1], er_sem.at[slot, 1 - row, 1], diag)

    def edge_recv(slot, row):
        return edge_send(slot, 1 - row)

    def edge_diag_recv(slot, row):
        return edge_diag(slot, 1 - row)

    def repeat_first(slot, row):
        @pl.when(r == 0)
        def _():
            for f in range(2):
                halo[slot, row, f] = vid[slot, row, 0]
                edge[slot, row, f] = edge[slot, row, 2]

    pieces = [(0, 1), (1, per), (1 + per, per), (1 + 2 * per, frames - 1 - 2 * per)]

    def x_piece(g):
        f0, n = pieces[g]
        return remote(lat.at[pl.ds(f0, n), 0, ot_cols, :], vid.at[0, OTH, pl.ds(f0, n)], xs_sem.at[g], xr_sem.at[g], partner)

    sums_start(0)
    edge_send(0, OWN).start()
    x_halo = remote(lat.at[tail, 0, my_cols, :], halo.at[0, OWN], hs_sem.at[OWN], hr_sem.at[0, OWN], nxt)
    e_nxt = remote(edge.at[0, OWN, pl.ds(frames, 2)], edge.at[0, OWN, pl.ds(0, 2)], es_sem.at[OTH, 1], er_sem.at[0, OWN, 1], nxt)

    @pl.when(not_last)
    def _():
        edge_diag(0, OWN).start()
        e_nxt.start()
        x_halo.start()

    for g in (3, 2, 1, 0):
        x_piece(g).start()
    w_copy(1).start()
    load_own.wait()
    coef = sums_finish(0, 0)
    for p in range(2, frames + 2):
        norm(coef, 0, OWN, p)

    @pl.when(not_last)
    def _():
        x_halo.wait_send()
        e_nxt.wait_send()

    @pl.when(not_first)
    def _():
        x_halo.wait_recv()
        e_nxt.wait_recv()

    repeat_first(0, OWN)
    for p in range(2):
        norm(coef, 0, OWN, p)
    w_copy(0).wait()

    @pl.loop(0, 4)
    def _(c):
        i = c // 2
        f0 = lax.rem(c, 2) * (frames // 2)
        rows = pl.ds(pl.multiple_of(f0 * half, half), frames // 2 * half)
        acc[i, rows, :] = dots(0, i, (OWN,), frames_of(f0, frames // 2))

    edge_send(0, OWN).wait_send()
    edge_recv(0, OTH).wait_recv()

    @pl.when(not_last)
    def _():
        edge_diag(0, OWN).wait_send()

    @pl.when(not_first)
    def _():
        edge_diag_recv(0, OTH).wait_recv()

    for g in (3, 2, 1, 0):
        x_piece(g).wait()
        if g == 3:
            @pl.when(not_last)
            def _():
                halo_send(0, OTH).start()
        if g == 0:
            @pl.when(not_first)
            def _():
                halo_send(0, OTH).wait_recv()

            repeat_first(0, OTH)
        for p in range(g * per, frames + 2 if g == 3 else (g + 1) * per):
            norm(coef, 0, OTH, p)
        rows = pl.ds(g * per * half, per * half)
        for i in (OTH, OWN):
            finish(0, 1, i, g * per, acc[i, rows, :] + dots(0, i, (OTH,), frames_of(g * per, per)))
        if g == 1:
            @pl.when(not_last)
            def _():
                halo_send(0, OTH).wait_send()
                halo_send(1, OTH).start()

    edge_send(1, OTH).start()

    @pl.when(not_last)
    def _():
        edge_diag(1, OTH).start()

    def strip_send(row):
        return remote(vid.at[1, row, :, edge_strip, :], ext.at[1 - row, pl.ds(2, frames)], ts_sem.at[row, 0], tr_sem.at[1 - row, 0], partner)

    def strip_diag(row):
        return remote(vid.at[1, row, tail, edge_strip, :], ext.at[1 - row, pl.ds(0, 2)], ts_sem.at[row, 1], tr_sem.at[1 - row, 1], diag)

    def col2_send(row):
        return remote(ecol2.at[row], edge2.at[1 - row, pl.ds(2, frames)], cs_sem.at[row, 0], cr_sem.at[1 - row, 0], partner)

    def col2_diag(row):
        return remote(ecol2.at[row, tail], edge2.at[1 - row, pl.ds(0, 2)], cs_sem.at[row, 1], cr_sem.at[1 - row, 1], diag)

    def res_send():
        return remote(vid.at[0, OTH, :, edge_strip, :], xres, rs_sem.at[0], rs_sem.at[1], partner)

    def head(slot, layer):
        sums_start(slot)
        edge_send(slot, OWN).start()

        @pl.when(not_last)
        def _():
            edge_diag(slot, OWN).start()
            halo_send(slot, OWN).start()

    def head_finish(slot, layer):
        coef = sums_finish(slot, layer)
        for row in (OTH, OWN):
            edge_send(slot, row).wait_send()
            edge_recv(slot, row).wait_recv()

        @pl.when(not_last)
        def _():
            for row in (OTH, OWN):
                edge_diag(slot, row).wait_send()
                halo_send(slot, row).wait_send()

        @pl.when(not_first)
        def _():
            for row in (OTH, OWN):
                edge_diag_recv(slot, row).wait_recv()
                halo_send(slot, row).wait_recv()

        repeat_first(slot, OWN)
        repeat_first(slot, OTH)
        w_copy(layer).wait()
        return coef

    def layer_body(layer, carry):
        slot = lax.rem(layer, 2)
        nslot = 1 - slot
        head(slot, layer)

        @pl.when(layer == 2)
        def _():
            res_send().start()

        w_copy(layer + 1).start()
        coef = head_finish(slot, layer)

        def norms(lo, hi):
            for row in (OWN, OTH):
                for p in range(lo, hi):
                    norm(coef, slot, row, p)

        def chunk(i, g):
            finish(layer, nslot, i, g * per, dots(slot, i, (OWN, OTH), frames_of(g * per, per)))

        norms(3 * per, frames + 2)
        norms(2 * per, 3 * per)
        chunk(OTH, 3)
        norms(per, 2 * per)
        chunk(OTH, 2)
        norms(0, per)
        chunk(OTH, 1)
        chunk(OTH, 0)
        edge_send(nslot, OTH).start()

        @pl.when(not_last)
        def _():
            edge_diag(nslot, OTH).start()
            halo_send(nslot, OTH).start()

        @pl.when(layer == 2)
        def _():
            strip_send(OTH).start()

            @pl.when(not_last)
            def _():
                strip_diag(OTH).start()

        for g in (3, 2, 1, 0):
            chunk(OWN, g)
        return carry

    lax.fori_loop(1, 3, layer_body, 0)

    wide = frames // 3

    def out_send(k):
        fs = pl.ds(k * wide, wide)
        dst = out.at[fs, 0, pl.ds(pl.multiple_of(h * (half + strip), strip), part), :]
        return remote(vid.at[0, OTH, fs, part_cols, :], dst, os_sem.at[k], or_sem.at[k], partner)

    def out_local():
        return pltpu.make_async_copy(vid.at[0, OWN], out.at[:, 0, my_cols, :], o_sem.at[0])

    def out_ext():
        dst = out.at[:, 0, pl.ds(pl.multiple_of(half - h * strip, strip), strip), :]
        return pltpu.make_async_copy(xres, dst, o_sem.at[1])

    head(1, 3)
    strip_send(OWN).start()

    @pl.when(not_last)
    def _():
        strip_diag(OWN).start()

    def columns2(f, carry):
        for row in (OWN, OTH):
            v = vid[1, row, f, strip:half - strip, :].astype(F32)
            ecol2[row, f] = jnp.where(h == 0, v[half - 2 * strip - 1:half - 2 * strip], v[0:1])
        return carry

    lax.fori_loop(0, frames, columns2, 0)
    for row in (OWN, OTH):
        col2_send(row).start()

    @pl.when(not_last)
    def _():
        for row in (OWN, OTH):
            col2_diag(row).start()

    coef = head_finish(1, 3)

    def norms(lo, hi):
        for row in (OWN, OTH):
            for p in range(lo, hi):
                norm(coef, 1, row, p)

    def close(res, p):
        return (res.astype(F32) + (p + bias[3:4, :]).astype(BF16).astype(F32)).astype(BF16)

    def part_chunk(k):
        f0 = k * wide
        p = dots(1, OTH, (OWN, OTH), lambda j, t: act[j, pl.ds(f0 + t, wide), part_cols, :])
        for f in range(wide):
            vid[0, OTH, f0 + f, part_cols, :] = close(vid[0, OTH, f0 + f, part_cols, :], p[f * part:(f + 1) * part])

    def own_chunk(g):
        p = dots(1, OWN, (OWN, OTH), frames_of(g * per, per))
        for f in range(per):
            vid[0, OWN, g * per + f] = close(vid[0, OWN, g * per + f], p[f * half:(f + 1) * half])

    norms(2 * wide, frames + 2)
    norms(wide, 2 * wide)
    part_chunk(2)
    out_send(2).start()
    norms(0, wide)
    part_chunk(1)
    out_send(1).start()
    part_chunk(0)
    out_send(0).start()
    for row in (OWN, OTH):
        strip_send(row).wait()
        col2_send(row).wait()

    @pl.when(not_last)
    def _():
        for row in (OWN, OTH):
            strip_diag(row).wait_send()
            col2_diag(row).wait_send()

    @pl.when(not_first)
    def _():
        for row in (OWN, OTH):
            strip_diag(row).wait_recv()
            col2_diag(row).wait_recv()

    @pl.when(r == 0)
    def _():
        for row in (OWN, OTH):
            for f in range(2):
                ext[row, f] = ext[row, 2]
                edge2[row, f] = edge2[row, 2]

    res_send().wait()
    for row in (OWN, OTH):
        for p in range(frames + 2):
            norm_ext(coef, row, p)
    for g in (3, 2, 1, 0):
        own_chunk(g)
    p = dots(1, OWN, (OWN, OTH), lambda j, t: xact[j, pl.ds(t, frames)])
    out_local().start()
    for f in range(frames):
        xres[f] = close(xres[f], p[f * strip:(f + 1) * strip])
    out_ext().start()
    out_local().wait()
    out_ext().wait()
    for k in range(3):
        out_send(k).wait()


def solution(mesh):
    n_cp = mesh.shape["cp"]

    def local_decode(lat, conv_w, conv_b, gn_gamma, gn_beta):
        frames, _, width, chans = lat.shape
        half = width // 2
        strip = half // 4
        n_dev = 2 * n_cp
        count = frames * n_cp * 2 * width * (chans // GROUPS)
        dma = pltpu.SemaphoreType.DMA
        any_spec = pl.BlockSpec(memory_space=pl.ANY)
        vmem = pl.BlockSpec(memory_space=pltpu.VMEM)
        return pl.pallas_call(
            functools.partial(kernel, (n_cp, frames, half, strip, chans, count)),
            out_shape=jax.ShapeDtypeStruct(lat.shape, BF16),
            in_specs=[any_spec, any_spec, vmem, vmem, vmem],
            out_specs=any_spec,
            scratch_shapes=[
                pltpu.VMEM((2, 2, frames, half, chans), BF16),
                pltpu.VMEM((2, frames + 2, half, 3 * chans), BF16),
                pltpu.VMEM((2, frames * half, chans), F32),
                pltpu.VMEM((2, 3, 3, 3 * chans, chans), BF16),
                pltpu.VMEM(lat.shape, BF16),
                pltpu.VMEM((2, 2, 2, half, chans), BF16),
                pltpu.VMEM((2, 2, frames + 2, 1, chans), F32),
                pltpu.VMEM((2, frames, 1, chans), F32),
                pltpu.VMEM((2, frames + 2, strip, chans), BF16),
                pltpu.VMEM((2, frames + 2, strip, 3 * chans), BF16),
                pltpu.VMEM((2, frames + 2, 1, chans), F32),
                pltpu.VMEM((2, frames, 1, chans), F32),
                pltpu.VMEM((frames, strip, chans), BF16),
                pltpu.VMEM((2, 8, chans), F32),
                pltpu.VMEM((8, chans), F32),
                pltpu.VMEM((2, chans), F32),
                pltpu.VMEM((2, n_dev, 2, chans), F32),
                dma((2,)),
                dma((2,)),
                dma((4,)),
                dma((4,)),
                dma((2,)),
                dma((2, 2)),
                dma((2, 2)),
                dma((2, 2, 2)),
                dma((2, 2)),
                dma((2, 2)),
                dma((2, 2)),
                dma((2, 2)),
                dma((2,)),
                dma((n_dev,)),
                dma((2, n_dev)),
                dma((2,)),
                dma((3,)),
                dma((3,)),
            ],
            compiler_params=pltpu.CompilerParams(collective_id=0, has_side_effects=True, vmem_limit_bytes=60 * 1024 * 1024),
            name="decode",
        )(lat, conv_w.reshape(4, 3, 3, 3 * chans, chans), conv_b, gn_gamma, gn_beta)

    spec = P(("dp", "cp"), "hp", None, None)
    return jax.shard_map(local_decode, mesh=mesh, in_specs=(spec, P(), P(), P(), P()), out_specs=spec, check_vma=False)
```

```python
import functools

import jax
import jax.numpy as jnp
from jax import lax
from jax.experimental import pallas as pl
from jax.experimental.pallas import tpu as pltpu
from jax.sharding import PartitionSpec as P

GROUPS = 32
EPS = 1e-6
MESH = pl.DeviceIdType.MESH
F32 = jnp.float32
BF16 = jnp.bfloat16
OWN, OTH = 0, 1


def kernel(dims, lat, w_hbm, bias_hbm, gamma_hbm, beta_hbm, out, bias, gamma, beta, vid, act, acc, w_buf, x_in, halo, edge, ecol, ext, xact, edge2, ecol2, xres,
           s_acc, s_tot, s_send, s_recv, l_sem, w_sem, xs_sem, xr_sem, hs_sem, hr_sem, es_sem, er_sem, ts_sem, tr_sem, cs_sem, cr_sem,
           rs_sem, ss_sem, sr_sem, o_sem, os_sem, or_sem):
    n_cp, frames, half, strip, chans, count = dims
    n_dev = 2 * n_cp
    per = frames // 4
    h = lax.axis_index("hp")
    r = lax.axis_index("cp")
    me = h * n_cp + r
    partner = {"hp": 1 - h, "cp": r}
    nxt = {"hp": h, "cp": lax.rem(r + 1, n_cp)}
    diag = {"hp": 1 - h, "cp": lax.rem(r + 1, n_cp)}
    not_last = r < n_cp - 1
    not_first = r > 0
    tail = pl.ds(frames - 2, 2)
    my_cols = pl.ds(pl.multiple_of(h * half, half), half)
    ot_cols = pl.ds(pl.multiple_of((1 - h) * half, half), half)
    part = half - strip
    part_cols = pl.ds(pl.multiple_of(h * strip, strip), part)
    edge_strip = pl.ds(pl.multiple_of((1 - h) * part, strip), strip)

    def remote(src, dst, send, recv, dev):
        return pltpu.make_async_remote_copy(src_ref=src, dst_ref=dst, send_sem=send, recv_sem=recv, device_id=dev, device_id_type=MESH)

    def peer(step):
        t = lax.rem(me + step, n_dev)
        return {"hp": t // n_cp, "cp": lax.rem(t, n_cp)}

    def load_x(k):
        fs = pl.ds(k * per, per)
        return pltpu.make_async_copy(lat.at[fs], x_in.at[fs], l_sem.at[k])

    for k in range(4):
        load_x(k).start()
    small = [pltpu.make_async_copy(a, b, l_sem.at[4 + k]) for k, (a, b) in enumerate([(bias_hbm, bias), (gamma_hbm, gamma), (beta_hbm, beta)])]
    load_own = pltpu.make_async_copy(lat.at[:, 0, my_cols, :], vid.at[0, OWN], l_sem.at[7])

    def w_copy(layer):
        slot = lax.rem(layer, 2)
        return pltpu.make_async_copy(w_hbm.at[layer], w_buf.at[slot], w_sem.at[slot])

    barrier = pltpu.get_barrier_semaphore()
    for step in range(1, n_dev):
        pl.semaphore_signal(barrier, inc=1, device_id=peer(step), device_id_type=MESH)
    for c in small:
        c.start()
    load_own.start()
    w_copy(0).start()

    def fold(v):
        t = v[0:8]
        for k in range(1, v.shape[0] // 8):
            t = t + v[8 * k:8 * k + 8]
        return t

    s_acc[...] = jnp.zeros_like(s_acc)
    s_tot[...] = jnp.zeros_like(s_tot)

    def first_sums(f, carry):
        v = x_in[f, 0].astype(F32)
        s_acc[0] += fold(v)
        s_acc[1] += fold(v * v)
        lo, hi = v[half - 1:half], v[half:half + 1]
        ecol[OWN, f] = jnp.where(h == 0, lo, hi)
        edge[0, OWN, f + 2] = jnp.where(h == 0, hi, lo)
        return carry

    for k in range(4):
        load_x(k).wait()
        lax.fori_loop(k * per, (k + 1) * per, first_sums, 0)
    pl.semaphore_wait(barrier, n_dev - 1)

    lane = lax.broadcasted_iota(jnp.int32, (8, chans), 1)
    n_group = chans // GROUPS

    def sum_sends(slot):
        return [remote(s_send, s_recv.at[slot, step], ss_sem.at[step], sr_sem.at[slot, step], peer(step)) for step in range(1, n_dev)]

    def sums_start(slot):
        s_send[0:1] = jnp.sum(s_acc[0], axis=0, keepdims=True)
        s_send[1:2] = jnp.sum(s_acc[1], axis=0, keepdims=True)
        s_acc[...] = jnp.zeros_like(s_acc)
        for c in sum_sends(slot):
            c.start()

    def sums_finish(slot, layer):
        total = s_send[...]
        for c in sum_sends(slot):
            c.wait()
        for step in range(1, n_dev):
            total = total + s_recv[slot, step]
        s_tot[0:2] = total
        t = s_tot[...]
        unit = 1
        while unit < n_group:
            place = (lane // unit) & 3
            g = t
            for d in range(1, 4):
                up = pltpu.roll(t, chans - d * unit, 1)
                down = pltpu.roll(t, (4 - d) * unit, 1)
                g = g + jnp.where(place + d < 4, up, down)
            t = g
            unit *= 4
        t = t * (1.0 / count)
        mean = t[0:1]
        inv = lax.rsqrt(t[1:2] - mean * mean + EPS)
        scale = inv * gamma[pl.ds(layer, 1), :]
        return 0.5 * scale, 0.5 * (beta[pl.ds(layer, 1), :] - mean * scale)

    def silu(coef, v):
        u = v * coef[0] + coef[1]
        return u + u * jnp.tanh(u)

    def put_shifted(dst, row, p, y, left, right):
        n = y.shape[0]
        at = lax.broadcasted_iota(jnp.int32, (8, chans), 0)
        before = pltpu.roll(y, 1, 0)
        after = pltpu.roll(y, n - 1, 0)
        before = jnp.concatenate([jnp.where(at == 0, left, before[0:8]), before[8:]], axis=0)
        after = jnp.concatenate([after[:n - 8], jnp.where(at == 7, right, after[n - 8:])], axis=0)
        dst[row, p, :, 0:chans] = before.astype(BF16)
        dst[row, p, :, chans:2 * chans] = y.astype(BF16)
        dst[row, p, :, 2 * chans:3 * chans] = after.astype(BF16)

    def norm(coef, slot, row, p):
        v = halo[slot, row, p] if p < 2 else vid[slot, row, p - 2]
        y = silu(coef, v.astype(F32))
        ye = silu(coef, edge[slot, row, p])
        put_shifted(act, row, p, y, jnp.where(h == 0, 0.0, ye), jnp.where(h == 0, ye, 0.0))

    def norm_ext(coef, row, p):
        mine = silu(coef, (halo[1, row, p] if p < 2 else vid[1, row, p - 2]).astype(F32))
        y = silu(coef, ext[row, p].astype(F32))
        far = silu(coef, edge2[row, p])
        put_shifted(xact, row, p, y, jnp.where(h == 0, mine[half - 1:half], far), jnp.where(h == 0, far, mine[0:1]))

    def dots(slot, i, js, lhs):
        total = None
        for j in js:
            if isinstance(i, int):
                di = 1 if i == j else (2 - 2 * h if i == OWN else 2 * h)
            else:
                di = jnp.where(i == OWN, 1, 2 * h)
            for k in (2, 1, 0):
                v = lhs(j, k)
                v = v.reshape(v.shape[0] * v.shape[1], v.shape[2])
                q = jnp.dot(v, w_buf[slot, k, di], preferred_element_type=F32)
                total = q if total is None else total + q
        return total

    def frames_of(f0, n):
        return lambda j, k: act[j, pl.ds(f0 + k, n)]

    def finish(layer, nslot, i, f0, p):
        b = bias[pl.ds(layer, 1), :]
        t1 = t2 = None
        for f in range(p.shape[0] // half):
            v = (p[f * half:(f + 1) * half] + b).astype(BF16).astype(F32)
            if isinstance(layer, int):
                vb = v.astype(BF16)
            else:
                res = vid[0, i, f0 + f].astype(F32)
                vb = jnp.where(nslot == 0, res + v, v).astype(BF16)
            vid[nslot, i, f0 + f] = vb
            v = vb.astype(F32)
            t1 = fold(v) if t1 is None else t1 + fold(v)
            t2 = fold(v * v) if t2 is None else t2 + fold(v * v)
            ecol[i, f0 + f] = jnp.where(h == 0, v[half - 1:half], v[0:1])
        s_acc[0] += t1
        s_acc[1] += t2

    def halo_send(slot, row):
        return remote(vid.at[slot, row, tail], halo.at[slot, row], hs_sem.at[row], hr_sem.at[slot, row], nxt)

    def edge_send(slot, row):
        return remote(ecol.at[row], edge.at[slot, 1 - row, pl.ds(2, frames)], es_sem.at[row, 0], er_sem.at[slot, 1 - row, 0], partner)

    def edge_diag(slot, row):
        return remote(ecol.at[row, tail], edge.at[slot, 1 - row, pl.ds(0, 2)], es_sem.at[row, 1], er_sem.at[slot, 1 - row, 1], diag)

    def edge_recv(slot, row):
        return edge_send(slot, 1 - row)

    def edge_diag_recv(slot, row):
        return edge_diag(slot, 1 - row)

    def repeat_first(slot, row):
        @pl.when(r == 0)
        def _():
            for f in range(2):
                halo[slot, row, f] = vid[slot, row, 0]
                edge[slot, row, f] = edge[slot, row, 2]

    pieces = [(0, 1), (1, per), (1 + per, per), (1 + 2 * per, frames - 1 - 2 * per)]

    def x_piece(g):
        f0, n = pieces[g]
        return remote(lat.at[pl.ds(f0, n), 0, ot_cols, :], vid.at[0, OTH, pl.ds(f0, n)], xs_sem.at[g], xr_sem.at[g], partner)

    sums_start(0)
    edge_send(0, OWN).start()
    x_halo = remote(lat.at[tail, 0, my_cols, :], halo.at[0, OWN], hs_sem.at[OWN], hr_sem.at[0, OWN], nxt)
    e_nxt = remote(edge.at[0, OWN, pl.ds(frames, 2)], edge.at[0, OWN, pl.ds(0, 2)], es_sem.at[OTH, 1], er_sem.at[0, OWN, 1], nxt)

    @pl.when(not_last)
    def _():
        edge_diag(0, OWN).start()
        e_nxt.start()
        x_halo.start()

    for g in (3, 2, 1, 0):
        x_piece(g).start()
    w_copy(1).start()
    load_own.wait()
    for c in small:
        c.wait()
    coef = sums_finish(0, 0)
    for p in range(2, frames + 2):
        norm(coef, 0, OWN, p)

    @pl.when(not_last)
    def _():
        x_halo.wait_send()
        e_nxt.wait_send()

    @pl.when(not_first)
    def _():
        x_halo.wait_recv()
        e_nxt.wait_recv()

    repeat_first(0, OWN)
    for p in range(2):
        norm(coef, 0, OWN, p)
    w_copy(0).wait()

    @pl.loop(0, 4)
    def _(c):
        i = c // 2
        f0 = lax.rem(c, 2) * (frames // 2)
        rows = pl.ds(pl.multiple_of(f0 * half, half), frames // 2 * half)
        acc[i, rows, :] = dots(0, i, (OWN,), frames_of(f0, frames // 2))

    edge_send(0, OWN).wait_send()
    edge_recv(0, OTH).wait_recv()

    @pl.when(not_last)
    def _():
        edge_diag(0, OWN).wait_send()

    @pl.when(not_first)
    def _():
        edge_diag_recv(0, OTH).wait_recv()

    for g in (3, 2, 1, 0):
        x_piece(g).wait()
        if g == 3:
            @pl.when(not_last)
            def _():
                halo_send(0, OTH).start()
        if g == 0:
            @pl.when(not_first)
            def _():
                halo_send(0, OTH).wait_recv()

            repeat_first(0, OTH)
        for p in range(g * per, frames + 2 if g == 3 else (g + 1) * per):
            norm(coef, 0, OTH, p)
        rows = pl.ds(g * per * half, per * half)
        for i in (OTH, OWN):
            finish(0, 1, i, g * per, acc[i, rows, :] + dots(0, i, (OTH,), frames_of(g * per, per)))
        if g == 1:
            @pl.when(not_last)
            def _():
                halo_send(0, OTH).wait_send()
                halo_send(1, OTH).start()

    edge_send(1, OTH).start()

    @pl.when(not_last)
    def _():
        edge_diag(1, OTH).start()

    def strip_send(row):
        return remote(vid.at[1, row, :, edge_strip, :], ext.at[1 - row, pl.ds(2, frames)], ts_sem.at[row, 0], tr_sem.at[1 - row, 0], partner)

    def strip_diag(row):
        return remote(vid.at[1, row, tail, edge_strip, :], ext.at[1 - row, pl.ds(0, 2)], ts_sem.at[row, 1], tr_sem.at[1 - row, 1], diag)

    def col2_send(row):
        return remote(ecol2.at[row], edge2.at[1 - row, pl.ds(2, frames)], cs_sem.at[row, 0], cr_sem.at[1 - row, 0], partner)

    def col2_diag(row):
        return remote(ecol2.at[row, tail], edge2.at[1 - row, pl.ds(0, 2)], cs_sem.at[row, 1], cr_sem.at[1 - row, 1], diag)

    def res_send():
        return remote(vid.at[0, OTH, :, edge_strip, :], xres, rs_sem.at[0], rs_sem.at[1], partner)

    def head(slot, layer):
        sums_start(slot)
        edge_send(slot, OWN).start()

        @pl.when(not_last)
        def _():
            edge_diag(slot, OWN).start()
            halo_send(slot, OWN).start()

    def head_finish(slot, layer):
        coef = sums_finish(slot, layer)
        for row in (OTH, OWN):
            edge_send(slot, row).wait_send()
            edge_recv(slot, row).wait_recv()

        @pl.when(not_last)
        def _():
            for row in (OTH, OWN):
                edge_diag(slot, row).wait_send()
                halo_send(slot, row).wait_send()

        @pl.when(not_first)
        def _():
            for row in (OTH, OWN):
                edge_diag_recv(slot, row).wait_recv()
                halo_send(slot, row).wait_recv()

        repeat_first(slot, OWN)
        repeat_first(slot, OTH)
        w_copy(layer).wait()
        return coef

    def layer_body(layer, carry):
        slot = lax.rem(layer, 2)
        nslot = 1 - slot
        head(slot, layer)

        @pl.when(layer == 2)
        def _():
            res_send().start()

        w_copy(layer + 1).start()
        coef = head_finish(slot, layer)

        def norms(lo, hi):
            for row in (OWN, OTH):
                for p in reversed(range(lo, hi)):
                    norm(coef, slot, row, p)

        def chunk(i, g):
            finish(layer, nslot, i, g * per, dots(slot, i, (OWN, OTH), frames_of(g * per, per)))

        norms(3 * per, frames + 2)
        norms(2 * per, 3 * per)
        chunk(OTH, 3)
        norms(per, 2 * per)
        chunk(OTH, 2)
        norms(0, per)
        chunk(OTH, 1)
        chunk(OTH, 0)
        edge_send(nslot, OTH).start()

        @pl.when(not_last)
        def _():
            edge_diag(nslot, OTH).start()
            halo_send(nslot, OTH).start()

        @pl.when(layer == 2)
        def _():
            strip_send(OTH).start()

            @pl.when(not_last)
            def _():
                strip_diag(OTH).start()

        for g in (3, 2, 1, 0):
            chunk(OWN, g)
        return carry

    lax.fori_loop(1, 3, layer_body, 0)

    wide = frames // 3

    def out_send(k):
        fs = pl.ds(k * wide, wide)
        dst = out.at[fs, 0, pl.ds(pl.multiple_of(h * (half + strip), strip), part), :]
        return remote(vid.at[0, OTH, fs, part_cols, :], dst, os_sem.at[k], or_sem.at[k], partner)

    def out_local():
        return pltpu.make_async_copy(vid.at[0, OWN], out.at[:, 0, my_cols, :], o_sem.at[0])

    def out_ext():
        dst = out.at[:, 0, pl.ds(pl.multiple_of(half - h * strip, strip), strip), :]
        return pltpu.make_async_copy(xres, dst, o_sem.at[1])

    head(1, 3)
    strip_send(OWN).start()

    @pl.when(not_last)
    def _():
        strip_diag(OWN).start()

    def columns2(f, carry):
        for row in (OWN, OTH):
            v = vid[1, row, f, strip:half - strip, :].astype(F32)
            ecol2[row, f] = jnp.where(h == 0, v[half - 2 * strip - 1:half - 2 * strip], v[0:1])
        return carry

    lax.fori_loop(0, frames, columns2, 0)
    for row in (OWN, OTH):
        col2_send(row).start()

    @pl.when(not_last)
    def _():
        for row in (OWN, OTH):
            col2_diag(row).start()

    coef = head_finish(1, 3)

    def norms(lo, hi):
        for row in (OWN, OTH):
            for p in reversed(range(lo, hi)):
                norm(coef, 1, row, p)

    def close(res, p):
        return (res.astype(F32) + (p + bias[3:4, :]).astype(BF16).astype(F32)).astype(BF16)

    def part_chunk(k):
        f0 = k * wide
        p = dots(1, OTH, (OWN, OTH), lambda j, t: act[j, pl.ds(f0 + t, wide), part_cols, :])
        for f in range(wide):
            vid[0, OTH, f0 + f, part_cols, :] = close(vid[0, OTH, f0 + f, part_cols, :], p[f * part:(f + 1) * part])

    def own_chunk(g):
        p = dots(1, OWN, (OWN, OTH), frames_of(g * per, per))
        for f in range(per):
            vid[0, OWN, g * per + f] = close(vid[0, OWN, g * per + f], p[f * half:(f + 1) * half])

    norms(2 * wide, frames + 2)
    norms(wide, 2 * wide)
    part_chunk(2)
    out_send(2).start()
    norms(0, wide)
    part_chunk(1)
    out_send(1).start()
    part_chunk(0)
    out_send(0).start()
    for row in (OWN, OTH):
        strip_send(row).wait()
        col2_send(row).wait()

    @pl.when(not_last)
    def _():
        for row in (OWN, OTH):
            strip_diag(row).wait_send()
            col2_diag(row).wait_send()

    @pl.when(not_first)
    def _():
        for row in (OWN, OTH):
            strip_diag(row).wait_recv()
            col2_diag(row).wait_recv()

    @pl.when(r == 0)
    def _():
        for row in (OWN, OTH):
            for f in range(2):
                ext[row, f] = ext[row, 2]
                edge2[row, f] = edge2[row, 2]

    res_send().wait()
    for row in (OWN, OTH):
        for p in range(frames + 2):
            norm_ext(coef, row, p)
    for g in (3, 2, 1, 0):
        own_chunk(g)
    p = dots(1, OWN, (OWN, OTH), lambda j, t: xact[j, pl.ds(t, frames)])
    out_local().start()
    for f in range(frames):
        xres[f] = close(xres[f], p[f * strip:(f + 1) * strip])
    out_ext().start()
    out_local().wait()
    out_ext().wait()
    for k in range(3):
        out_send(k).wait()


def solution(mesh):
    n_cp = mesh.shape["cp"]

    def local_decode(lat, conv_w, conv_b, gn_gamma, gn_beta):
        frames, _, width, chans = lat.shape
        half = width // 2
        strip = half // 4
        n_dev = 2 * n_cp
        count = frames * n_cp * 2 * width * (chans // GROUPS)
        dma = pltpu.SemaphoreType.DMA
        any_spec = pl.BlockSpec(memory_space=pl.ANY)
        return pl.pallas_call(
            functools.partial(kernel, (n_cp, frames, half, strip, chans, count)),
            out_shape=jax.ShapeDtypeStruct(lat.shape, BF16),
            in_specs=[any_spec] * 5,
            out_specs=any_spec,
            scratch_shapes=[
                pltpu.VMEM(conv_b.shape, F32),
                pltpu.VMEM(gn_gamma.shape, F32),
                pltpu.VMEM(gn_beta.shape, F32),
                pltpu.VMEM((2, 2, frames, half, chans), BF16),
                pltpu.VMEM((2, frames + 2, half, 3 * chans), BF16),
                pltpu.VMEM((2, frames * half, chans), F32),
                pltpu.VMEM((2, 3, 3, 3 * chans, chans), BF16),
                pltpu.VMEM(lat.shape, BF16),
                pltpu.VMEM((2, 2, 2, half, chans), BF16),
                pltpu.VMEM((2, 2, frames + 2, 1, chans), F32),
                pltpu.VMEM((2, frames, 1, chans), F32),
                pltpu.VMEM((2, frames + 2, strip, chans), BF16),
                pltpu.VMEM((2, frames + 2, strip, 3 * chans), BF16),
                pltpu.VMEM((2, frames + 2, 1, chans), F32),
                pltpu.VMEM((2, frames, 1, chans), F32),
                pltpu.VMEM((frames, strip, chans), BF16),
                pltpu.VMEM((2, 8, chans), F32),
                pltpu.VMEM((8, chans), F32),
                pltpu.VMEM((2, chans), F32),
                pltpu.VMEM((2, n_dev, 2, chans), F32),
                dma((8,)),
                dma((2,)),
                dma((4,)),
                dma((4,)),
                dma((2,)),
                dma((2, 2)),
                dma((2, 2)),
                dma((2, 2, 2)),
                dma((2, 2)),
                dma((2, 2)),
                dma((2, 2)),
                dma((2, 2)),
                dma((2,)),
                dma((n_dev,)),
                dma((2, n_dev)),
                dma((2,)),
                dma((3,)),
                dma((3,)),
            ],
            compiler_params=pltpu.CompilerParams(collective_id=0, has_side_effects=True, vmem_limit_bytes=52 * 1024 * 1024),
            name="decode",
        )(*(pltpu.with_memory_space_constraint(a, pltpu.HBM) for a in (lat, conv_w.reshape(4, 3, 3, 3 * chans, chans), conv_b, gn_gamma, gn_beta)))

    spec = P(("dp", "cp"), "hp", None, None)
    return jax.shard_map(local_decode, mesh=mesh, in_specs=(spec, P(), P(), P(), P()), out_specs=spec, check_vma=False)
```

```python
import functools

import jax
import jax.numpy as jnp
from jax import lax
from jax.experimental import pallas as pl
from jax.experimental.pallas import tpu as pltpu
from jax.sharding import PartitionSpec as P

GROUPS = 32
EPS = 1e-6
MESH = pl.DeviceIdType.MESH
F32 = jnp.float32
BF16 = jnp.bfloat16
HALVES = OWN, OTH = 0, 1


def kernel(dims, lat, w_hbm, bias_hbm, gamma_hbm, beta_hbm, out, bias, gamma, beta, vid, act, acc, w_buf, x_in, halo, edge, ecol, ext, xact, edge2, ecol2, xres,
           s_acc, s_tot, s_send, s_recv, l_sem, w_sem, xs_sem, xr_sem, hs_sem, hr_sem, es_sem, er_sem, ts_sem, tr_sem, cs_sem, cr_sem,
           rs_sem, ss_sem, sr_sem, o_sem, os_sem, or_sem):
    n_cp, frames, half, strip, chans, count = dims
    n_dev = 2 * n_cp
    per = frames // 4
    h = lax.axis_index("hp")
    r = lax.axis_index("cp")
    me = h * n_cp + r
    partner = {"hp": 1 - h, "cp": r}
    nxt = {"hp": h, "cp": lax.rem(r + 1, n_cp)}
    diag = {"hp": 1 - h, "cp": lax.rem(r + 1, n_cp)}
    not_last = r < n_cp - 1
    not_first = r > 0
    tail = pl.ds(frames - 2, 2)
    my_cols = pl.ds(pl.multiple_of(h * half, half), half)
    ot_cols = pl.ds(pl.multiple_of((1 - h) * half, half), half)
    hc = chans // 2
    lanes = [slice(c * hc, (c + 1) * hc) for c in HALVES]
    part = half - strip
    part_cols = pl.ds(pl.multiple_of(h * strip, strip), part)
    edge_strip = pl.ds(pl.multiple_of((1 - h) * part, strip), strip)

    def remote(src, dst, send, recv, dev):
        return pltpu.make_async_remote_copy(src_ref=src, dst_ref=dst, send_sem=send, recv_sem=recv, device_id=dev, device_id_type=MESH)

    def peer(step):
        t = lax.rem(me + step, n_dev)
        return {"hp": t // n_cp, "cp": lax.rem(t, n_cp)}

    def load_x(k):
        fs = pl.ds(k * per, per)
        return pltpu.make_async_copy(lat.at[fs], x_in.at[fs], l_sem.at[k])

    for k in range(4):
        load_x(k).start()
    small = [pltpu.make_async_copy(a, b, l_sem.at[4 + k]) for k, (a, b) in enumerate([(bias_hbm, bias), (gamma_hbm, gamma), (beta_hbm, beta)])]
    load_own = pltpu.make_async_copy(lat.at[:, 0, my_cols, :], vid.at[0, OWN], l_sem.at[7])

    def w_copy(layer):
        slot = lax.rem(layer, 2)
        return pltpu.make_async_copy(w_hbm.at[layer], w_buf.at[slot], w_sem.at[slot])

    barrier = pltpu.get_barrier_semaphore()
    for step in range(1, n_dev):
        pl.semaphore_signal(barrier, inc=1, device_id=peer(step), device_id_type=MESH)
    for c in small:
        c.start()
    load_own.start()
    w_copy(0).start()

    def fold(v):
        t = v[0:8]
        for k in range(1, v.shape[0] // 8):
            t = t + v[8 * k:8 * k + 8]
        return t

    s_acc[...] = jnp.zeros_like(s_acc)
    s_tot[...] = jnp.zeros_like(s_tot)

    def first_sums(f, carry):
        v = x_in[f, 0].astype(F32)
        for c in HALVES:
            s_acc[c, 0] += fold(v[:, lanes[c]])
            s_acc[c, 1] += fold(v[:, lanes[c]] * v[:, lanes[c]])
        lo, hi = v[half - 1:half], v[half:half + 1]
        ecol[OWN, f] = jnp.where(h == 0, lo, hi)
        edge[0, OWN, f + 2] = jnp.where(h == 0, hi, lo)
        return carry

    for k in range(4):
        load_x(k).wait()
        lax.fori_loop(k * per, (k + 1) * per, first_sums, 0)
    pl.semaphore_wait(barrier, n_dev - 1)

    lane = lax.broadcasted_iota(jnp.int32, (8, hc), 1)
    n_group = chans // GROUPS

    def sum_sends(slot, c):
        return [remote(s_send.at[c], s_recv.at[slot, c, step], ss_sem.at[c, step], sr_sem.at[slot, c, step], peer(step)) for step in range(1, n_dev)]

    def sums_start(slot, c):
        s_send[c, 0:1] = jnp.sum(s_acc[c, 0], axis=0, keepdims=True)
        s_send[c, 1:2] = jnp.sum(s_acc[c, 1], axis=0, keepdims=True)
        s_acc[c] = jnp.zeros_like(s_acc[c])
        for d in sum_sends(slot, c):
            d.start()

    def coefficients(slot, c, layer):
        total = s_send[c]
        for step in range(1, n_dev):
            total = total + s_recv[slot, c, step]
        s_tot[c, 0:2] = total
        t = s_tot[c]
        unit = 1
        while unit < n_group:
            place = (lane // unit) & 3
            g = t
            for d in range(1, 4):
                up = pltpu.roll(t, hc - d * unit, 1)
                down = pltpu.roll(t, (4 - d) * unit, 1)
                g = g + jnp.where(place + d < 4, up, down)
            t = g
            unit *= 4
        t = t * (1.0 / count)
        mean = t[0:1]
        inv = lax.rsqrt(t[1:2] - mean * mean + EPS)
        scale = inv * gamma[pl.ds(layer, 1), lanes[c]]
        return 0.5 * scale, 0.5 * (beta[pl.ds(layer, 1), lanes[c]] - mean * scale)

    def silu(coef, v):
        u = v * coef[0] + coef[1]
        return u + u * jnp.tanh(u)

    def put_shifted(dst, row, p, y, left, right, start):
        n, w = y.shape
        at = lax.broadcasted_iota(jnp.int32, (8, w), 0)
        before = pltpu.roll(y, 1, 0)
        after = pltpu.roll(y, n - 1, 0)
        before = jnp.concatenate([jnp.where(at == 0, left, before[0:8]), before[8:]], axis=0)
        after = jnp.concatenate([after[:n - 8], jnp.where(at == 7, right, after[n - 8:])], axis=0)
        for d, v in enumerate((before, y, after)):
            dst[row, p, :, d * chans + start:d * chans + start + w] = v.astype(BF16)

    def norm(coef, slot, row, p, c):
        v = halo[slot, row, p, :, lanes[c]] if p < 2 else vid[slot, row, p - 2, :, lanes[c]]
        y = silu(coef, v.astype(F32))
        ye = silu(coef, edge[slot, row, p, :, lanes[c]])
        put_shifted(act, row, p, y, jnp.where(h == 0, 0.0, ye), jnp.where(h == 0, ye, 0.0), c * hc)

    def norm_ext(coef, row, p, c):
        mine = silu(coef, (halo[1, row, p, :, lanes[c]] if p < 2 else vid[1, row, p - 2, :, lanes[c]]).astype(F32))
        y = silu(coef, ext[row, p, :, lanes[c]].astype(F32))
        far = silu(coef, edge2[row, p, :, lanes[c]])
        put_shifted(xact, row, p, y, jnp.where(h == 0, mine[half - 1:half], far), jnp.where(h == 0, far, mine[0:1]), c * hc)

    def dots(slot, i, js, lhs, k_half=None, n_half=None):
        cols = slice(0, chans) if n_half is None else lanes[n_half]
        total = None
        for j in js:
            if isinstance(i, int):
                di = 1 if i == j else (2 - 2 * h if i == OWN else 2 * h)
            else:
                di = jnp.where(i == OWN, 1, 2 * h)
            left, right = [], []
            for k in (2, 1, 0):
                for d in range(3):
                    for c in HALVES:
                        if k_half is None or c == k_half:
                            at = slice(d * chans + c * hc, d * chans + (c + 1) * hc)
                            v = lhs(j, k, at)
                            left.append(v.reshape(v.shape[0] * v.shape[1], v.shape[2]))
                            right.append(w_buf[slot, k, di, at, cols])
            q = jnp.dot(jnp.concatenate(left, axis=1), jnp.concatenate(right, axis=0), preferred_element_type=F32)
            total = q if total is None else total + q
        return total

    def frames_of(f0, n):
        return lambda j, k, at: act[j, pl.ds(f0 + k, n), :, at]

    def finish(layer, nslot, i, f0, p, c):
        b = bias[pl.ds(layer, 1), lanes[c]]
        t1 = t2 = None
        for f in range(p.shape[0] // half):
            v = (p[f * half:(f + 1) * half] + b).astype(BF16).astype(F32)
            if isinstance(layer, int):
                vb = v.astype(BF16)
            else:
                res = vid[0, i, f0 + f, :, lanes[c]].astype(F32)
                vb = jnp.where(nslot == 0, res + v, v).astype(BF16)
            vid[nslot, i, f0 + f, :, lanes[c]] = vb
            v = vb.astype(F32)
            t1 = fold(v) if t1 is None else t1 + fold(v)
            t2 = fold(v * v) if t2 is None else t2 + fold(v * v)
            ecol[i, f0 + f, :, lanes[c]] = jnp.where(h == 0, v[half - 1:half], v[0:1])
        s_acc[c, 0] += t1
        s_acc[c, 1] += t2

    def halo_send(slot, row, c):
        return remote(vid.at[slot, row, tail, :, lanes[c]], halo.at[slot, row, :, :, lanes[c]], hs_sem.at[row, c], hr_sem.at[slot, row, c], nxt)

    def edge_send(slot, row, c):
        return remote(ecol.at[row, :, :, lanes[c]], edge.at[slot, 1 - row, pl.ds(2, frames), :, lanes[c]], es_sem.at[row, 0, c],
                      er_sem.at[slot, 1 - row, 0, c], partner)

    def edge_diag(slot, row, c):
        return remote(ecol.at[row, tail, :, lanes[c]], edge.at[slot, 1 - row, pl.ds(0, 2), :, lanes[c]], es_sem.at[row, 1, c],
                      er_sem.at[slot, 1 - row, 1, c], diag)

    def repeat_first(slot, row, cols):
        @pl.when(r == 0)
        def _():
            for f in HALVES:
                halo[slot, row, f, :, cols] = vid[slot, row, 0, :, cols]
                edge[slot, row, f, :, cols] = edge[slot, row, 2, :, cols]

    def half_out(slot, c):
        sums_start(slot, c)
        for row in (OTH, OWN):
            edge_send(slot, row, c).start()

        @pl.when(not_last)
        def _():
            for row in (OTH, OWN):
                edge_diag(slot, row, c).start()
                halo_send(slot, row, c).start()

    def half_in(slot, c, layer):
        for d in sum_sends(slot, c):
            d.wait()
        for row in (OTH, OWN):
            edge_send(slot, row, c).wait()

        @pl.when(not_last)
        def _():
            for row in (OTH, OWN):
                edge_diag(slot, row, c).wait_send()
                halo_send(slot, row, c).wait_send()

        @pl.when(not_first)
        def _():
            for row in (OTH, OWN):
                edge_diag(slot, row, c).wait_recv()
                halo_send(slot, row, c).wait_recv()

        repeat_first(slot, OWN, lanes[c])
        repeat_first(slot, OTH, lanes[c])
        return coefficients(slot, c, layer)

    pieces = [(0, 1), (1, per), (1 + per, per), (1 + 2 * per, frames - 1 - 2 * per)]

    def x_piece(g):
        f0, n = pieces[g]
        return remote(lat.at[pl.ds(f0, n), 0, ot_cols, :], vid.at[0, OTH, pl.ds(f0, n)], xs_sem.at[g], xr_sem.at[g], partner)

    every = slice(0, chans)
    x_halo = remote(lat.at[tail, 0, my_cols, :], halo.at[0, OWN], hs_sem.at[OWN, 0], hr_sem.at[0, OWN, 0], nxt)
    x_pass = remote(vid.at[0, OTH, tail], halo.at[0, OTH], hs_sem.at[OTH, 0], hr_sem.at[0, OTH, 0], nxt)
    e_part = remote(ecol.at[OWN], edge.at[0, OTH, pl.ds(2, frames)], es_sem.at[OWN, 0, 0], er_sem.at[0, OTH, 0, 0], partner)
    e_nxt = remote(edge.at[0, OWN, pl.ds(frames, 2)], edge.at[0, OWN, pl.ds(0, 2)], es_sem.at[OTH, 1, 0], er_sem.at[0, OWN, 1, 0], nxt)
    e_diag = remote(ecol.at[OWN, tail], edge.at[0, OTH, pl.ds(0, 2)], es_sem.at[OWN, 1, 0], er_sem.at[0, OTH, 1, 0], diag)
    for c in HALVES:
        sums_start(0, c)
    e_part.start()

    @pl.when(not_last)
    def _():
        e_diag.start()
        e_nxt.start()
        x_halo.start()

    for g in (3, 2, 1, 0):
        x_piece(g).start()
    w_copy(1).start()
    load_own.wait()
    for c in small:
        c.wait()
    for c in HALVES:
        for d in sum_sends(0, c):
            d.wait()
    coef = [coefficients(0, c, 0) for c in HALVES]
    for p in range(2, frames + 2):
        for c in HALVES:
            norm(coef[c], 0, OWN, p, c)

    @pl.when(not_last)
    def _():
        x_halo.wait_send()
        e_nxt.wait_send()

    @pl.when(not_first)
    def _():
        x_halo.wait_recv()
        e_nxt.wait_recv()

    repeat_first(0, OWN, every)
    for p in range(2):
        for c in HALVES:
            norm(coef[c], 0, OWN, p, c)
    w_copy(0).wait()

    @pl.loop(0, 4)
    def _(c):
        i = c // 2
        f0 = lax.rem(c, 2) * (frames // 2)
        rows = pl.ds(pl.multiple_of(f0 * half, half), frames // 2 * half)
        acc[i, rows, :] = dots(0, i, (OWN,), frames_of(f0, frames // 2))

    e_part.wait()

    @pl.when(not_last)
    def _():
        e_diag.wait_send()

    @pl.when(not_first)
    def _():
        e_diag.wait_recv()

    def last_k(i, g, c):
        rows = pl.ds(g * per * half, per * half)
        finish(0, 1, i, g * per, acc[i, rows, lanes[c]] + dots(0, i, (OTH,), frames_of(g * per, per), n_half=c), c)

    for g in (3, 2, 1, 0):
        x_piece(g).wait()
        if g == 3:
            @pl.when(not_last)
            def _():
                x_pass.start()
        if g == 0:
            @pl.when(not_last)
            def _():
                x_pass.wait_send()

            @pl.when(not_first)
            def _():
                x_pass.wait_recv()

            repeat_first(0, OTH, every)
        for p in reversed(range(g * per, frames + 2 if g == 3 else (g + 1) * per)):
            for c in HALVES:
                norm(coef[c], 0, OTH, p, c)
        rows = pl.ds(g * per * half, per * half)
        for i in (OTH, OWN):
            if g > 1:
                p = acc[i, rows, :] + dots(0, i, (OTH,), frames_of(g * per, per))
                for c in HALVES:
                    finish(0, 1, i, g * per, p[:, lanes[c]], c)
            else:
                last_k(i, g, 0)
    half_out(1, 0)
    for g in (1, 0):
        for i in (OTH, OWN):
            last_k(i, g, 1)
    half_out(1, 1)

    def strip_send(row, c):
        return remote(vid.at[1, row, :, edge_strip, lanes[c]], ext.at[1 - row, pl.ds(2, frames), :, lanes[c]], ts_sem.at[row, 0, c],
                      tr_sem.at[1 - row, 0, c], partner)

    def strip_diag(row, c):
        return remote(vid.at[1, row, tail, edge_strip, lanes[c]], ext.at[1 - row, pl.ds(0, 2), :, lanes[c]], ts_sem.at[row, 1, c],
                      tr_sem.at[1 - row, 1, c], diag)

    def col2_send(row):
        return remote(ecol2.at[row], edge2.at[1 - row, pl.ds(2, frames)], cs_sem.at[row, 0], cr_sem.at[1 - row, 0], partner)

    def col2_diag(row):
        return remote(ecol2.at[row, tail], edge2.at[1 - row, pl.ds(0, 2)], cs_sem.at[row, 1], cr_sem.at[1 - row, 1], diag)

    def res_send():
        return remote(vid.at[0, OTH, :, edge_strip, :], xres, rs_sem.at[0], rs_sem.at[1], partner)

    def layer_body(layer, carry):
        slot = lax.rem(layer, 2)
        nslot = 1 - slot
        w_copy(layer + 1).start()

        @pl.when(layer == 2)
        def _():
            res_send().start()

        def norms(lo, hi, c):
            for row in (OWN, OTH):
                for p in reversed(range(lo, hi)):
                    norm(coef[c], slot, row, p, c)

        def first_k(i, g):
            acc[i, g * per * half:(g + 1) * per * half, :] = dots(slot, i, (OWN, OTH), frames_of(g * per, per), k_half=0)

        coef = [half_in(slot, 0, layer)]
        w_copy(layer).wait()
        norms(3 * per, frames + 2, 0)
        norms(2 * per, 3 * per, 0)
        first_k(OTH, 3)
        norms(per, 2 * per, 0)
        first_k(OTH, 2)
        norms(0, per, 0)
        first_k(OTH, 1)
        first_k(OTH, 0)
        coef.append(half_in(slot, 1, layer))
        norms(3 * per, frames + 2, 1)
        first_k(OWN, 3)
        norms(2 * per, 3 * per, 1)
        first_k(OWN, 2)
        norms(per, 2 * per, 1)
        first_k(OWN, 1)
        norms(0, per, 1)
        first_k(OWN, 0)
        for c in HALVES:
            for i in (OTH, OWN):
                for g in (3, 2, 1, 0):
                    rows = slice(g * per * half, (g + 1) * per * half)
                    p = dots(slot, i, (OWN, OTH), frames_of(g * per, per), k_half=1, n_half=c)
                    finish(layer, nslot, i, g * per, acc[i, rows, lanes[c]] + p, c)
            half_out(nslot, c)

            @pl.when(layer == 2)
            def _():
                for row in (OTH, OWN):
                    strip_send(row, c).start()

                @pl.when(not_last)
                def _():
                    for row in (OTH, OWN):
                        strip_diag(row, c).start()

        return carry

    lax.fori_loop(1, 3, layer_body, 0)

    wide = frames // 4
    pieces_out = (3, 2, 1, 0)

    def out_send(k):
        fs = pl.ds(k * wide, wide)
        dst = out.at[fs, 0, pl.ds(pl.multiple_of(h * (half + strip), strip), part), :]
        return remote(vid.at[0, OTH, fs, part_cols, :], dst, os_sem.at[k], or_sem.at[k], partner)

    def out_local():
        return pltpu.make_async_copy(vid.at[0, OWN], out.at[:, 0, my_cols, :], o_sem.at[0])

    def out_ext():
        dst = out.at[:, 0, pl.ds(pl.multiple_of(half - h * strip, strip), strip), :]
        return pltpu.make_async_copy(xres, dst, o_sem.at[1])

    def norms(lo, hi, c):
        for row in (OWN, OTH):
            for p in reversed(range(lo, hi)):
                norm(coef[c], 1, row, p, c)

    def close(res, p):
        return (res.astype(F32) + (p + bias[3:4, :]).astype(BF16).astype(F32)).astype(BF16)

    def part_dots(k, k_half):
        return dots(1, OTH, (OWN, OTH), lambda j, t, at: act[j, pl.ds(k * wide + t, wide), part_cols, at], k_half)

    def part_chunk(k):
        rows = slice(k * wide * part, (k + 1) * wide * part)
        p = acc[OTH, rows, :] + part_dots(k, 1)
        for f in range(wide):
            fr = k * wide + f
            vid[0, OTH, fr, part_cols, :] = close(vid[0, OTH, fr, part_cols, :], p[f * part:(f + 1) * part])
        out_send(k).start()

    def own_chunk(g):
        if g == 3:
            p = acc[OWN, g * per * half:(g + 1) * per * half, :] + dots(1, OWN, (OWN, OTH), frames_of(g * per, per), 1)
        else:
            p = dots(1, OWN, (OWN, OTH), frames_of(g * per, per))
        for f in range(per):
            vid[0, OWN, g * per + f] = close(vid[0, OWN, g * per + f], p[f * half:(f + 1) * half])

    coef = [half_in(1, 0, 3)]
    w_copy(3).wait()
    def norms_for(k, c):
        norms(k * wide, frames + 2 if k == 3 else (k + 1) * wide, c)

    norms_for(3, 0)
    norms_for(2, 0)
    for k in pieces_out:
        acc[OTH, k * wide * part:(k + 1) * wide * part, :] = part_dots(k, 0)
        if k > 1:
            norms_for(k - 2, 0)
    acc[OWN, 3 * per * half:4 * per * half, :] = dots(1, OWN, (OWN, OTH), frames_of(3 * per, per), 0)

    def columns2(f, carry):
        for row in (OWN, OTH):
            v = vid[1, row, f, strip:half - strip, :].astype(F32)
            ecol2[row, f] = jnp.where(h == 0, v[half - 2 * strip - 1:half - 2 * strip], v[0:1])
        return carry

    lax.fori_loop(0, frames, columns2, 0)
    for row in (OWN, OTH):
        col2_send(row).start()

    @pl.when(not_last)
    def _():
        for row in (OWN, OTH):
            col2_diag(row).start()

    coef.append(half_in(1, 1, 3))
    norms_for(3, 1)
    for k in pieces_out:
        if k > 0:
            norms_for(k - 1, 1)
        part_chunk(k)
    for row in (OWN, OTH):
        col2_send(row).wait()
        for c in HALVES:
            strip_send(row, c).wait()

    @pl.when(not_last)
    def _():
        for row in (OWN, OTH):
            col2_diag(row).wait_send()
            for c in HALVES:
                strip_diag(row, c).wait_send()

    @pl.when(not_first)
    def _():
        for row in (OWN, OTH):
            col2_diag(row).wait_recv()
            for c in HALVES:
                strip_diag(row, c).wait_recv()

    @pl.when(r == 0)
    def _():
        for row in (OWN, OTH):
            for f in HALVES:
                ext[row, f] = ext[row, 2]
                edge2[row, f] = edge2[row, 2]

    res_send().wait()
    for row in (OWN, OTH):
        for p in range(frames + 2):
            for c in HALVES:
                norm_ext(coef[c], row, p, c)
    for g in (3, 2, 1, 0):
        own_chunk(g)
    p = dots(1, OWN, (OWN, OTH), lambda j, t, at: xact[j, pl.ds(t, frames), :, at])
    out_local().start()
    for f in range(frames):
        xres[f] = close(xres[f], p[f * strip:(f + 1) * strip])
    out_ext().start()
    out_local().wait()
    out_ext().wait()
    for k in pieces_out:
        out_send(k).wait()


def solution(mesh):
    n_cp = mesh.shape["cp"]

    def local_decode(lat, conv_w, conv_b, gn_gamma, gn_beta):
        frames, _, width, chans = lat.shape
        half = width // 2
        strip = half // 4
        n_dev = 2 * n_cp
        count = frames * n_cp * 2 * width * (chans // GROUPS)
        dma = pltpu.SemaphoreType.DMA

        def pair(*more):
            return dma((2, *more))

        any_spec = pl.BlockSpec(memory_space=pl.ANY)
        return pl.pallas_call(
            functools.partial(kernel, (n_cp, frames, half, strip, chans, count)),
            out_shape=jax.ShapeDtypeStruct(lat.shape, BF16),
            in_specs=[any_spec] * 5,
            out_specs=any_spec,
            scratch_shapes=[
                pltpu.VMEM(conv_b.shape, F32),
                pltpu.VMEM(gn_gamma.shape, F32),
                pltpu.VMEM(gn_beta.shape, F32),
                pltpu.VMEM((2, 2, frames, half, chans), BF16),
                pltpu.VMEM((2, frames + 2, half, 3 * chans), BF16),
                pltpu.VMEM((2, frames * half, chans), F32),
                pltpu.VMEM((2, 3, 3, 3 * chans, chans), BF16),
                pltpu.VMEM(lat.shape, BF16),
                pltpu.VMEM((2, 2, 2, half, chans), BF16),
                pltpu.VMEM((2, 2, frames + 2, 1, chans), F32),
                pltpu.VMEM((2, frames, 1, chans), F32),
                pltpu.VMEM((2, frames + 2, strip, chans), BF16),
                pltpu.VMEM((2, frames + 2, strip, 3 * chans), BF16),
                pltpu.VMEM((2, frames + 2, 1, chans), F32),
                pltpu.VMEM((2, frames, 1, chans), F32),
                pltpu.VMEM((frames, strip, chans), BF16),
                pltpu.VMEM((2, 2, 8, chans // 2), F32),
                pltpu.VMEM((2, 8, chans // 2), F32),
                pltpu.VMEM((2, 2, chans // 2), F32),
                pltpu.VMEM((2, 2, n_dev, 2, chans // 2), F32),
                dma((8,)),
                pair(),
                dma((4,)),
                dma((4,)),
                pair(2),
                pair(2, 2),
                pair(2, 2),
                pair(2, 2, 2),
                pair(2, 2),
                pair(2, 2),
                pair(2),
                pair(2),
                pair(),
                pair(n_dev),
                pair(2, n_dev),
                pair(),
                dma((4,)),
                dma((4,)),
            ],
            compiler_params=pltpu.CompilerParams(collective_id=0, has_side_effects=True, vmem_limit_bytes=52 * 1024 * 1024),
            name="decode",
        )(*(pltpu.with_memory_space_constraint(a, pltpu.HBM) for a in (lat, conv_w.reshape(4, 3, 3, 3 * chans, chans), conv_b, gn_gamma, gn_beta)))

    spec = P(("dp", "cp"), "hp", None, None)
    return jax.shard_map(local_decode, mesh=mesh, in_specs=(spec, P(), P(), P(), P()), out_specs=spec, check_vma=False)
```

```python
import functools

import jax
import jax.numpy as jnp
from jax import lax
from jax.experimental import pallas as pl
from jax.experimental.pallas import tpu as pltpu
from jax.sharding import PartitionSpec as P

GROUPS = 32
EPS = 1e-6
MESH = pl.DeviceIdType.MESH
F32 = jnp.float32
BF16 = jnp.bfloat16
HALVES = OWN, OTH = 0, 1


def kernel(dims, lat, w_hbm, bias_hbm, gamma_hbm, beta_hbm, out, bias, gamma, beta, vid, act, acc, w_buf, x_in, halo, edge, ecol, ext, xact, edge2, ecol2, xres,
           s_acc, s_tot, s_send, s_recv, l_sem, w_sem, xs_sem, xr_sem, hs_sem, hr_sem, es_sem, er_sem, ts_sem, tr_sem, cs_sem, cr_sem,
           rs_sem, ss_sem, sr_sem, o_sem, os_sem, or_sem):
    n_cp, frames, half, strip, chans, count = dims
    n_dev = 2 * n_cp
    per = frames // 4
    h = lax.axis_index("hp")
    r = lax.axis_index("cp")
    me = h * n_cp + r
    partner = {"hp": 1 - h, "cp": r}
    nxt = {"hp": h, "cp": lax.rem(r + 1, n_cp)}
    diag = {"hp": 1 - h, "cp": lax.rem(r + 1, n_cp)}
    not_last = r < n_cp - 1
    not_first = r > 0
    tail = pl.ds(frames - 2, 2)
    my_cols = pl.ds(pl.multiple_of(h * half, half), half)
    ot_cols = pl.ds(pl.multiple_of((1 - h) * half, half), half)
    hc = chans // 2
    lanes = [slice(c * hc, (c + 1) * hc) for c in HALVES]
    part = half - strip
    part_cols = pl.ds(pl.multiple_of(h * strip, strip), part)
    edge_strip = pl.ds(pl.multiple_of((1 - h) * part, strip), strip)

    def remote(src, dst, send, recv, dev):
        return pltpu.make_async_remote_copy(src_ref=src, dst_ref=dst, send_sem=send, recv_sem=recv, device_id=dev, device_id_type=MESH)

    def peer(step):
        t = lax.rem(me + step, n_dev)
        return {"hp": t // n_cp, "cp": lax.rem(t, n_cp)}

    def load_x(k):
        fs = pl.ds(k * per, per)
        return pltpu.make_async_copy(lat.at[fs], x_in.at[fs], l_sem.at[k])

    for k in range(4):
        load_x(k).start()
    small = [pltpu.make_async_copy(a, b, l_sem.at[4 + k]) for k, (a, b) in enumerate([(bias_hbm, bias), (gamma_hbm, gamma), (beta_hbm, beta)])]
    load_own = pltpu.make_async_copy(lat.at[:, 0, my_cols, :], vid.at[0, OWN], l_sem.at[7])

    def w_copy(layer):
        slot = lax.rem(layer, 2)
        return pltpu.make_async_copy(w_hbm.at[layer], w_buf.at[slot], w_sem.at[slot])

    barrier = pltpu.get_barrier_semaphore()
    for step in range(1, n_dev):
        pl.semaphore_signal(barrier, inc=1, device_id=peer(step), device_id_type=MESH)
    for c in small:
        c.start()
    load_own.start()
    w_copy(0).start()

    def fold(v):
        t = v[0:8]
        for k in range(1, v.shape[0] // 8):
            t = t + v[8 * k:8 * k + 8]
        return t

    s_acc[...] = jnp.zeros_like(s_acc)
    s_tot[...] = jnp.zeros_like(s_tot)

    def first_sums(f, carry):
        v = x_in[f, 0].astype(F32)
        for c in HALVES:
            s_acc[c, 0] += fold(v[:, lanes[c]])
            s_acc[c, 1] += fold(v[:, lanes[c]] * v[:, lanes[c]])
        lo, hi = v[half - 1:half], v[half:half + 1]
        ecol[OWN, f] = jnp.where(h == 0, lo, hi)
        edge[0, OWN, f + 2] = jnp.where(h == 0, hi, lo)
        return carry

    starts = (0, 1, 1 + per, 1 + 2 * per, frames - 1, frames)

    def x_piece(g):
        fs = pl.ds(starts[g], starts[g + 1] - starts[g])
        return remote(lat.at[fs, 0, ot_cols, :], vid.at[0, OTH, fs], xs_sem.at[g], xr_sem.at[g], partner)

    for k in range(4):
        load_x(k).wait()
        if k == 1:
            pl.semaphore_wait(barrier, n_dev - 1)
            x_piece(4).start()
        lax.fori_loop(k * per, (k + 1) * per, first_sums, 0)

    lane = lax.broadcasted_iota(jnp.int32, (8, hc), 1)
    n_group = chans // GROUPS

    def sum_sends(slot, c):
        return [remote(s_send.at[c], s_recv.at[slot, c, step], ss_sem.at[c, step], sr_sem.at[slot, c, step], peer(step)) for step in range(1, n_dev)]

    def sums_start(slot, c):
        s_send[c, 0:1] = jnp.sum(s_acc[c, 0], axis=0, keepdims=True)
        s_send[c, 1:2] = jnp.sum(s_acc[c, 1], axis=0, keepdims=True)
        s_acc[c] = jnp.zeros_like(s_acc[c])
        for d in sum_sends(slot, c):
            d.start()

    def coefficients(slot, c, layer):
        total = s_send[c]
        for step in range(1, n_dev):
            total = total + s_recv[slot, c, step]
        s_tot[c, 0:2] = total
        t = s_tot[c]
        unit = 1
        while unit < n_group:
            place = (lane // unit) & 3
            g = t
            for d in range(1, 4):
                up = pltpu.roll(t, hc - d * unit, 1)
                down = pltpu.roll(t, (4 - d) * unit, 1)
                g = g + jnp.where(place + d < 4, up, down)
            t = g
            unit *= 4
        t = t * (1.0 / count)
        mean = t[0:1]
        inv = lax.rsqrt(t[1:2] - mean * mean + EPS)
        scale = inv * gamma[pl.ds(layer, 1), lanes[c]]
        return 0.5 * scale, 0.5 * (beta[pl.ds(layer, 1), lanes[c]] - mean * scale)

    def silu(coef, v):
        u = v * coef[0] + coef[1]
        return u + u * jnp.tanh(u)

    def put_shifted(dst, row, p, y, left, right, start):
        n, w = y.shape
        at = lax.broadcasted_iota(jnp.int32, (8, w), 0)
        before = pltpu.roll(y, 1, 0)
        after = pltpu.roll(y, n - 1, 0)
        before = jnp.concatenate([jnp.where(at == 0, left, before[0:8]), before[8:]], axis=0)
        after = jnp.concatenate([after[:n - 8], jnp.where(at == 7, right, after[n - 8:])], axis=0)
        for d, v in enumerate((before, y, after)):
            dst[row, p, :, d * chans + start:d * chans + start + w] = v.astype(BF16)

    def norm(coef, slot, row, p, c):
        v = halo[slot, row, p, :, lanes[c]] if p < 2 else vid[slot, row, p - 2, :, lanes[c]]
        y = silu(coef, v.astype(F32))
        ye = silu(coef, edge[slot, row, p, :, lanes[c]])
        put_shifted(act, row, p, y, jnp.where(h == 0, 0.0, ye), jnp.where(h == 0, ye, 0.0), c * hc)

    def norm_ext(coef, row, p, c):
        mine = silu(coef, (halo[1, row, p, :, lanes[c]] if p < 2 else vid[1, row, p - 2, :, lanes[c]]).astype(F32))
        y = silu(coef, ext[row, p, :, lanes[c]].astype(F32))
        far = silu(coef, edge2[row, p, :, lanes[c]])
        put_shifted(xact, row, p, y, jnp.where(h == 0, mine[half - 1:half], far), jnp.where(h == 0, far, mine[0:1]), c * hc)

    def dots(slot, i, js, lhs, k_half=None, n_half=None):
        cols = slice(0, chans) if n_half is None else lanes[n_half]
        total = None
        for j in js:
            if isinstance(i, int):
                di = 1 if i == j else (2 - 2 * h if i == OWN else 2 * h)
            else:
                di = jnp.where(i == OWN, 1, 2 * h)
            left, right = [], []
            for k in reversed(range(3)):
                for d in range(3):
                    for c in HALVES:
                        if k_half is None or c == k_half:
                            at = slice(d * chans + c * hc, d * chans + (c + 1) * hc)
                            v = lhs(j, k, at)
                            left.append(v.reshape(v.shape[0] * v.shape[1], v.shape[2]))
                            right.append(w_buf[slot, k, di, at, cols])
            q = jnp.dot(jnp.concatenate(left, axis=1), jnp.concatenate(right, axis=0), preferred_element_type=F32)
            total = q if total is None else total + q
        return total

    def frames_of(f0, n):
        return lambda j, k, at: act[j, pl.ds(f0 + k, n), :, at]

    def finish(layer, nslot, i, f0, p, c):
        b = bias[pl.ds(layer, 1), lanes[c]]
        t1 = t2 = None
        for f in range(p.shape[0] // half):
            v = (p[f * half:(f + 1) * half] + b).astype(BF16).astype(F32)
            if isinstance(layer, int):
                vb = v.astype(BF16)
            else:
                res = vid[0, i, f0 + f, :, lanes[c]].astype(F32)
                vb = jnp.where(nslot == 0, res + v, v).astype(BF16)
            vid[nslot, i, f0 + f, :, lanes[c]] = vb
            v = vb.astype(F32)
            t1 = fold(v) if t1 is None else t1 + fold(v)
            t2 = fold(v * v) if t2 is None else t2 + fold(v * v)
            ecol[i, f0 + f, :, lanes[c]] = jnp.where(h == 0, v[half - 1:half], v[0:1])
        s_acc[c, 0] += t1
        s_acc[c, 1] += t2

    def halo_send(slot, row, c):
        return remote(vid.at[slot, row, tail, :, lanes[c]], halo.at[slot, row, :, :, lanes[c]], hs_sem.at[row, c], hr_sem.at[slot, row, c], nxt)

    def edge_send(slot, row, c):
        return remote(ecol.at[row, :, :, lanes[c]], edge.at[slot, 1 - row, pl.ds(2, frames), :, lanes[c]], es_sem.at[row, 0, c],
                      er_sem.at[slot, 1 - row, 0, c], partner)

    def edge_diag(slot, row, c):
        return remote(ecol.at[row, tail, :, lanes[c]], edge.at[slot, 1 - row, pl.ds(0, 2), :, lanes[c]], es_sem.at[row, 1, c],
                      er_sem.at[slot, 1 - row, 1, c], diag)

    def repeat_first(slot, row, cols):
        @pl.when(r == 0)
        def _():
            for f in HALVES:
                halo[slot, row, f, :, cols] = vid[slot, row, 0, :, cols]
                edge[slot, row, f, :, cols] = edge[slot, row, 2, :, cols]

    def half_out(slot, c):
        sums_start(slot, c)
        for row in (OTH, OWN):
            edge_send(slot, row, c).start()

        @pl.when(not_last)
        def _():
            for row in (OTH, OWN):
                edge_diag(slot, row, c).start()
                halo_send(slot, row, c).start()

    def half_in(slot, c, layer):
        for d in sum_sends(slot, c):
            d.wait()
        for row in (OTH, OWN):
            edge_send(slot, row, c).wait()

        @pl.when(not_last)
        def _():
            for row in (OTH, OWN):
                edge_diag(slot, row, c).wait_send()
                halo_send(slot, row, c).wait_send()

        @pl.when(not_first)
        def _():
            for row in (OTH, OWN):
                edge_diag(slot, row, c).wait_recv()
                halo_send(slot, row, c).wait_recv()

        repeat_first(slot, OWN, lanes[c])
        repeat_first(slot, OTH, lanes[c])
        return coefficients(slot, c, layer)

    every = slice(0, chans)
    x_halo = remote(lat.at[tail, 0, my_cols, :], halo.at[0, OWN], hs_sem.at[OWN, 0], hr_sem.at[0, OWN, 0], nxt)
    x_pass = remote(vid.at[0, OTH, tail], halo.at[0, OTH], hs_sem.at[OTH, 0], hr_sem.at[0, OTH, 0], nxt)
    e_part = remote(ecol.at[OWN], edge.at[0, OTH, pl.ds(2, frames)], es_sem.at[OWN, 0, 0], er_sem.at[0, OTH, 0, 0], partner)
    e_nxt = remote(edge.at[0, OWN, pl.ds(frames, 2)], edge.at[0, OWN, pl.ds(0, 2)], es_sem.at[OTH, 1, 0], er_sem.at[0, OWN, 1, 0], nxt)
    e_diag = remote(ecol.at[OWN, tail], edge.at[0, OTH, pl.ds(0, 2)], es_sem.at[OWN, 1, 0], er_sem.at[0, OTH, 1, 0], diag)
    for c in HALVES:
        sums_start(0, c)
    e_part.start()

    @pl.when(not_last)
    def _():
        e_diag.start()
        e_nxt.start()
        x_halo.start()

    for g in (3, 2, 1, 0):
        x_piece(g).start()
    w_copy(1).start()
    load_own.wait()
    for c in small:
        c.wait()
    for c in HALVES:
        for d in sum_sends(0, c):
            d.wait()
    coef = [coefficients(0, c, 0) for c in HALVES]
    for p in range(2, frames + 2):
        for c in HALVES:
            norm(coef[c], 0, OWN, p, c)

    @pl.when(not_last)
    def _():
        x_halo.wait_send()
        e_nxt.wait_send()

    @pl.when(not_first)
    def _():
        x_halo.wait_recv()
        e_nxt.wait_recv()

    repeat_first(0, OWN, every)
    for p in range(2):
        for c in HALVES:
            norm(coef[c], 0, OWN, p, c)
    w_copy(0).wait()

    @pl.loop(0, 4)
    def _(c):
        i = c // 2
        f0 = lax.rem(c, 2) * (frames // 2)
        rows = pl.ds(pl.multiple_of(f0 * half, half), frames // 2 * half)
        acc[i, rows, :] = dots(0, i, (OWN,), frames_of(f0, frames // 2))

    e_part.wait()

    @pl.when(not_last)
    def _():
        e_diag.wait_send()

    @pl.when(not_first)
    def _():
        e_diag.wait_recv()

    def last_k(i, g, c):
        rows = pl.ds(g * per * half, per * half)
        finish(0, 1, i, g * per, acc[i, rows, lanes[c]] + dots(0, i, (OTH,), frames_of(g * per, per), n_half=c), c)

    for g in (3, 2, 1, 0):
        x_piece(g).wait()
        if g == 3:
            x_piece(4).wait()

            @pl.when(not_last)
            def _():
                x_pass.start()
        if g == 0:
            @pl.when(not_last)
            def _():
                x_pass.wait_send()

            @pl.when(not_first)
            def _():
                x_pass.wait_recv()

            repeat_first(0, OTH, every)
        for p in reversed(range(g * per, frames + 2 if g == 3 else (g + 1) * per)):
            for c in HALVES:
                norm(coef[c], 0, OTH, p, c)
        rows = pl.ds(g * per * half, per * half)
        for i in (OTH, OWN):
            if g > 1:
                p = acc[i, rows, :] + dots(0, i, (OTH,), frames_of(g * per, per))
                for c in HALVES:
                    finish(0, 1, i, g * per, p[:, lanes[c]], c)
            else:
                last_k(i, g, 0)
    half_out(1, 0)
    for g in (1, 0):
        for i in (OTH, OWN):
            last_k(i, g, 1)
    half_out(1, 1)

    def strip_send(row, c):
        return remote(vid.at[1, row, :, edge_strip, lanes[c]], ext.at[1 - row, pl.ds(2, frames), :, lanes[c]], ts_sem.at[row, 0, c],
                      tr_sem.at[1 - row, 0, c], partner)

    def strip_diag(row, c):
        return remote(vid.at[1, row, tail, edge_strip, lanes[c]], ext.at[1 - row, pl.ds(0, 2), :, lanes[c]], ts_sem.at[row, 1, c],
                      tr_sem.at[1 - row, 1, c], diag)

    def col2_send(row):
        return remote(ecol2.at[row], edge2.at[1 - row, pl.ds(2, frames)], cs_sem.at[row, 0], cr_sem.at[1 - row, 0], partner)

    def col2_diag(row):
        return remote(ecol2.at[row, tail], edge2.at[1 - row, pl.ds(0, 2)], cs_sem.at[row, 1], cr_sem.at[1 - row, 1], diag)

    def res_send():
        return remote(vid.at[0, OTH, :, edge_strip, :], xres, rs_sem.at[0], rs_sem.at[1], partner)

    def layer_body(layer, carry):
        slot = lax.rem(layer, 2)
        nslot = 1 - slot
        w_copy(layer + 1).start()

        @pl.when(layer == 2)
        def _():
            res_send().start()

        def norms(lo, hi, c):
            for row in (OWN, OTH):
                for p in reversed(range(lo, hi)):
                    norm(coef[c], slot, row, p, c)

        def first_k(i, g):
            acc[i, g * per * half:(g + 1) * per * half, :] = dots(slot, i, (OWN, OTH), frames_of(g * per, per), k_half=0)

        coef = [half_in(slot, 0, layer)]
        w_copy(layer).wait()
        norms(3 * per, frames + 2, 0)
        norms(2 * per, 3 * per, 0)
        first_k(OTH, 3)
        norms(per, 2 * per, 0)
        first_k(OTH, 2)
        norms(0, per, 0)
        first_k(OTH, 1)
        first_k(OTH, 0)
        coef.append(half_in(slot, 1, layer))
        norms(3 * per, frames + 2, 1)
        first_k(OWN, 3)
        norms(2 * per, 3 * per, 1)
        first_k(OWN, 2)
        norms(per, 2 * per, 1)
        first_k(OWN, 1)
        norms(0, per, 1)
        first_k(OWN, 0)
        for c in HALVES:
            for i in (OTH, OWN):
                for g in (3, 2, 1, 0):
                    rows = slice(g * per * half, (g + 1) * per * half)
                    p = dots(slot, i, (OWN, OTH), frames_of(g * per, per), k_half=1, n_half=c)
                    finish(layer, nslot, i, g * per, acc[i, rows, lanes[c]] + p, c)
            half_out(nslot, c)

            @pl.when(layer == 2)
            def _():
                for row in (OTH, OWN):
                    strip_send(row, c).start()

                @pl.when(not_last)
                def _():
                    for row in (OTH, OWN):
                        strip_diag(row, c).start()

        return carry

    lax.fori_loop(1, 3, layer_body, 0)

    wide = frames // 4
    pieces_out = (3, 2, 1, 0)

    def out_send(k):
        fs = pl.ds(k * wide, wide)
        dst = out.at[fs, 0, pl.ds(pl.multiple_of(h * (half + strip), strip), part), :]
        return remote(vid.at[0, OTH, fs, part_cols, :], dst, os_sem.at[k], or_sem.at[k], partner)

    def out_local():
        return pltpu.make_async_copy(vid.at[0, OWN], out.at[:, 0, my_cols, :], o_sem.at[0])

    def out_ext():
        dst = out.at[:, 0, pl.ds(pl.multiple_of(half - h * strip, strip), strip), :]
        return pltpu.make_async_copy(xres, dst, o_sem.at[1])

    def norms(lo, hi, c):
        for row in (OWN, OTH):
            for p in reversed(range(lo, hi)):
                norm(coef[c], 1, row, p, c)

    def close(res, p):
        return (res.astype(F32) + (p + bias[3:4, :]).astype(BF16).astype(F32)).astype(BF16)

    def part_dots(k, k_half):
        return dots(1, OTH, (OWN, OTH), lambda j, t, at: act[j, pl.ds(k * wide + t, wide), part_cols, at], k_half)

    def part_chunk(k):
        rows = slice(k * wide * part, (k + 1) * wide * part)
        p = acc[OTH, rows, :] + part_dots(k, 1)
        for f in range(wide):
            fr = k * wide + f
            vid[0, OTH, fr, part_cols, :] = close(vid[0, OTH, fr, part_cols, :], p[f * part:(f + 1) * part])
        out_send(k).start()

    def own_chunk(g):
        if g == 3:
            p = acc[OWN, g * per * half:(g + 1) * per * half, :] + dots(1, OWN, (OWN, OTH), frames_of(g * per, per), 1)
        else:
            p = dots(1, OWN, (OWN, OTH), frames_of(g * per, per))
        for f in range(per):
            vid[0, OWN, g * per + f] = close(vid[0, OWN, g * per + f], p[f * half:(f + 1) * half])

    coef = [half_in(1, 0, 3)]
    w_copy(3).wait()
    def norms_for(k, c):
        norms(k * wide, frames + 2 if k == 3 else (k + 1) * wide, c)

    norms_for(3, 0)
    norms_for(2, 0)
    for k in pieces_out:
        acc[OTH, k * wide * part:(k + 1) * wide * part, :] = part_dots(k, 0)
        if k > 1:
            norms_for(k - 2, 0)
    acc[OWN, 3 * per * half:4 * per * half, :] = dots(1, OWN, (OWN, OTH), frames_of(3 * per, per), 0)

    def columns2(f, carry):
        for row in (OWN, OTH):
            v = vid[1, row, f, strip:half - strip, :].astype(F32)
            ecol2[row, f] = jnp.where(h == 0, v[half - 2 * strip - 1:half - 2 * strip], v[0:1])
        return carry

    lax.fori_loop(0, frames, columns2, 0)
    for row in (OWN, OTH):
        col2_send(row).start()

    @pl.when(not_last)
    def _():
        for row in (OWN, OTH):
            col2_diag(row).start()

    coef.append(half_in(1, 1, 3))
    norms_for(3, 1)
    for k in pieces_out:
        if k > 0:
            norms_for(k - 1, 1)
        part_chunk(k)
    for row in (OWN, OTH):
        col2_send(row).wait()
        for c in HALVES:
            strip_send(row, c).wait()

    @pl.when(not_last)
    def _():
        for row in (OWN, OTH):
            col2_diag(row).wait_send()
            for c in HALVES:
                strip_diag(row, c).wait_send()

    @pl.when(not_first)
    def _():
        for row in (OWN, OTH):
            col2_diag(row).wait_recv()
            for c in HALVES:
                strip_diag(row, c).wait_recv()

    @pl.when(r == 0)
    def _():
        for row in (OWN, OTH):
            for f in HALVES:
                ext[row, f] = ext[row, 2]
                edge2[row, f] = edge2[row, 2]

    res_send().wait()
    for row in (OWN, OTH):
        for p in range(frames + 2):
            for c in HALVES:
                norm_ext(coef[c], row, p, c)
    for g in (3, 2, 1, 0):
        own_chunk(g)
    p = dots(1, OWN, (OWN, OTH), lambda j, t, at: xact[j, pl.ds(t, frames), :, at])
    out_local().start()
    for f in range(frames):
        xres[f] = close(xres[f], p[f * strip:(f + 1) * strip])
    out_ext().start()
    out_local().wait()
    out_ext().wait()
    for k in pieces_out:
        out_send(k).wait()


def solution(mesh):
    n_cp = mesh.shape["cp"]

    def local_decode(lat, conv_w, conv_b, gn_gamma, gn_beta):
        frames, _, width, chans = lat.shape
        half = width // 2
        strip = half // 4
        n_dev = 2 * n_cp
        count = frames * n_cp * 2 * width * (chans // GROUPS)
        dma = pltpu.SemaphoreType.DMA

        def pair(*more):
            return dma((2, *more))

        any_spec = pl.BlockSpec(memory_space=pl.ANY)
        return pl.pallas_call(
            functools.partial(kernel, (n_cp, frames, half, strip, chans, count)),
            out_shape=jax.ShapeDtypeStruct(lat.shape, BF16),
            in_specs=[any_spec] * 5,
            out_specs=any_spec,
            scratch_shapes=[
                pltpu.VMEM(conv_b.shape, F32),
                pltpu.VMEM(gn_gamma.shape, F32),
                pltpu.VMEM(gn_beta.shape, F32),
                pltpu.VMEM((2, 2, frames, half, chans), BF16),
                pltpu.VMEM((2, frames + 2, half, 3 * chans), BF16),
                pltpu.VMEM((2, frames * half, chans), F32),
                pltpu.VMEM((2, 3, 3, 3 * chans, chans), BF16),
                pltpu.VMEM(lat.shape, BF16),
                pltpu.VMEM((2, 2, 2, half, chans), BF16),
                pltpu.VMEM((2, 2, frames + 2, 1, chans), F32),
                pltpu.VMEM((2, frames, 1, chans), F32),
                pltpu.VMEM((2, frames + 2, strip, chans), BF16),
                pltpu.VMEM((2, frames + 2, strip, 3 * chans), BF16),
                pltpu.VMEM((2, frames + 2, 1, chans), F32),
                pltpu.VMEM((2, frames, 1, chans), F32),
                pltpu.VMEM((frames, strip, chans), BF16),
                pltpu.VMEM((2, 2, 8, chans // 2), F32),
                pltpu.VMEM((2, 8, chans // 2), F32),
                pltpu.VMEM((2, 2, chans // 2), F32),
                pltpu.VMEM((2, 2, n_dev, 2, chans // 2), F32),
                dma((8,)),
                pair(),
                dma((5,)),
                dma((5,)),
                pair(2),
                pair(2, 2),
                pair(2, 2),
                pair(2, 2, 2),
                pair(2, 2),
                pair(2, 2),
                pair(2),
                pair(2),
                pair(),
                pair(n_dev),
                pair(2, n_dev),
                pair(),
                dma((4,)),
                dma((4,)),
            ],
            compiler_params=pltpu.CompilerParams(collective_id=0, has_side_effects=True, vmem_limit_bytes=52 * 1024 * 1024),
            name="decode",
        )(*(pltpu.with_memory_space_constraint(a, pltpu.HBM) for a in (lat, conv_w.reshape(4, 3, 3, 3 * chans, chans), conv_b, gn_gamma, gn_beta)))

    spec = P(("dp", "cp"), "hp", None, None)
    return jax.shard_map(local_decode, mesh=mesh, in_specs=(spec, P(), P(), P(), P()), out_specs=spec, check_vma=False)
```

```python
import functools

import jax
import jax.numpy as jnp
from jax import lax
from jax.experimental import pallas as pl
from jax.experimental.pallas import tpu as pltpu
from jax.sharding import PartitionSpec as P

GROUPS = 32
EPS = 1e-6
MESH = pl.DeviceIdType.MESH
F32 = jnp.float32
BF16 = jnp.bfloat16
HALVES = OWN, OTH = 0, 1


def kernel(dims, lat, w_hbm, bias_hbm, gamma_hbm, beta_hbm, out, bias, gamma, beta, vid, act, acc, w_buf, x_in, halo, edge, ecol, ext, xact, edge2, ecol2, xres,
           s_acc, s_tot, s_send, s_recv, l_sem, w_sem, xs_sem, xr_sem, hs_sem, hr_sem, es_sem, er_sem, ts_sem, tr_sem, cs_sem, cr_sem,
           rs_sem, ss_sem, sr_sem, o_sem, os_sem, or_sem):
    n_cp, frames, half, strip, chans, count = dims
    n_dev = 2 * n_cp
    per = frames // 4
    h = lax.axis_index("hp")
    r = lax.axis_index("cp")
    me = h * n_cp + r
    partner = {"hp": 1 - h, "cp": r}
    nxt = {"hp": h, "cp": lax.rem(r + 1, n_cp)}
    diag = {"hp": 1 - h, "cp": lax.rem(r + 1, n_cp)}
    not_last = r < n_cp - 1
    not_first = r > 0
    tail = pl.ds(frames - 2, 2)
    my_cols = pl.ds(pl.multiple_of(h * half, half), half)
    ot_cols = pl.ds(pl.multiple_of((1 - h) * half, half), half)
    hc = chans // 2
    lanes = [slice(c * hc, (c + 1) * hc) for c in HALVES]
    part = half - strip
    part_cols = pl.ds(pl.multiple_of(h * strip, strip), part)
    edge_strip = pl.ds(pl.multiple_of((1 - h) * part, strip), strip)

    def remote(src, dst, send, recv, dev):
        return pltpu.make_async_remote_copy(src_ref=src, dst_ref=dst, send_sem=send, recv_sem=recv, device_id=dev, device_id_type=MESH)

    def peer(step):
        t = lax.rem(me + step, n_dev)
        return {"hp": t // n_cp, "cp": lax.rem(t, n_cp)}

    def load_x(k):
        fs = pl.ds(k * per, per)
        return pltpu.make_async_copy(lat.at[fs], x_in.at[fs], l_sem.at[k])

    for k in range(4):
        load_x(k).start()
    small = [pltpu.make_async_copy(a, b, l_sem.at[4 + k]) for k, (a, b) in enumerate([(bias_hbm, bias), (gamma_hbm, gamma), (beta_hbm, beta)])]
    load_own = pltpu.make_async_copy(lat.at[:, 0, my_cols, :], vid.at[0, OWN], l_sem.at[7])

    def w_copy(layer):
        slot = lax.rem(layer, 2)
        return pltpu.make_async_copy(w_hbm.at[layer], w_buf.at[slot], w_sem.at[slot])

    barrier = pltpu.get_barrier_semaphore()
    for step in range(1, n_dev):
        pl.semaphore_signal(barrier, inc=1, device_id=peer(step), device_id_type=MESH)
    for c in small:
        c.start()
    load_own.start()
    w_copy(0).start()

    def fold(v):
        t = v[0:8]
        for k in range(1, v.shape[0] // 8):
            t = t + v[8 * k:8 * k + 8]
        return t

    s_acc[...] = jnp.zeros_like(s_acc)
    s_tot[...] = jnp.zeros_like(s_tot)

    def first_sums(f, carry):
        v = x_in[f, 0].astype(F32)
        for c in HALVES:
            s_acc[c, 0] += fold(v[:, lanes[c]])
            s_acc[c, 1] += fold(v[:, lanes[c]] * v[:, lanes[c]])
        lo, hi = v[half - 1:half], v[half:half + 1]
        ecol[OWN, f] = jnp.where(h == 0, lo, hi)
        edge[0, OWN, f + 2] = jnp.where(h == 0, hi, lo)
        return carry

    starts = (0, 1, 1 + per, 1 + 2 * per, frames - 1, frames)

    def x_piece(g):
        fs = pl.ds(starts[g], starts[g + 1] - starts[g])
        return remote(lat.at[fs, 0, ot_cols, :], vid.at[0, OTH, fs], xs_sem.at[g], xr_sem.at[g], partner)

    for k in range(4):
        load_x(k).wait()
        if k == 1:
            pl.semaphore_wait(barrier, n_dev - 1)
            x_piece(4).start()
        lax.fori_loop(k * per, (k + 1) * per, first_sums, 0)

    lane = lax.broadcasted_iota(jnp.int32, (8, hc), 1)
    n_group = chans // GROUPS

    def sum_sends(slot, c):
        return [remote(s_send.at[c], s_recv.at[slot, c, step], ss_sem.at[c, step], sr_sem.at[slot, c, step], peer(step)) for step in range(1, n_dev)]

    def sums_start(slot, c):
        s_send[c, 0:1] = jnp.sum(s_acc[c, 0], axis=0, keepdims=True)
        s_send[c, 1:2] = jnp.sum(s_acc[c, 1], axis=0, keepdims=True)
        s_acc[c] = jnp.zeros_like(s_acc[c])
        for d in sum_sends(slot, c):
            d.start()

    def coefficients(slot, c, layer):
        total = s_send[c]
        for step in range(1, n_dev):
            total = total + s_recv[slot, c, step]
        s_tot[c, 0:2] = total
        t = s_tot[c]
        unit = 1
        while unit < n_group:
            place = (lane // unit) & 3
            g = t
            for d in range(1, 4):
                up = pltpu.roll(t, hc - d * unit, 1)
                down = pltpu.roll(t, (4 - d) * unit, 1)
                g = g + jnp.where(place + d < 4, up, down)
            t = g
            unit *= 4
        t = t * (1.0 / count)
        mean = t[0:1]
        inv = lax.rsqrt(t[1:2] - mean * mean + EPS)
        scale = inv * gamma[pl.ds(layer, 1), lanes[c]]
        return 0.5 * scale, 0.5 * (beta[pl.ds(layer, 1), lanes[c]] - mean * scale)

    def silu(coef, v):
        u = v * coef[0] + coef[1]
        return u + u * jnp.tanh(u)

    def put_shifted(dst, row, p, y, left, right, start):
        n, w = y.shape
        at = lax.broadcasted_iota(jnp.int32, (8, w), 0)
        before = pltpu.roll(y, 1, 0)
        after = pltpu.roll(y, n - 1, 0)
        before = jnp.concatenate([jnp.where(at == 0, left, before[0:8]), before[8:]], axis=0)
        after = jnp.concatenate([after[:n - 8], jnp.where(at == 7, right, after[n - 8:])], axis=0)
        for d, v in enumerate((before, y, after)):
            dst[row, p, :, d * chans + start:d * chans + start + w] = v.astype(BF16)

    def norm(coef, slot, row, p, c):
        v = halo[slot, row, p, :, lanes[c]] if p < 2 else vid[slot, row, p - 2, :, lanes[c]]
        y = silu(coef, v.astype(F32))
        ye = silu(coef, edge[slot, row, p, :, lanes[c]])
        put_shifted(act, row, p, y, jnp.where(h == 0, 0.0, ye), jnp.where(h == 0, ye, 0.0), c * hc)

    def norm_ext(coef, row, p, c):
        mine = silu(coef, (halo[1, row, p, :, lanes[c]] if p < 2 else vid[1, row, p - 2, :, lanes[c]]).astype(F32))
        y = silu(coef, ext[row, p, :, lanes[c]].astype(F32))
        far = silu(coef, edge2[row, p, :, lanes[c]])
        put_shifted(xact, row, p, y, jnp.where(h == 0, mine[half - 1:half], far), jnp.where(h == 0, far, mine[0:1]), c * hc)

    def dots(slot, i, js, lhs, k_half=None, n_half=None):
        cols = slice(0, chans) if n_half is None else lanes[n_half]
        total = None
        for j in js:
            if isinstance(i, int):
                di = 1 if i == j else (2 - 2 * h if i == OWN else 2 * h)
            else:
                di = jnp.where(i == OWN, 1, 2 * h)
            left, right = [], []
            for k in reversed(range(3)):
                for d in range(3):
                    for c in HALVES:
                        if k_half is None or c == k_half:
                            at = slice(d * chans + c * hc, d * chans + (c + 1) * hc)
                            v = lhs(j, k, at)
                            left.append(v.reshape(v.shape[0] * v.shape[1], v.shape[2]))
                            right.append(w_buf[slot, k, di, at, cols])
            q = jnp.dot(jnp.concatenate(left, axis=1), jnp.concatenate(right, axis=0), preferred_element_type=F32)
            total = q if total is None else total + q
        return total

    def frames_of(f0, n):
        return lambda j, k, at: act[j, pl.ds(f0 + k, n), :, at]

    def finish(layer, nslot, i, f0, p, c):
        b = bias[pl.ds(layer, 1), lanes[c]]
        t1 = t2 = None
        for f in range(p.shape[0] // half):
            v = (p[f * half:(f + 1) * half] + b).astype(BF16).astype(F32)
            if isinstance(layer, int):
                vb = v.astype(BF16)
            else:
                res = vid[0, i, f0 + f, :, lanes[c]].astype(F32)
                vb = jnp.where(nslot == 0, res + v, v).astype(BF16)
            vid[nslot, i, f0 + f, :, lanes[c]] = vb
            v = vb.astype(F32)
            t1 = fold(v) if t1 is None else t1 + fold(v)
            t2 = fold(v * v) if t2 is None else t2 + fold(v * v)
            ecol[i, f0 + f, :, lanes[c]] = jnp.where(h == 0, v[half - 1:half], v[0:1])
        s_acc[c, 0] += t1
        s_acc[c, 1] += t2

    def halo_send(slot, row, c):
        return remote(vid.at[slot, row, tail, :, lanes[c]], halo.at[slot, row, :, :, lanes[c]], hs_sem.at[row, c], hr_sem.at[slot, row, c], nxt)

    def edge_send(slot, row, c):
        return remote(ecol.at[row, :, :, lanes[c]], edge.at[slot, 1 - row, pl.ds(2, frames), :, lanes[c]], es_sem.at[row, 0, c],
                      er_sem.at[slot, 1 - row, 0, c], partner)

    def edge_diag(slot, row, c):
        return remote(ecol.at[row, tail, :, lanes[c]], edge.at[slot, 1 - row, pl.ds(0, 2), :, lanes[c]], es_sem.at[row, 1, c],
                      er_sem.at[slot, 1 - row, 1, c], diag)

    def repeat_first(slot, row, cols):
        @pl.when(r == 0)
        def _():
            for f in HALVES:
                halo[slot, row, f, :, cols] = vid[slot, row, 0, :, cols]
                edge[slot, row, f, :, cols] = edge[slot, row, 2, :, cols]

    def half_out(slot, c):
        sums_start(slot, c)
        for row in (OTH, OWN):
            edge_send(slot, row, c).start()

        @pl.when(not_last)
        def _():
            for row in (OTH, OWN):
                edge_diag(slot, row, c).start()
                halo_send(slot, row, c).start()

    def half_in(slot, c, layer):
        for d in sum_sends(slot, c):
            d.wait()
        for row in (OTH, OWN):
            edge_send(slot, row, c).wait()

        @pl.when(not_last)
        def _():
            for row in (OTH, OWN):
                edge_diag(slot, row, c).wait_send()
                halo_send(slot, row, c).wait_send()

        @pl.when(not_first)
        def _():
            for row in (OTH, OWN):
                edge_diag(slot, row, c).wait_recv()
                halo_send(slot, row, c).wait_recv()

        repeat_first(slot, OWN, lanes[c])
        repeat_first(slot, OTH, lanes[c])
        return coefficients(slot, c, layer)

    every = slice(0, chans)
    x_halo = remote(lat.at[tail, 0, my_cols, :], halo.at[0, OWN], hs_sem.at[OWN, 0], hr_sem.at[0, OWN, 0], nxt)
    x_pass = remote(vid.at[0, OTH, tail], halo.at[0, OTH], hs_sem.at[OTH, 0], hr_sem.at[0, OTH, 0], nxt)
    e_part = remote(ecol.at[OWN], edge.at[0, OTH, pl.ds(2, frames)], es_sem.at[OWN, 0, 0], er_sem.at[0, OTH, 0, 0], partner)
    e_nxt = remote(edge.at[0, OWN, pl.ds(frames, 2)], edge.at[0, OWN, pl.ds(0, 2)], es_sem.at[OTH, 1, 0], er_sem.at[0, OWN, 1, 0], nxt)
    e_diag = remote(ecol.at[OWN, tail], edge.at[0, OTH, pl.ds(0, 2)], es_sem.at[OWN, 1, 0], er_sem.at[0, OTH, 1, 0], diag)
    for c in HALVES:
        sums_start(0, c)
    e_part.start()

    @pl.when(not_last)
    def _():
        e_diag.start()
        e_nxt.start()
        x_halo.start()

    for g in (3, 2, 1, 0):
        x_piece(g).start()
    w_copy(1).start()
    load_own.wait()
    for c in small:
        c.wait()
    for c in HALVES:
        for d in sum_sends(0, c):
            d.wait()
    coef = [coefficients(0, c, 0) for c in HALVES]
    for p in range(2, frames + 2):
        for c in HALVES:
            norm(coef[c], 0, OWN, p, c)

    @pl.when(not_last)
    def _():
        x_halo.wait_send()
        e_nxt.wait_send()

    @pl.when(not_first)
    def _():
        x_halo.wait_recv()
        e_nxt.wait_recv()

    repeat_first(0, OWN, every)
    for p in range(2):
        for c in HALVES:
            norm(coef[c], 0, OWN, p, c)
    w_copy(0).wait()

    @pl.loop(0, 4)
    def _(c):
        i = c // 2
        f0 = lax.rem(c, 2) * (frames // 2)
        rows = pl.ds(pl.multiple_of(f0 * half, half), frames // 2 * half)
        acc[i, rows, :] = dots(0, i, (OWN,), frames_of(f0, frames // 2))

    e_part.wait()

    @pl.when(not_last)
    def _():
        e_diag.wait_send()

    @pl.when(not_first)
    def _():
        e_diag.wait_recv()

    def last_k(i, g, c):
        rows = pl.ds(g * per * half, per * half)
        finish(0, 1, i, g * per, acc[i, rows, lanes[c]] + dots(0, i, (OTH,), frames_of(g * per, per), n_half=c), c)

    for g in (3, 2, 1, 0):
        x_piece(g).wait()
        if g == 3:
            x_piece(4).wait()

            @pl.when(not_last)
            def _():
                x_pass.start()
        if g == 0:
            @pl.when(not_last)
            def _():
                x_pass.wait_send()

            @pl.when(not_first)
            def _():
                x_pass.wait_recv()

            repeat_first(0, OTH, every)
        for p in reversed(range(g * per, frames + 2 if g == 3 else (g + 1) * per)):
            for c in HALVES:
                norm(coef[c], 0, OTH, p, c)
        rows = pl.ds(g * per * half, per * half)
        for i in (OTH, OWN):
            if g > 1:
                p = acc[i, rows, :] + dots(0, i, (OTH,), frames_of(g * per, per))
                for c in HALVES:
                    finish(0, 1, i, g * per, p[:, lanes[c]], c)
            else:
                last_k(i, g, 0)
    half_out(1, 0)
    for g in (1, 0):
        for i in (OTH, OWN):
            last_k(i, g, 1)
    half_out(1, 1)

    def strip_send(row, c):
        return remote(vid.at[1, row, :, edge_strip, lanes[c]], ext.at[1 - row, pl.ds(2, frames), :, lanes[c]], ts_sem.at[row, 0, c],
                      tr_sem.at[1 - row, 0, c], partner)

    def strip_pass(row):
        return remote(ext.at[row, pl.ds(frames, 2)], ext.at[row, pl.ds(0, 2)], ts_sem.at[row, 1, 0], tr_sem.at[row, 1, 0], nxt)

    def col2_send(row):
        return remote(ecol2.at[row], edge2.at[1 - row, pl.ds(2, frames)], cs_sem.at[row, 0], cr_sem.at[1 - row, 0], partner)

    def col2_diag(row):
        return remote(ecol2.at[row, tail], edge2.at[1 - row, pl.ds(0, 2)], cs_sem.at[row, 1], cr_sem.at[1 - row, 1], diag)

    def res_send():
        return remote(vid.at[0, OTH, :, edge_strip, :], xres, rs_sem.at[0], rs_sem.at[1], partner)

    def layer_body(layer, carry):
        slot = lax.rem(layer, 2)
        nslot = 1 - slot
        w_copy(layer + 1).start()

        @pl.when(layer == 2)
        def _():
            res_send().start()

        def norms(lo, hi, c):
            for row in (OWN, OTH):
                for p in reversed(range(lo, hi)):
                    norm(coef[c], slot, row, p, c)

        def first_k(i, g):
            acc[i, g * per * half:(g + 1) * per * half, :] = dots(slot, i, (OWN, OTH), frames_of(g * per, per), k_half=0)

        coef = [half_in(slot, 0, layer)]
        w_copy(layer).wait()
        norms(3 * per, frames + 2, 0)
        norms(2 * per, 3 * per, 0)
        first_k(OTH, 3)
        norms(per, 2 * per, 0)
        first_k(OTH, 2)
        norms(0, per, 0)
        first_k(OTH, 1)
        first_k(OTH, 0)
        coef.append(half_in(slot, 1, layer))
        norms(3 * per, frames + 2, 1)
        first_k(OWN, 3)
        norms(2 * per, 3 * per, 1)
        first_k(OWN, 2)
        norms(per, 2 * per, 1)
        first_k(OWN, 1)
        norms(0, per, 1)
        first_k(OWN, 0)
        for c in HALVES:
            for i in (OTH, OWN):
                for g in (3, 2, 1, 0):
                    rows = slice(g * per * half, (g + 1) * per * half)
                    p = dots(slot, i, (OWN, OTH), frames_of(g * per, per), k_half=1, n_half=c)
                    finish(layer, nslot, i, g * per, acc[i, rows, lanes[c]] + p, c)
            half_out(nslot, c)

            @pl.when(layer == 2)
            def _():
                for row in (OTH, OWN):
                    strip_send(row, c).start()

        return carry

    lax.fori_loop(1, 3, layer_body, 0)

    wide = frames // 4
    pieces_out = (3, 2, 1, 0)

    def out_send(k):
        fs = pl.ds(k * wide, wide)
        dst = out.at[fs, 0, pl.ds(pl.multiple_of(h * (half + strip), strip), part), :]
        return remote(vid.at[0, OTH, fs, part_cols, :], dst, os_sem.at[k], or_sem.at[k], partner)

    def out_local():
        return pltpu.make_async_copy(vid.at[0, OWN], out.at[:, 0, my_cols, :], o_sem.at[0])

    def out_ext():
        dst = out.at[:, 0, pl.ds(pl.multiple_of(half - h * strip, strip), strip), :]
        return pltpu.make_async_copy(xres, dst, o_sem.at[1])

    def norms(lo, hi, c):
        for row in (OWN, OTH):
            for p in reversed(range(lo, hi)):
                norm(coef[c], 1, row, p, c)

    def close(res, p):
        return (res.astype(F32) + (p + bias[3:4, :]).astype(BF16).astype(F32)).astype(BF16)

    def part_dots(k, k_half):
        return dots(1, OTH, (OWN, OTH), lambda j, t, at: act[j, pl.ds(k * wide + t, wide), part_cols, at], k_half)

    def part_chunk(k):
        rows = slice(k * wide * part, (k + 1) * wide * part)
        p = acc[OTH, rows, :] + part_dots(k, 1)
        for f in range(wide):
            fr = k * wide + f
            vid[0, OTH, fr, part_cols, :] = close(vid[0, OTH, fr, part_cols, :], p[f * part:(f + 1) * part])
        out_send(k).start()

    def own_chunk(g):
        if g == 3:
            p = acc[OWN, g * per * half:(g + 1) * per * half, :] + dots(1, OWN, (OWN, OTH), frames_of(g * per, per), 1)
        else:
            p = dots(1, OWN, (OWN, OTH), frames_of(g * per, per))
        for f in range(per):
            vid[0, OWN, g * per + f] = close(vid[0, OWN, g * per + f], p[f * half:(f + 1) * half])

    coef = [half_in(1, 0, 3)]
    w_copy(3).wait()
    def norms_for(k, c):
        norms(k * wide, frames + 2 if k == 3 else (k + 1) * wide, c)

    norms_for(3, 0)
    norms_for(2, 0)
    for k in pieces_out:
        acc[OTH, k * wide * part:(k + 1) * wide * part, :] = part_dots(k, 0)
        if k > 1:
            norms_for(k - 2, 0)
    acc[OWN, 3 * per * half:4 * per * half, :] = dots(1, OWN, (OWN, OTH), frames_of(3 * per, per), 0)

    def columns2(f, carry):
        for row in (OWN, OTH):
            v = vid[1, row, f, strip:half - strip, :].astype(F32)
            ecol2[row, f] = jnp.where(h == 0, v[half - 2 * strip - 1:half - 2 * strip], v[0:1])
        return carry

    lax.fori_loop(0, frames, columns2, 0)
    for row in (OWN, OTH):
        col2_send(row).start()

    @pl.when(not_last)
    def _():
        for row in (OWN, OTH):
            col2_diag(row).start()

    coef.append(half_in(1, 1, 3))
    norms_for(3, 1)
    for k in pieces_out:
        if k > 0:
            norms_for(k - 1, 1)
        part_chunk(k)
    for row in (OWN, OTH):
        col2_send(row).wait()
        for c in HALVES:
            strip_send(row, c).wait()

    @pl.when(not_last)
    def _():
        for row in (OWN, OTH):
            col2_diag(row).wait_send()
            strip_pass(row).start()

    @pl.when(not_first)
    def _():
        for row in (OWN, OTH):
            col2_diag(row).wait_recv()

    @pl.when(r == 0)
    def _():
        for row in (OWN, OTH):
            for f in HALVES:
                ext[row, f] = ext[row, 2]
                edge2[row, f] = edge2[row, 2]

    res_send().wait()
    for row in (OWN, OTH):
        for p in range(2, frames + 2):
            for c in HALVES:
                norm_ext(coef[c], row, p, c)
    for g in (3, 2, 1, 0):
        own_chunk(g)
    out_local().start()

    @pl.when(not_last)
    def _():
        for row in (OWN, OTH):
            strip_pass(row).wait_send()

    @pl.when(not_first)
    def _():
        for row in (OWN, OTH):
            strip_pass(row).wait_recv()

    for row in (OWN, OTH):
        for p in HALVES:
            for c in HALVES:
                norm_ext(coef[c], row, p, c)
    p = dots(1, OWN, (OWN, OTH), lambda j, t, at: xact[j, pl.ds(t, frames), :, at])
    for f in range(frames):
        xres[f] = close(xres[f], p[f * strip:(f + 1) * strip])
    out_ext().start()
    out_local().wait()
    out_ext().wait()
    for k in pieces_out:
        out_send(k).wait()


def solution(mesh):
    n_cp = mesh.shape["cp"]

    def local_decode(lat, conv_w, conv_b, gn_gamma, gn_beta):
        frames, _, width, chans = lat.shape
        half = width // 2
        strip = half // 4
        n_dev = 2 * n_cp
        count = frames * n_cp * 2 * width * (chans // GROUPS)
        dma = pltpu.SemaphoreType.DMA

        def pair(*more):
            return dma((2, *more))

        any_spec = pl.BlockSpec(memory_space=pl.ANY)
        return pl.pallas_call(
            functools.partial(kernel, (n_cp, frames, half, strip, chans, count)),
            out_shape=jax.ShapeDtypeStruct(lat.shape, BF16),
            in_specs=[any_spec] * 5,
            out_specs=any_spec,
            scratch_shapes=[
                pltpu.VMEM(conv_b.shape, F32),
                pltpu.VMEM(gn_gamma.shape, F32),
                pltpu.VMEM(gn_beta.shape, F32),
                pltpu.VMEM((2, 2, frames, half, chans), BF16),
                pltpu.VMEM((2, frames + 2, half, 3 * chans), BF16),
                pltpu.VMEM((2, frames * half, chans), F32),
                pltpu.VMEM((2, 3, 3, 3 * chans, chans), BF16),
                pltpu.VMEM(lat.shape, BF16),
                pltpu.VMEM((2, 2, 2, half, chans), BF16),
                pltpu.VMEM((2, 2, frames + 2, 1, chans), F32),
                pltpu.VMEM((2, frames, 1, chans), F32),
                pltpu.VMEM((2, frames + 2, strip, chans), BF16),
                pltpu.VMEM((2, frames + 2, strip, 3 * chans), BF16),
                pltpu.VMEM((2, frames + 2, 1, chans), F32),
                pltpu.VMEM((2, frames, 1, chans), F32),
                pltpu.VMEM((frames, strip, chans), BF16),
                pltpu.VMEM((2, 2, 8, chans // 2), F32),
                pltpu.VMEM((2, 8, chans // 2), F32),
                pltpu.VMEM((2, 2, chans // 2), F32),
                pltpu.VMEM((2, 2, n_dev, 2, chans // 2), F32),
                dma((8,)),
                pair(),
                dma((5,)),
                dma((5,)),
                pair(2),
                pair(2, 2),
                pair(2, 2),
                pair(2, 2, 2),
                pair(2, 2),
                pair(2, 2),
                pair(2),
                pair(2),
                pair(),
                pair(n_dev),
                pair(2, n_dev),
                pair(),
                dma((4,)),
                dma((4,)),
            ],
            compiler_params=pltpu.CompilerParams(collective_id=0, has_side_effects=True, vmem_limit_bytes=52 * 1024 * 1024),
            name="decode",
        )(*(pltpu.with_memory_space_constraint(a, pltpu.HBM) for a in (lat, conv_w.reshape(4, 3, 3, 3 * chans, chans), conv_b, gn_gamma, gn_beta)))

    spec = P(("dp", "cp"), "hp", None, None)
    return jax.shard_map(local_decode, mesh=mesh, in_specs=(spec, P(), P(), P(), P()), out_specs=spec, check_vma=False)
```

```python
import functools

import jax
import jax.numpy as jnp
from jax import lax
from jax.experimental import pallas as pl
from jax.experimental.pallas import tpu as pltpu
from jax.sharding import PartitionSpec as P

GROUPS = 32
EPS = 1e-6
MESH = pl.DeviceIdType.MESH
F32 = jnp.float32
BF16 = jnp.bfloat16
HALVES = OWN, OTH = 0, 1


def kernel(dims, lat, w_hbm, bias_hbm, gamma_hbm, beta_hbm, out, bias, gamma, beta, vid, act, acc, w_buf, x_in, halo, edge, ecol, ext, xact, edge2, ecol2, xres,
           s_acc, s_tot, s_send, s_recv, l_sem, w_sem, xs_sem, xr_sem, hs_sem, hr_sem, es_sem, er_sem, ts_sem, tr_sem, cs_sem, cr_sem,
           rs_sem, ss_sem, sr_sem, o_sem, os_sem, or_sem):
    n_cp, frames, half, strip, chans, count = dims
    n_dev = 2 * n_cp
    per = frames // 4
    h = lax.axis_index("hp")
    r = lax.axis_index("cp")
    me = h * n_cp + r
    partner = {"hp": 1 - h, "cp": r}
    nxt = {"hp": h, "cp": lax.rem(r + 1, n_cp)}
    diag = {"hp": 1 - h, "cp": lax.rem(r + 1, n_cp)}
    not_last = r < n_cp - 1
    not_first = r > 0
    tail = pl.ds(frames - 2, 2)
    my_cols = pl.ds(pl.multiple_of(h * half, half), half)
    ot_cols = pl.ds(pl.multiple_of((1 - h) * half, half), half)
    hc = chans // 2
    lanes = [slice(c * hc, (c + 1) * hc) for c in HALVES]
    part = half - strip
    part_cols = pl.ds(pl.multiple_of(h * strip, strip), part)
    edge_strip = pl.ds(pl.multiple_of((1 - h) * part, strip), strip)

    def remote(src, dst, send, recv, dev):
        return pltpu.make_async_remote_copy(src_ref=src, dst_ref=dst, send_sem=send, recv_sem=recv, device_id=dev, device_id_type=MESH)

    def peer(step):
        t = lax.rem(me + step, n_dev)
        return {"hp": t // n_cp, "cp": lax.rem(t, n_cp)}

    def load_x(k):
        fs = pl.ds(k * per, per)
        return pltpu.make_async_copy(lat.at[fs], x_in.at[fs], l_sem.at[k])

    for k in range(4):
        load_x(k).start()
    small = [pltpu.make_async_copy(a, b, l_sem.at[4 + k]) for k, (a, b) in enumerate([(bias_hbm, bias), (gamma_hbm, gamma), (beta_hbm, beta)])]
    load_own = pltpu.make_async_copy(lat.at[:, 0, my_cols, :], vid.at[0, OWN], l_sem.at[7])

    def w_copy(layer):
        slot = lax.rem(layer, 2)
        return pltpu.make_async_copy(w_hbm.at[layer], w_buf.at[slot], w_sem.at[slot])

    def w_first(d, k):
        return pltpu.make_async_copy(w_hbm.at[0, :, d], w_buf.at[0, :, d], w_sem.at[k])

    w_mid, w_rest = w_first(1, 0), (w_first(0, 2), w_first(2, 3))
    barrier = pltpu.get_barrier_semaphore()
    for step in range(1, n_dev):
        pl.semaphore_signal(barrier, inc=1, device_id=peer(step), device_id_type=MESH)
    for c in small:
        c.start()
    load_own.start()
    w_mid.start()

    def fold(v):
        t = v[0:8]
        for k in range(1, v.shape[0] // 8):
            t = t + v[8 * k:8 * k + 8]
        return t

    s_acc[...] = jnp.zeros_like(s_acc)
    s_tot[...] = jnp.zeros_like(s_tot)

    def first_sums(f, carry):
        v = x_in[f, 0].astype(F32)
        for c in HALVES:
            s_acc[c, 0] += fold(v[:, lanes[c]])
            s_acc[c, 1] += fold(v[:, lanes[c]] * v[:, lanes[c]])
        lo, hi = v[half - 1:half], v[half:half + 1]
        ecol[OWN, f] = jnp.where(h == 0, lo, hi)
        edge[0, OWN, f + 2] = jnp.where(h == 0, hi, lo)
        return carry

    starts = (0, 1, 1 + per, 1 + 2 * per, frames - 1, frames)

    def x_piece(g):
        fs = pl.ds(starts[g], starts[g + 1] - starts[g])
        return remote(lat.at[fs, 0, ot_cols, :], vid.at[0, OTH, fs], xs_sem.at[g], xr_sem.at[g], partner)

    for k in range(4):
        load_x(k).wait()
        if k == 1:
            pl.semaphore_wait(barrier, n_dev - 1)
            x_piece(4).start()
        lax.fori_loop(k * per, (k + 1) * per, first_sums, 0)

    lane = lax.broadcasted_iota(jnp.int32, (8, hc), 1)
    n_group = chans // GROUPS

    def sum_sends(slot, c):
        return [remote(s_send.at[c], s_recv.at[slot, c, step], ss_sem.at[c, step], sr_sem.at[slot, c, step], peer(step)) for step in range(1, n_dev)]

    def sums_start(slot, c):
        s_send[c, 0:1] = jnp.sum(s_acc[c, 0], axis=0, keepdims=True)
        s_send[c, 1:2] = jnp.sum(s_acc[c, 1], axis=0, keepdims=True)
        s_acc[c] = jnp.zeros_like(s_acc[c])
        for d in sum_sends(slot, c):
            d.start()

    def coefficients(slot, c, layer):
        total = s_send[c]
        for step in range(1, n_dev):
            total = total + s_recv[slot, c, step]
        s_tot[c, 0:2] = total
        t = s_tot[c]
        unit = 1
        while unit < n_group:
            place = (lane // unit) & 3
            g = t
            for d in range(1, 4):
                up = pltpu.roll(t, hc - d * unit, 1)
                down = pltpu.roll(t, (4 - d) * unit, 1)
                g = g + jnp.where(place + d < 4, up, down)
            t = g
            unit *= 4
        t = t * (1.0 / count)
        mean = t[0:1]
        inv = lax.rsqrt(t[1:2] - mean * mean + EPS)
        scale = inv * gamma[pl.ds(layer, 1), lanes[c]]
        return 0.5 * scale, 0.5 * (beta[pl.ds(layer, 1), lanes[c]] - mean * scale)

    def silu(coef, v):
        u = v * coef[0] + coef[1]
        return u + u * jnp.tanh(u)

    def put_shifted(dst, row, p, y, left, right, start):
        n, w = y.shape
        at = lax.broadcasted_iota(jnp.int32, (8, w), 0)
        before = pltpu.roll(y, 1, 0)
        after = pltpu.roll(y, n - 1, 0)
        before = jnp.concatenate([jnp.where(at == 0, left, before[0:8]), before[8:]], axis=0)
        after = jnp.concatenate([after[:n - 8], jnp.where(at == 7, right, after[n - 8:])], axis=0)
        for d, v in enumerate((before, y, after)):
            dst[row, p, :, d * chans + start:d * chans + start + w] = v.astype(BF16)

    def norm(coef, slot, row, p, c):
        v = halo[slot, row, p, :, lanes[c]] if p < 2 else vid[slot, row, p - 2, :, lanes[c]]
        y = silu(coef, v.astype(F32))
        ye = silu(coef, edge[slot, row, p, :, lanes[c]])
        put_shifted(act, row, p, y, jnp.where(h == 0, 0.0, ye), jnp.where(h == 0, ye, 0.0), c * hc)

    def norm_ext(coef, row, p, c):
        mine = silu(coef, (halo[1, row, p, :, lanes[c]] if p < 2 else vid[1, row, p - 2, :, lanes[c]]).astype(F32))
        y = silu(coef, ext[row, p, :, lanes[c]].astype(F32))
        far = silu(coef, edge2[row, p, :, lanes[c]])
        put_shifted(xact, row, p, y, jnp.where(h == 0, mine[half - 1:half], far), jnp.where(h == 0, far, mine[0:1]), c * hc)

    def dots(slot, i, js, lhs, k_half=None, n_half=None):
        cols = slice(0, chans) if n_half is None else lanes[n_half]
        total = None
        for j in js:
            if isinstance(i, int):
                di = 1 if i == j else (2 - 2 * h if i == OWN else 2 * h)
            else:
                di = jnp.where(i == OWN, 1, 2 * h)
            left, right = [], []
            for k in reversed(range(3)):
                for d in range(3):
                    for c in HALVES:
                        if k_half is None or c == k_half:
                            at = slice(d * chans + c * hc, d * chans + (c + 1) * hc)
                            v = lhs(j, k, at)
                            left.append(v.reshape(v.shape[0] * v.shape[1], v.shape[2]))
                            right.append(w_buf[slot, k, di, at, cols])
            q = jnp.dot(jnp.concatenate(left, axis=1), jnp.concatenate(right, axis=0), preferred_element_type=F32)
            total = q if total is None else total + q
        return total

    def frames_of(f0, n):
        return lambda j, k, at: act[j, pl.ds(f0 + k, n), :, at]

    def finish(layer, nslot, i, f0, p, c):
        b = bias[pl.ds(layer, 1), lanes[c]]
        t1 = t2 = None
        for f in range(p.shape[0] // half):
            v = (p[f * half:(f + 1) * half] + b).astype(BF16).astype(F32)
            if isinstance(layer, int):
                vb = v.astype(BF16)
            else:
                res = vid[0, i, f0 + f, :, lanes[c]].astype(F32)
                vb = jnp.where(nslot == 0, res + v, v).astype(BF16)
            vid[nslot, i, f0 + f, :, lanes[c]] = vb
            v = vb.astype(F32)
            t1 = fold(v) if t1 is None else t1 + fold(v)
            t2 = fold(v * v) if t2 is None else t2 + fold(v * v)
            ecol[i, f0 + f, :, lanes[c]] = jnp.where(h == 0, v[half - 1:half], v[0:1])
        s_acc[c, 0] += t1
        s_acc[c, 1] += t2

    def halo_send(slot, row, c):
        return remote(vid.at[slot, row, tail, :, lanes[c]], halo.at[slot, row, :, :, lanes[c]], hs_sem.at[row, c], hr_sem.at[slot, row, c], nxt)

    def edge_send(slot, row, c):
        return remote(ecol.at[row, :, :, lanes[c]], edge.at[slot, 1 - row, pl.ds(2, frames), :, lanes[c]], es_sem.at[row, 0, c],
                      er_sem.at[slot, 1 - row, 0, c], partner)

    def edge_diag(slot, row, c):
        return remote(ecol.at[row, tail, :, lanes[c]], edge.at[slot, 1 - row, pl.ds(0, 2), :, lanes[c]], es_sem.at[row, 1, c],
                      er_sem.at[slot, 1 - row, 1, c], diag)

    def repeat_first(slot, row, cols):
        @pl.when(r == 0)
        def _():
            for f in HALVES:
                halo[slot, row, f, :, cols] = vid[slot, row, 0, :, cols]
                edge[slot, row, f, :, cols] = edge[slot, row, 2, :, cols]

    def half_out(slot, c):
        sums_start(slot, c)
        for row in (OTH, OWN):
            edge_send(slot, row, c).start()

        @pl.when(not_last)
        def _():
            for row in (OTH, OWN):
                edge_diag(slot, row, c).start()
                halo_send(slot, row, c).start()

    def half_in(slot, c, layer):
        for d in sum_sends(slot, c):
            d.wait()
        for row in (OTH, OWN):
            edge_send(slot, row, c).wait()

        @pl.when(not_last)
        def _():
            for row in (OTH, OWN):
                edge_diag(slot, row, c).wait_send()
                halo_send(slot, row, c).wait_send()

        @pl.when(not_first)
        def _():
            for row in (OTH, OWN):
                edge_diag(slot, row, c).wait_recv()
                halo_send(slot, row, c).wait_recv()

        repeat_first(slot, OWN, lanes[c])
        repeat_first(slot, OTH, lanes[c])
        return coefficients(slot, c, layer)

    every = slice(0, chans)
    x_halo = remote(lat.at[tail, 0, my_cols, :], halo.at[0, OWN], hs_sem.at[OWN, 0], hr_sem.at[0, OWN, 0], nxt)
    x_pass = remote(vid.at[0, OTH, tail], halo.at[0, OTH], hs_sem.at[OTH, 0], hr_sem.at[0, OTH, 0], nxt)
    e_part = remote(ecol.at[OWN], edge.at[0, OTH, pl.ds(2, frames)], es_sem.at[OWN, 0, 0], er_sem.at[0, OTH, 0, 0], partner)
    e_nxt = remote(edge.at[0, OWN, pl.ds(frames, 2)], edge.at[0, OWN, pl.ds(0, 2)], es_sem.at[OTH, 1, 0], er_sem.at[0, OWN, 1, 0], nxt)
    e_diag = remote(ecol.at[OWN, tail], edge.at[0, OTH, pl.ds(0, 2)], es_sem.at[OWN, 1, 0], er_sem.at[0, OTH, 1, 0], diag)
    for c in HALVES:
        sums_start(0, c)
    e_part.start()

    @pl.when(not_last)
    def _():
        e_diag.start()
        e_nxt.start()
        x_halo.start()

    for g in (3, 2, 1, 0):
        x_piece(g).start()
        if g == 3:
            for c in w_rest:
                c.start()
    w_copy(1).start()
    load_own.wait()
    for c in small:
        c.wait()
    for c in HALVES:
        for d in sum_sends(0, c):
            d.wait()
    coef = [coefficients(0, c, 0) for c in HALVES]
    for p in range(2, frames + 2):
        for c in HALVES:
            norm(coef[c], 0, OWN, p, c)

    @pl.when(not_last)
    def _():
        x_halo.wait_send()
        e_nxt.wait_send()

    @pl.when(not_first)
    def _():
        x_halo.wait_recv()
        e_nxt.wait_recv()

    repeat_first(0, OWN, every)
    for p in range(2):
        for c in HALVES:
            norm(coef[c], 0, OWN, p, c)
    w_mid.wait()

    @pl.loop(0, 4)
    def _(c):
        @pl.when(c == 2)
        def _():
            for w in w_rest:
                w.wait()

        i = c // 2
        f0 = lax.rem(c, 2) * (frames // 2)
        rows = pl.ds(pl.multiple_of(f0 * half, half), frames // 2 * half)
        acc[i, rows, :] = dots(0, i, (OWN,), frames_of(f0, frames // 2))

    e_part.wait()

    @pl.when(not_last)
    def _():
        e_diag.wait_send()

    @pl.when(not_first)
    def _():
        e_diag.wait_recv()

    def last_k(i, g, c):
        rows = pl.ds(g * per * half, per * half)
        finish(0, 1, i, g * per, acc[i, rows, lanes[c]] + dots(0, i, (OTH,), frames_of(g * per, per), n_half=c), c)

    for g in (3, 2, 1, 0):
        x_piece(g).wait()
        if g == 3:
            x_piece(4).wait()

            @pl.when(not_last)
            def _():
                x_pass.start()
        if g == 0:
            @pl.when(not_last)
            def _():
                x_pass.wait_send()

            @pl.when(not_first)
            def _():
                x_pass.wait_recv()

            repeat_first(0, OTH, every)
        for p in reversed(range(g * per, frames + 2 if g == 3 else (g + 1) * per)):
            for c in HALVES:
                norm(coef[c], 0, OTH, p, c)
        rows = pl.ds(g * per * half, per * half)
        for i in (OTH, OWN):
            if g > 1:
                p = acc[i, rows, :] + dots(0, i, (OTH,), frames_of(g * per, per))
                for c in HALVES:
                    finish(0, 1, i, g * per, p[:, lanes[c]], c)
            else:
                last_k(i, g, 0)
    half_out(1, 0)
    for g in (1, 0):
        for i in (OTH, OWN):
            last_k(i, g, 1)
    half_out(1, 1)

    def strip_send(row, c):
        return remote(vid.at[1, row, :, edge_strip, lanes[c]], ext.at[1 - row, pl.ds(2, frames), :, lanes[c]], ts_sem.at[row, 0, c],
                      tr_sem.at[1 - row, 0, c], partner)

    def strip_pass(row):
        return remote(ext.at[row, pl.ds(frames, 2)], ext.at[row, pl.ds(0, 2)], ts_sem.at[row, 1, 0], tr_sem.at[row, 1, 0], nxt)

    def col2_send(row):
        return remote(ecol2.at[row], edge2.at[1 - row, pl.ds(2, frames)], cs_sem.at[row, 0], cr_sem.at[1 - row, 0], partner)

    def col2_diag(row):
        return remote(ecol2.at[row, tail], edge2.at[1 - row, pl.ds(0, 2)], cs_sem.at[row, 1], cr_sem.at[1 - row, 1], diag)

    def res_send():
        return remote(vid.at[0, OTH, :, edge_strip, :], xres, rs_sem.at[0], rs_sem.at[1], partner)

    def layer_body(layer, carry):
        slot = lax.rem(layer, 2)
        nslot = 1 - slot
        w_copy(layer + 1).start()

        @pl.when(layer == 2)
        def _():
            res_send().start()

        def norms(lo, hi, c):
            for row in (OWN, OTH):
                for p in reversed(range(lo, hi)):
                    norm(coef[c], slot, row, p, c)

        def first_k(i, g):
            acc[i, g * per * half:(g + 1) * per * half, :] = dots(slot, i, (OWN, OTH), frames_of(g * per, per), k_half=0)

        coef = [half_in(slot, 0, layer)]
        w_copy(layer).wait()
        norms(3 * per, frames + 2, 0)
        norms(2 * per, 3 * per, 0)
        first_k(OTH, 3)
        norms(per, 2 * per, 0)
        first_k(OTH, 2)
        norms(0, per, 0)
        first_k(OTH, 1)
        first_k(OTH, 0)
        coef.append(half_in(slot, 1, layer))
        norms(3 * per, frames + 2, 1)
        first_k(OWN, 3)
        norms(2 * per, 3 * per, 1)
        first_k(OWN, 2)
        norms(per, 2 * per, 1)
        first_k(OWN, 1)
        norms(0, per, 1)
        first_k(OWN, 0)
        for c in HALVES:
            for i in (OTH, OWN):
                for g in (3, 2, 1, 0):
                    rows = slice(g * per * half, (g + 1) * per * half)
                    p = dots(slot, i, (OWN, OTH), frames_of(g * per, per), k_half=1, n_half=c)
                    finish(layer, nslot, i, g * per, acc[i, rows, lanes[c]] + p, c)
            half_out(nslot, c)

            @pl.when(layer == 2)
            def _():
                for row in (OTH, OWN):
                    strip_send(row, c).start()

        return carry

    lax.fori_loop(1, 3, layer_body, 0)

    wide = frames // 4
    pieces_out = (3, 2, 1, 0)

    def out_send(k):
        fs = pl.ds(k * wide, wide)
        dst = out.at[fs, 0, pl.ds(pl.multiple_of(h * (half + strip), strip), part), :]
        return remote(vid.at[0, OTH, fs, part_cols, :], dst, os_sem.at[k], or_sem.at[k], partner)

    def out_local():
        return pltpu.make_async_copy(vid.at[0, OWN], out.at[:, 0, my_cols, :], o_sem.at[0])

    def out_ext():
        dst = out.at[:, 0, pl.ds(pl.multiple_of(half - h * strip, strip), strip), :]
        return pltpu.make_async_copy(xres, dst, o_sem.at[1])

    def norms(lo, hi, c):
        for row in (OWN, OTH):
            for p in reversed(range(lo, hi)):
                norm(coef[c], 1, row, p, c)

    def close(res, p):
        return (res.astype(F32) + (p + bias[3:4, :]).astype(BF16).astype(F32)).astype(BF16)

    def part_dots(k, k_half):
        return dots(1, OTH, (OWN, OTH), lambda j, t, at: act[j, pl.ds(k * wide + t, wide), part_cols, at], k_half)

    def part_chunk(k):
        rows = slice(k * wide * part, (k + 1) * wide * part)
        p = acc[OTH, rows, :] + part_dots(k, 1)
        for f in range(wide):
            fr = k * wide + f
            vid[0, OTH, fr, part_cols, :] = close(vid[0, OTH, fr, part_cols, :], p[f * part:(f + 1) * part])
        out_send(k).start()

    def own_chunk(g):
        if g == 3:
            p = acc[OWN, g * per * half:(g + 1) * per * half, :] + dots(1, OWN, (OWN, OTH), frames_of(g * per, per), 1)
        else:
            p = dots(1, OWN, (OWN, OTH), frames_of(g * per, per))
        for f in range(per):
            vid[0, OWN, g * per + f] = close(vid[0, OWN, g * per + f], p[f * half:(f + 1) * half])

    coef = [half_in(1, 0, 3)]
    w_copy(3).wait()
    def norms_for(k, c):
        norms(k * wide, frames + 2 if k == 3 else (k + 1) * wide, c)

    norms_for(3, 0)
    norms_for(2, 0)
    for k in pieces_out:
        acc[OTH, k * wide * part:(k + 1) * wide * part, :] = part_dots(k, 0)
        if k > 1:
            norms_for(k - 2, 0)
    acc[OWN, 3 * per * half:4 * per * half, :] = dots(1, OWN, (OWN, OTH), frames_of(3 * per, per), 0)

    def columns2(f, carry):
        for row in (OWN, OTH):
            v = vid[1, row, f, strip:half - strip, :].astype(F32)
            ecol2[row, f] = jnp.where(h == 0, v[half - 2 * strip - 1:half - 2 * strip], v[0:1])
        return carry

    lax.fori_loop(0, frames, columns2, 0)
    for row in (OWN, OTH):
        col2_send(row).start()

    @pl.when(not_last)
    def _():
        for row in (OWN, OTH):
            col2_diag(row).start()

    coef.append(half_in(1, 1, 3))
    norms_for(3, 1)
    for k in pieces_out:
        if k > 0:
            norms_for(k - 1, 1)
        part_chunk(k)
    for row in (OWN, OTH):
        col2_send(row).wait()
        for c in HALVES:
            strip_send(row, c).wait()

    @pl.when(not_last)
    def _():
        for row in (OWN, OTH):
            col2_diag(row).wait_send()
            strip_pass(row).start()

    @pl.when(not_first)
    def _():
        for row in (OWN, OTH):
            col2_diag(row).wait_recv()

    @pl.when(r == 0)
    def _():
        for row in (OWN, OTH):
            for f in HALVES:
                ext[row, f] = ext[row, 2]
                edge2[row, f] = edge2[row, 2]

    res_send().wait()
    for row in (OWN, OTH):
        for p in range(2, frames + 2):
            for c in HALVES:
                norm_ext(coef[c], row, p, c)
    for g in (3, 2, 1, 0):
        own_chunk(g)
    out_local().start()

    @pl.when(not_last)
    def _():
        for row in (OWN, OTH):
            strip_pass(row).wait_send()

    @pl.when(not_first)
    def _():
        for row in (OWN, OTH):
            strip_pass(row).wait_recv()

    for row in (OWN, OTH):
        for p in HALVES:
            for c in HALVES:
                norm_ext(coef[c], row, p, c)
    p = dots(1, OWN, (OWN, OTH), lambda j, t, at: xact[j, pl.ds(t, frames), :, at])
    for f in range(frames):
        xres[f] = close(xres[f], p[f * strip:(f + 1) * strip])
    out_ext().start()
    out_local().wait()
    out_ext().wait()
    for k in pieces_out:
        out_send(k).wait()


def solution(mesh):
    n_cp = mesh.shape["cp"]

    def local_decode(lat, conv_w, conv_b, gn_gamma, gn_beta):
        frames, _, width, chans = lat.shape
        half = width // 2
        strip = half // 4
        n_dev = 2 * n_cp
        count = frames * n_cp * 2 * width * (chans // GROUPS)
        dma = pltpu.SemaphoreType.DMA

        def pair(*more):
            return dma((2, *more))

        any_spec = pl.BlockSpec(memory_space=pl.ANY)
        return pl.pallas_call(
            functools.partial(kernel, (n_cp, frames, half, strip, chans, count)),
            out_shape=jax.ShapeDtypeStruct(lat.shape, BF16),
            in_specs=[any_spec] * 5,
            out_specs=any_spec,
            scratch_shapes=[
                pltpu.VMEM(conv_b.shape, F32),
                pltpu.VMEM(gn_gamma.shape, F32),
                pltpu.VMEM(gn_beta.shape, F32),
                pltpu.VMEM((2, 2, frames, half, chans), BF16),
                pltpu.VMEM((2, frames + 2, half, 3 * chans), BF16),
                pltpu.VMEM((2, frames * half, chans), F32),
                pltpu.VMEM((2, 3, 3, 3 * chans, chans), BF16),
                pltpu.VMEM(lat.shape, BF16),
                pltpu.VMEM((2, 2, 2, half, chans), BF16),
                pltpu.VMEM((2, 2, frames + 2, 1, chans), F32),
                pltpu.VMEM((2, frames, 1, chans), F32),
                pltpu.VMEM((2, frames + 2, strip, chans), BF16),
                pltpu.VMEM((2, frames + 2, strip, 3 * chans), BF16),
                pltpu.VMEM((2, frames + 2, 1, chans), F32),
                pltpu.VMEM((2, frames, 1, chans), F32),
                pltpu.VMEM((frames, strip, chans), BF16),
                pltpu.VMEM((2, 2, 8, chans // 2), F32),
                pltpu.VMEM((2, 8, chans // 2), F32),
                pltpu.VMEM((2, 2, chans // 2), F32),
                pltpu.VMEM((2, 2, n_dev, 2, chans // 2), F32),
                dma((8,)),
                dma((4,)),
                dma((5,)),
                dma((5,)),
                pair(2),
                pair(2, 2),
                pair(2, 2),
                pair(2, 2, 2),
                pair(2, 2),
                pair(2, 2),
                pair(2),
                pair(2),
                pair(),
                pair(n_dev),
                pair(2, n_dev),
                pair(),
                dma((4,)),
                dma((4,)),
            ],
            compiler_params=pltpu.CompilerParams(collective_id=0, has_side_effects=True, vmem_limit_bytes=52 * 1024 * 1024),
            name="decode",
        )(*(pltpu.with_memory_space_constraint(a, pltpu.HBM) for a in (lat, conv_w.reshape(4, 3, 3, 3 * chans, chans), conv_b, gn_gamma, gn_beta)))

    spec = P(("dp", "cp"), "hp", None, None)
    return jax.shard_map(local_decode, mesh=mesh, in_specs=(spec, P(), P(), P(), P()), out_specs=spec, check_vma=False)
```

```python
import functools

import jax
import jax.numpy as jnp
from jax import lax
from jax.experimental import pallas as pl
from jax.experimental.pallas import tpu as pltpu
from jax.sharding import PartitionSpec as P

GROUPS = 32
EPS = 1e-6
MESH = pl.DeviceIdType.MESH
F32 = jnp.float32
BF16 = jnp.bfloat16
HALVES = OWN, OTH = 0, 1


def kernel(dims, lat, w_hbm, bias_hbm, gamma_hbm, beta_hbm, out, bias, gamma, beta, vid, act, acc, w_buf, x_in, halo, edge, ecol, ext, xact, edge2, ecol2, xres,
           s_acc, s_tot, s_send, s_recv, l_sem, w_sem, xs_sem, xr_sem, hs_sem, hr_sem, es_sem, er_sem, ts_sem, tr_sem, cs_sem, cr_sem,
           rs_sem, ss_sem, sr_sem, o_sem, os_sem, or_sem):
    n_cp, frames, half, strip, chans, count = dims
    n_dev = 2 * n_cp
    per = frames // 4
    h = lax.axis_index("hp")
    r = lax.axis_index("cp")
    me = h * n_cp + r
    partner = {"hp": 1 - h, "cp": r}
    nxt = {"hp": h, "cp": lax.rem(r + 1, n_cp)}
    diag = {"hp": 1 - h, "cp": lax.rem(r + 1, n_cp)}
    not_last = r < n_cp - 1
    not_first = r > 0
    tail = pl.ds(frames - 2, 2)
    my_cols = pl.ds(pl.multiple_of(h * half, half), half)
    ot_cols = pl.ds(pl.multiple_of((1 - h) * half, half), half)
    hc = chans // 2
    lanes = [slice(c * hc, (c + 1) * hc) for c in HALVES]
    part = half - strip
    part_cols = pl.ds(pl.multiple_of(h * strip, strip), part)
    edge_strip = pl.ds(pl.multiple_of((1 - h) * part, strip), strip)

    def remote(src, dst, send, recv, dev):
        return pltpu.make_async_remote_copy(src_ref=src, dst_ref=dst, send_sem=send, recv_sem=recv, device_id=dev, device_id_type=MESH)

    def peer(step):
        t = lax.rem(me + step, n_dev)
        return {"hp": t // n_cp, "cp": lax.rem(t, n_cp)}

    def load_x(k):
        fs = pl.ds(k * per, per)
        return pltpu.make_async_copy(lat.at[fs], x_in.at[fs], l_sem.at[k])

    for k in range(4):
        load_x(k).start()
    small = [pltpu.make_async_copy(a, b, l_sem.at[4 + k]) for k, (a, b) in enumerate([(bias_hbm, bias), (gamma_hbm, gamma), (beta_hbm, beta)])]
    load_own = pltpu.make_async_copy(lat.at[:, 0, my_cols, :], vid.at[0, OWN], l_sem.at[7])

    def w_copy(layer):
        slot = lax.rem(layer, 2)
        return pltpu.make_async_copy(w_hbm.at[layer], w_buf.at[slot], w_sem.at[slot])

    barrier = pltpu.get_barrier_semaphore()
    for step in range(1, n_dev):
        pl.semaphore_signal(barrier, inc=1, device_id=peer(step), device_id_type=MESH)
    for c in small:
        c.start()
    load_own.start()
    w_copy(0).start()

    def fold(v):
        t = v[0:8]
        for k in range(1, v.shape[0] // 8):
            t = t + v[8 * k:8 * k + 8]
        return t

    s_acc[...] = jnp.zeros_like(s_acc)
    s_tot[...] = jnp.zeros_like(s_tot)

    def first_sums(f, carry):
        v = x_in[f, 0].astype(F32)
        for c in HALVES:
            s_acc[c, 0] += fold(v[:, lanes[c]])
            s_acc[c, 1] += fold(v[:, lanes[c]] * v[:, lanes[c]])
        lo, hi = v[half - 1:half], v[half:half + 1]
        ecol[OWN, f] = jnp.where(h == 0, lo, hi)
        edge[0, OWN, f + 2] = jnp.where(h == 0, hi, lo)
        return carry

    starts = (0, 1, 1 + per, 1 + 2 * per, frames - 1, frames)

    def x_piece(g):
        fs = pl.ds(starts[g], starts[g + 1] - starts[g])
        return remote(lat.at[fs, 0, ot_cols, :], vid.at[0, OTH, fs], xs_sem.at[g], xr_sem.at[g], partner)

    for k in range(4):
        load_x(k).wait()
        if k == 1:
            pl.semaphore_wait(barrier, n_dev - 1)
            x_piece(4).start()
        lax.fori_loop(k * per, (k + 1) * per, first_sums, 0)

    lane = lax.broadcasted_iota(jnp.int32, (8, hc), 1)
    n_group = chans // GROUPS

    def sum_sends(slot, c):
        return [remote(s_send.at[c], s_recv.at[slot, c, step], ss_sem.at[c, step], sr_sem.at[slot, c, step], peer(step)) for step in range(1, n_dev)]

    def sums_start(slot, c):
        s_send[c, 0:1] = jnp.sum(s_acc[c, 0], axis=0, keepdims=True)
        s_send[c, 1:2] = jnp.sum(s_acc[c, 1], axis=0, keepdims=True)
        s_acc[c] = jnp.zeros_like(s_acc[c])
        for d in sum_sends(slot, c):
            d.start()

    def coefficients(slot, c, layer):
        total = s_send[c]
        for step in range(1, n_dev):
            total = total + s_recv[slot, c, step]
        s_tot[c, 0:2] = total
        t = s_tot[c]
        unit = 1
        while unit < n_group:
            place = (lane // unit) & 3
            g = t
            for d in range(1, 4):
                up = pltpu.roll(t, hc - d * unit, 1)
                down = pltpu.roll(t, (4 - d) * unit, 1)
                g = g + jnp.where(place + d < 4, up, down)
            t = g
            unit *= 4
        t = t * (1.0 / count)
        mean = t[0:1]
        inv = lax.rsqrt(t[1:2] - mean * mean + EPS)
        scale = inv * gamma[pl.ds(layer, 1), lanes[c]]
        return 0.5 * scale, 0.5 * (beta[pl.ds(layer, 1), lanes[c]] - mean * scale)

    def silu(coef, v):
        u = v * coef[0] + coef[1]
        return u + u * jnp.tanh(u)

    def put_shifted(dst, row, p, y, left, right, start):
        n, w = y.shape
        at = lax.broadcasted_iota(jnp.int32, (8, w), 0)
        before = pltpu.roll(y, 1, 0)
        after = pltpu.roll(y, n - 1, 0)
        before = jnp.concatenate([jnp.where(at == 0, left, before[0:8]), before[8:]], axis=0)
        after = jnp.concatenate([after[:n - 8], jnp.where(at == 7, right, after[n - 8:])], axis=0)
        for d, v in enumerate((before, y, after)):
            dst[row, p, :, d * chans + start:d * chans + start + w] = v.astype(BF16)

    def norm(coef, slot, row, p, c):
        v = halo[slot, row, p, :, lanes[c]] if p < 2 else vid[slot, row, p - 2, :, lanes[c]]
        y = silu(coef, v.astype(F32))
        ye = silu(coef, edge[slot, row, p, :, lanes[c]])
        put_shifted(act, row, p, y, jnp.where(h == 0, 0.0, ye), jnp.where(h == 0, ye, 0.0), c * hc)

    def norm_ext(coef, row, p, c):
        mine = silu(coef, (halo[1, row, p, :, lanes[c]] if p < 2 else vid[1, row, p - 2, :, lanes[c]]).astype(F32))
        y = silu(coef, ext[row, p, :, lanes[c]].astype(F32))
        far = silu(coef, edge2[row, p, :, lanes[c]])
        put_shifted(xact, row, p, y, jnp.where(h == 0, mine[half - 1:half], far), jnp.where(h == 0, far, mine[0:1]), c * hc)

    def dots(slot, i, js, lhs, k_half=None, n_half=None):
        cols = slice(0, chans) if n_half is None else lanes[n_half]
        total = None
        for j in js:
            if isinstance(i, int):
                di = 1 if i == j else (2 - 2 * h if i == OWN else 2 * h)
            else:
                di = jnp.where(i == OWN, 1, 2 * h)
            left, right = [], []
            for k in reversed(range(3)):
                for d in range(3):
                    for c in HALVES:
                        if k_half is None or c == k_half:
                            at = slice(d * chans + c * hc, d * chans + (c + 1) * hc)
                            v = lhs(j, k, at)
                            left.append(v.reshape(v.shape[0] * v.shape[1], v.shape[2]))
                            right.append(w_buf[slot, k, di, at, cols])
            q = jnp.dot(jnp.concatenate(left, axis=1), jnp.concatenate(right, axis=0), preferred_element_type=F32)
            total = q if total is None else total + q
        return total

    def frames_of(f0, n):
        return lambda j, k, at: act[j, pl.ds(f0 + k, n), :, at]

    def finish(layer, nslot, i, f0, p, c):
        b = bias[pl.ds(layer, 1), lanes[c]]
        t1 = t2 = None
        for f in range(p.shape[0] // half):
            v = (p[f * half:(f + 1) * half] + b).astype(BF16).astype(F32)
            if isinstance(layer, int):
                vb = v.astype(BF16)
            else:
                res = vid[0, i, f0 + f, :, lanes[c]].astype(F32)
                vb = jnp.where(nslot == 0, res + v, v).astype(BF16)
            vid[nslot, i, f0 + f, :, lanes[c]] = vb
            v = vb.astype(F32)
            t1 = fold(v) if t1 is None else t1 + fold(v)
            t2 = fold(v * v) if t2 is None else t2 + fold(v * v)
            ecol[i, f0 + f, :, lanes[c]] = jnp.where(h == 0, v[half - 1:half], v[0:1])
        s_acc[c, 0] += t1
        s_acc[c, 1] += t2

    def halo_send(slot, row, c):
        return remote(vid.at[slot, row, tail, :, lanes[c]], halo.at[slot, row, :, :, lanes[c]], hs_sem.at[row, c], hr_sem.at[slot, row, c], nxt)

    def edge_send(slot, row, c):
        return remote(ecol.at[row, :, :, lanes[c]], edge.at[slot, 1 - row, pl.ds(2, frames), :, lanes[c]], es_sem.at[row, 0, c],
                      er_sem.at[slot, 1 - row, 0, c], partner)

    def edge_diag(slot, row, c):
        return remote(ecol.at[row, tail, :, lanes[c]], edge.at[slot, 1 - row, pl.ds(0, 2), :, lanes[c]], es_sem.at[row, 1, c],
                      er_sem.at[slot, 1 - row, 1, c], diag)

    def repeat_first(slot, row, cols):
        @pl.when(r == 0)
        def _():
            for f in HALVES:
                halo[slot, row, f, :, cols] = vid[slot, row, 0, :, cols]
                edge[slot, row, f, :, cols] = edge[slot, row, 2, :, cols]

    def half_out(slot, c):
        sums_start(slot, c)
        for row in (OTH, OWN):
            edge_send(slot, row, c).start()

        @pl.when(not_last)
        def _():
            for row in (OTH, OWN):
                edge_diag(slot, row, c).start()
                halo_send(slot, row, c).start()

    def half_in(slot, c, layer):
        for d in sum_sends(slot, c):
            d.wait()
        for row in (OTH, OWN):
            edge_send(slot, row, c).wait()

        @pl.when(not_last)
        def _():
            for row in (OTH, OWN):
                edge_diag(slot, row, c).wait_send()
                halo_send(slot, row, c).wait_send()

        @pl.when(not_first)
        def _():
            for row in (OTH, OWN):
                edge_diag(slot, row, c).wait_recv()
                halo_send(slot, row, c).wait_recv()

        repeat_first(slot, OWN, lanes[c])
        repeat_first(slot, OTH, lanes[c])
        return coefficients(slot, c, layer)

    every = slice(0, chans)
    x_halo = remote(lat.at[tail, 0, my_cols, :], halo.at[0, OWN], hs_sem.at[OWN, 0], hr_sem.at[0, OWN, 0], nxt)
    x_pass = remote(vid.at[0, OTH, tail], halo.at[0, OTH], hs_sem.at[OTH, 0], hr_sem.at[0, OTH, 0], nxt)
    e_part = remote(ecol.at[OWN], edge.at[0, OTH, pl.ds(2, frames)], es_sem.at[OWN, 0, 0], er_sem.at[0, OTH, 0, 0], partner)
    e_nxt = remote(edge.at[0, OWN, pl.ds(frames, 2)], edge.at[0, OWN, pl.ds(0, 2)], es_sem.at[OTH, 1, 0], er_sem.at[0, OWN, 1, 0], nxt)
    e_diag = remote(ecol.at[OWN, tail], edge.at[0, OTH, pl.ds(0, 2)], es_sem.at[OWN, 1, 0], er_sem.at[0, OTH, 1, 0], diag)
    for c in HALVES:
        sums_start(0, c)
    e_part.start()

    @pl.when(not_last)
    def _():
        e_diag.start()
        e_nxt.start()
        x_halo.start()

    for g in (3, 2, 1, 0):
        x_piece(g).start()
    w_copy(1).start()
    load_own.wait()
    for c in small:
        c.wait()
    for c in HALVES:
        for d in sum_sends(0, c):
            d.wait()
    coef = [coefficients(0, c, 0) for c in HALVES]
    for p in range(2, frames + 2):
        for c in HALVES:
            norm(coef[c], 0, OWN, p, c)

    @pl.when(not_last)
    def _():
        x_halo.wait_send()
        e_nxt.wait_send()

    @pl.when(not_first)
    def _():
        x_halo.wait_recv()
        e_nxt.wait_recv()

    repeat_first(0, OWN, every)
    for p in range(2):
        for c in HALVES:
            norm(coef[c], 0, OWN, p, c)
    w_copy(0).wait()

    @pl.loop(0, 4)
    def _(c):
        i = c // 2
        f0 = lax.rem(c, 2) * (frames // 2)
        rows = pl.ds(pl.multiple_of(f0 * half, half), frames // 2 * half)
        acc[i, rows, :] = dots(0, i, (OWN,), frames_of(f0, frames // 2))

    e_part.wait()

    @pl.when(not_last)
    def _():
        e_diag.wait_send()

    @pl.when(not_first)
    def _():
        e_diag.wait_recv()

    def last_k(i, g, c):
        rows = pl.ds(g * per * half, per * half)
        finish(0, 1, i, g * per, acc[i, rows, lanes[c]] + dots(0, i, (OTH,), frames_of(g * per, per), n_half=c), c)

    for g in (3, 2, 1, 0):
        x_piece(g).wait()
        if g == 3:
            x_piece(4).wait()

            @pl.when(not_last)
            def _():
                x_pass.start()
        if g == 0:
            @pl.when(not_last)
            def _():
                x_pass.wait_send()

            @pl.when(not_first)
            def _():
                x_pass.wait_recv()

            repeat_first(0, OTH, every)
        for p in reversed(range(g * per, frames + 2 if g == 3 else (g + 1) * per)):
            for c in HALVES:
                norm(coef[c], 0, OTH, p, c)
        rows = pl.ds(g * per * half, per * half)
        for i in (OTH, OWN):
            if g > 1:
                p = acc[i, rows, :] + dots(0, i, (OTH,), frames_of(g * per, per))
                for c in HALVES:
                    finish(0, 1, i, g * per, p[:, lanes[c]], c)
            else:
                last_k(i, g, 0)
    half_out(1, 0)
    for g in (1, 0):
        for i in (OTH, OWN):
            last_k(i, g, 1)
    half_out(1, 1)

    def strip_send(row, c):
        return remote(vid.at[1, row, :, edge_strip, lanes[c]], ext.at[1 - row, pl.ds(2, frames), :, lanes[c]], ts_sem.at[row, 0, c],
                      tr_sem.at[1 - row, 0, c], partner)

    def strip_pass(row):
        return remote(ext.at[row, pl.ds(frames, 2)], ext.at[row, pl.ds(0, 2)], ts_sem.at[row, 1, 0], tr_sem.at[row, 1, 0], nxt)

    def col2_send(row):
        return remote(ecol2.at[row], edge2.at[1 - row, pl.ds(2, frames)], cs_sem.at[row, 0], cr_sem.at[1 - row, 0], partner)

    def col2_diag(row):
        return remote(ecol2.at[row, tail], edge2.at[1 - row, pl.ds(0, 2)], cs_sem.at[row, 1], cr_sem.at[1 - row, 1], diag)

    def res_send():
        return remote(vid.at[0, OTH, :, edge_strip, :], xres, rs_sem.at[0], rs_sem.at[1], partner)

    def layer_body(layer, carry):
        slot = lax.rem(layer, 2)
        nslot = 1 - slot
        w_copy(layer + 1).start()

        @pl.when(layer == 2)
        def _():
            res_send().start()

        def norms(lo, hi, c):
            for row in (OWN, OTH):
                for p in reversed(range(lo, hi)):
                    norm(coef[c], slot, row, p, c)

        def first_k(i, g):
            acc[i, g * per * half:(g + 1) * per * half, :] = dots(slot, i, (OWN, OTH), frames_of(g * per, per), k_half=0)

        coef = [half_in(slot, 0, layer)]
        w_copy(layer).wait()
        norms(3 * per, frames + 2, 0)
        norms(2 * per, 3 * per, 0)
        first_k(OTH, 3)
        norms(per, 2 * per, 0)
        first_k(OTH, 2)
        norms(0, per, 0)
        first_k(OTH, 1)
        first_k(OTH, 0)
        coef.append(half_in(slot, 1, layer))
        norms(3 * per, frames + 2, 1)
        first_k(OWN, 3)
        norms(2 * per, 3 * per, 1)
        first_k(OWN, 2)
        norms(per, 2 * per, 1)
        first_k(OWN, 1)
        norms(0, per, 1)
        first_k(OWN, 0)
        for c in HALVES:
            for i in (OTH, OWN):
                for g in (3, 2, 1, 0):
                    rows = slice(g * per * half, (g + 1) * per * half)
                    p = dots(slot, i, (OWN, OTH), frames_of(g * per, per), k_half=1, n_half=c)
                    finish(layer, nslot, i, g * per, acc[i, rows, lanes[c]] + p, c)
                if i == OTH and c == 0:
                    @pl.when(layer == 2)
                    def _():
                        strip_send(OTH, 0).start()

            half_out(nslot, c)

            @pl.when(layer == 2)
            def _():
                if c == 1:
                    strip_send(OTH, 1).start()
                strip_send(OWN, c).start()

        return carry

    lax.fori_loop(1, 3, layer_body, 0)

    wide = frames // 4
    pieces_out = (3, 2, 1, 0)

    def out_send(k):
        fs = pl.ds(k * wide, wide)
        dst = out.at[fs, 0, pl.ds(pl.multiple_of(h * (half + strip), strip), part), :]
        return remote(vid.at[0, OTH, fs, part_cols, :], dst, os_sem.at[k], or_sem.at[k], partner)

    def out_local():
        return pltpu.make_async_copy(vid.at[0, OWN], out.at[:, 0, my_cols, :], o_sem.at[0])

    def out_ext():
        dst = out.at[:, 0, pl.ds(pl.multiple_of(half - h * strip, strip), strip), :]
        return pltpu.make_async_copy(xres, dst, o_sem.at[1])

    def norms(lo, hi, c):
        for row in (OWN, OTH):
            for p in reversed(range(lo, hi)):
                norm(coef[c], 1, row, p, c)

    def close(res, p):
        return (res.astype(F32) + (p + bias[3:4, :]).astype(BF16).astype(F32)).astype(BF16)

    def part_dots(k, k_half):
        return dots(1, OTH, (OWN, OTH), lambda j, t, at: act[j, pl.ds(k * wide + t, wide), part_cols, at], k_half)

    def part_chunk(k):
        rows = slice(k * wide * part, (k + 1) * wide * part)
        p = acc[OTH, rows, :] + part_dots(k, 1)
        for f in range(wide):
            fr = k * wide + f
            vid[0, OTH, fr, part_cols, :] = close(vid[0, OTH, fr, part_cols, :], p[f * part:(f + 1) * part])
        out_send(k).start()

    def own_chunk(g):
        p = dots(1, OWN, (OWN, OTH), frames_of(g * per, per))
        for f in range(per):
            vid[0, OWN, g * per + f] = close(vid[0, OWN, g * per + f], p[f * half:(f + 1) * half])

    coef = [half_in(1, 0, 3)]
    w_copy(3).wait()
    def norms_for(k, c):
        norms(k * wide, frames + 2 if k == 3 else (k + 1) * wide, c)

    norms_for(3, 0)
    norms_for(2, 0)
    for k in pieces_out:
        acc[OTH, k * wide * part:(k + 1) * wide * part, :] = part_dots(k, 0)
        if k > 1:
            norms_for(k - 2, 0)
    def columns2(f, carry):
        for row in (OWN, OTH):
            v = vid[1, row, f, strip:half - strip, :].astype(F32)
            ecol2[row, f] = jnp.where(h == 0, v[half - 2 * strip - 1:half - 2 * strip], v[0:1])
        return carry

    lax.fori_loop(0, frames, columns2, 0)
    for row in (OWN, OTH):
        col2_send(row).start()

    @pl.when(not_last)
    def _():
        for row in (OWN, OTH):
            col2_diag(row).start()

    coef.append(half_in(1, 1, 3))
    norms_for(3, 1)
    for k in pieces_out:
        if k > 0:
            norms_for(k - 1, 1)
        part_chunk(k)
    for row in (OWN, OTH):
        col2_send(row).wait()
        for c in HALVES:
            strip_send(row, c).wait()

    @pl.when(not_last)
    def _():
        for row in (OWN, OTH):
            col2_diag(row).wait_send()
            strip_pass(row).start()

    @pl.when(not_first)
    def _():
        for row in (OWN, OTH):
            col2_diag(row).wait_recv()

    @pl.when(r == 0)
    def _():
        for row in (OWN, OTH):
            for f in HALVES:
                ext[row, f] = ext[row, 2]
                edge2[row, f] = edge2[row, 2]

    res_send().wait()
    for row in (OWN, OTH):
        for p in range(2, frames + 2):
            for c in HALVES:
                norm_ext(coef[c], row, p, c)
    for g in (3, 2, 1, 0):
        own_chunk(g)
    out_local().start()

    @pl.when(not_last)
    def _():
        for row in (OWN, OTH):
            strip_pass(row).wait_send()

    @pl.when(not_first)
    def _():
        for row in (OWN, OTH):
            strip_pass(row).wait_recv()

    for row in (OWN, OTH):
        for p in HALVES:
            for c in HALVES:
                norm_ext(coef[c], row, p, c)
    p = dots(1, OWN, (OWN, OTH), lambda j, t, at: xact[j, pl.ds(t, frames), :, at])
    for f in range(frames):
        xres[f] = close(xres[f], p[f * strip:(f + 1) * strip])
    out_ext().start()
    out_local().wait()
    out_ext().wait()
    for k in pieces_out:
        out_send(k).wait()


def solution(mesh):
    n_cp = mesh.shape["cp"]

    def local_decode(lat, conv_w, conv_b, gn_gamma, gn_beta):
        frames, _, width, chans = lat.shape
        half = width // 2
        strip = half // 4
        n_dev = 2 * n_cp
        count = frames * n_cp * 2 * width * (chans // GROUPS)
        dma = pltpu.SemaphoreType.DMA

        def pair(*more):
            return dma((2, *more))

        any_spec = pl.BlockSpec(memory_space=pl.ANY)
        return pl.pallas_call(
            functools.partial(kernel, (n_cp, frames, half, strip, chans, count)),
            out_shape=jax.ShapeDtypeStruct(lat.shape, BF16),
            in_specs=[any_spec] * 5,
            out_specs=any_spec,
            scratch_shapes=[
                pltpu.VMEM(conv_b.shape, F32),
                pltpu.VMEM(gn_gamma.shape, F32),
                pltpu.VMEM(gn_beta.shape, F32),
                pltpu.VMEM((2, 2, frames, half, chans), BF16),
                pltpu.VMEM((2, frames + 2, half, 3 * chans), BF16),
                pltpu.VMEM((2, frames * half, chans), F32),
                pltpu.VMEM((2, 3, 3, 3 * chans, chans), BF16),
                pltpu.VMEM(lat.shape, BF16),
                pltpu.VMEM((2, 2, 2, half, chans), BF16),
                pltpu.VMEM((2, 2, frames + 2, 1, chans), F32),
                pltpu.VMEM((2, frames, 1, chans), F32),
                pltpu.VMEM((2, frames + 2, strip, chans), BF16),
                pltpu.VMEM((2, frames + 2, strip, 3 * chans), BF16),
                pltpu.VMEM((2, frames + 2, 1, chans), F32),
                pltpu.VMEM((2, frames, 1, chans), F32),
                pltpu.VMEM((frames, strip, chans), BF16),
                pltpu.VMEM((2, 2, 8, chans // 2), F32),
                pltpu.VMEM((2, 8, chans // 2), F32),
                pltpu.VMEM((2, 2, chans // 2), F32),
                pltpu.VMEM((2, 2, n_dev, 2, chans // 2), F32),
                dma((8,)),
                pair(),
                dma((5,)),
                dma((5,)),
                pair(2),
                pair(2, 2),
                pair(2, 2),
                pair(2, 2, 2),
                pair(2, 2),
                pair(2, 2),
                pair(2),
                pair(2),
                pair(),
                pair(n_dev),
                pair(2, n_dev),
                pair(),
                dma((4,)),
                dma((4,)),
            ],
            compiler_params=pltpu.CompilerParams(collective_id=0, has_side_effects=True, vmem_limit_bytes=52 * 1024 * 1024),
            name="decode",
        )(*(pltpu.with_memory_space_constraint(a, pltpu.HBM) for a in (lat, conv_w.reshape(4, 3, 3, 3 * chans, chans), conv_b, gn_gamma, gn_beta)))

    spec = P(("dp", "cp"), "hp", None, None)
    return jax.shard_map(local_decode, mesh=mesh, in_specs=(spec, P(), P(), P(), P()), out_specs=spec, check_vma=False)
```

```python
import functools

import jax
import jax.numpy as jnp
from jax import lax
from jax.experimental import pallas as pl
from jax.experimental.pallas import tpu as pltpu
from jax.sharding import PartitionSpec as P

GROUPS = 32
EPS = 1e-6
MESH = pl.DeviceIdType.MESH
F32 = jnp.float32
BF16 = jnp.bfloat16
HALVES = OWN, OTH = 0, 1


def kernel(dims, lat, w_hbm, bias_hbm, gamma_hbm, beta_hbm, out, bias, gamma, beta, vid, act, acc, w_buf, x_in, halo, edge, ecol, ext, xact, edge2, ecol2, xres,
           s_acc, s_tot, s_send, s_recv, l_sem, w_sem, xs_sem, xr_sem, hs_sem, hr_sem, es_sem, er_sem, ts_sem, tr_sem, cs_sem, cr_sem,
           rs_sem, ss_sem, sr_sem, o_sem, os_sem, or_sem):
    n_cp, frames, half, strip, chans, count = dims
    n_dev = 2 * n_cp
    per = frames // 4
    h = lax.axis_index("hp")
    r = lax.axis_index("cp")
    me = h * n_cp + r
    partner = {"hp": 1 - h, "cp": r}
    nxt = {"hp": h, "cp": lax.rem(r + 1, n_cp)}
    diag = {"hp": 1 - h, "cp": lax.rem(r + 1, n_cp)}
    not_last = r < n_cp - 1
    not_first = r > 0
    tail = pl.ds(frames - 2, 2)
    my_cols = pl.ds(pl.multiple_of(h * half, half), half)
    ot_cols = pl.ds(pl.multiple_of((1 - h) * half, half), half)
    hc = chans // 2
    lanes = [slice(c * hc, (c + 1) * hc) for c in HALVES]
    part = half - strip
    part_cols = pl.ds(pl.multiple_of(h * strip, strip), part)
    edge_strip = pl.ds(pl.multiple_of((1 - h) * part, strip), strip)

    def remote(src, dst, send, recv, dev):
        return pltpu.make_async_remote_copy(src_ref=src, dst_ref=dst, send_sem=send, recv_sem=recv, device_id=dev, device_id_type=MESH)

    def peer(step):
        t = lax.rem(me + step, n_dev)
        return {"hp": t // n_cp, "cp": lax.rem(t, n_cp)}

    def load_x(k):
        fs = pl.ds(k * per, per)
        return pltpu.make_async_copy(lat.at[fs], x_in.at[fs], l_sem.at[k])

    for k in range(4):
        load_x(k).start()
    small = [pltpu.make_async_copy(a, b, l_sem.at[4 + k]) for k, (a, b) in enumerate([(bias_hbm, bias), (gamma_hbm, gamma), (beta_hbm, beta)])]
    load_own = pltpu.make_async_copy(lat.at[:, 0, my_cols, :], vid.at[0, OWN], l_sem.at[7])

    def w_copy(layer):
        slot = lax.rem(layer, 2)
        return pltpu.make_async_copy(w_hbm.at[layer], w_buf.at[slot], w_sem.at[slot])

    barrier = pltpu.get_barrier_semaphore()
    for step in range(1, n_dev):
        pl.semaphore_signal(barrier, inc=1, device_id=peer(step), device_id_type=MESH)
    for c in small:
        c.start()
    load_own.start()
    w_copy(0).start()

    def fold(v):
        t = v[0:8]
        for k in range(1, v.shape[0] // 8):
            t = t + v[8 * k:8 * k + 8]
        return t

    s_acc[...] = jnp.zeros_like(s_acc)
    s_tot[...] = jnp.zeros_like(s_tot)

    def first_sums(f, carry):
        v = x_in[f, 0].astype(F32)
        for c in HALVES:
            s_acc[c, 0] += fold(v[:, lanes[c]])
            s_acc[c, 1] += fold(v[:, lanes[c]] * v[:, lanes[c]])
        lo, hi = v[half - 1:half], v[half:half + 1]
        ecol[OWN, f] = jnp.where(h == 0, lo, hi)
        edge[0, OWN, f + 2] = jnp.where(h == 0, hi, lo)
        return carry

    starts = (0, 1, 1 + per, 1 + 2 * per, frames - 1, frames)

    def x_piece(g):
        fs = pl.ds(starts[g], starts[g + 1] - starts[g])
        return remote(lat.at[fs, 0, ot_cols, :], vid.at[0, OTH, fs], xs_sem.at[g], xr_sem.at[g], partner)

    for k in range(4):
        load_x(k).wait()
        if k == 1:
            pl.semaphore_wait(barrier, n_dev - 1)
            x_piece(4).start()
        lax.fori_loop(k * per, (k + 1) * per, first_sums, 0)

    lane = lax.broadcasted_iota(jnp.int32, (8, hc), 1)
    n_group = chans // GROUPS

    def sum_sends(slot, c):
        return [remote(s_send.at[c], s_recv.at[slot, c, step], ss_sem.at[c, step], sr_sem.at[slot, c, step], peer(step)) for step in range(1, n_dev)]

    def sums_start(slot, c):
        s_send[c, 0:1] = jnp.sum(s_acc[c, 0], axis=0, keepdims=True)
        s_send[c, 1:2] = jnp.sum(s_acc[c, 1], axis=0, keepdims=True)
        s_acc[c] = jnp.zeros_like(s_acc[c])
        for d in sum_sends(slot, c):
            d.start()

    def coefficients(slot, c, layer):
        total = s_send[c]
        for step in range(1, n_dev):
            total = total + s_recv[slot, c, step]
        s_tot[c, 0:2] = total
        t = s_tot[c]
        unit = 1
        while unit < n_group:
            place = (lane // unit) & 3
            g = t
            for d in range(1, 4):
                up = pltpu.roll(t, hc - d * unit, 1)
                down = pltpu.roll(t, (4 - d) * unit, 1)
                g = g + jnp.where(place + d < 4, up, down)
            t = g
            unit *= 4
        t = t * (1.0 / count)
        mean = t[0:1]
        inv = lax.rsqrt(t[1:2] - mean * mean + EPS)
        scale = inv * gamma[pl.ds(layer, 1), lanes[c]]
        return 0.5 * scale, 0.5 * (beta[pl.ds(layer, 1), lanes[c]] - mean * scale)

    def silu(coef, v):
        u = v * coef[0] + coef[1]
        return u + u * jnp.tanh(u)

    def put_shifted(dst, row, p, y, left, right, start):
        n, w = y.shape
        at = lax.broadcasted_iota(jnp.int32, (8, w), 0)
        before = pltpu.roll(y, 1, 0)
        after = pltpu.roll(y, n - 1, 0)
        before = jnp.concatenate([jnp.where(at == 0, left, before[0:8]), before[8:]], axis=0)
        after = jnp.concatenate([after[:n - 8], jnp.where(at == 7, right, after[n - 8:])], axis=0)
        for d, v in enumerate((before, y, after)):
            dst[row, p, :, d * chans + start:d * chans + start + w] = v.astype(BF16)

    def norm(coef, slot, row, p, c):
        v = halo[slot, row, p, :, lanes[c]] if p < 2 else vid[slot, row, p - 2, :, lanes[c]]
        y = silu(coef, v.astype(F32))
        ye = silu(coef, edge[slot, row, p, :, lanes[c]])
        put_shifted(act, row, p, y, jnp.where(h == 0, 0.0, ye), jnp.where(h == 0, ye, 0.0), c * hc)

    def norm_ext(coef, row, p, c):
        mine = silu(coef, (halo[1, row, p, :, lanes[c]] if p < 2 else vid[1, row, p - 2, :, lanes[c]]).astype(F32))
        y = silu(coef, ext[row, p, :, lanes[c]].astype(F32))
        far = silu(coef, edge2[row, p, :, lanes[c]])
        put_shifted(xact, row, p, y, jnp.where(h == 0, mine[half - 1:half], far), jnp.where(h == 0, far, mine[0:1]), c * hc)

    def dots(slot, i, js, lhs, k_half=None, n_half=None):
        cols = slice(0, chans) if n_half is None else lanes[n_half]
        total = None
        for j in js:
            if isinstance(i, int):
                di = 1 if i == j else (2 - 2 * h if i == OWN else 2 * h)
            else:
                di = jnp.where(i == OWN, 1, 2 * h)
            left, right = [], []
            for k in reversed(range(3)):
                for d in range(3):
                    for c in HALVES:
                        if k_half is None or c == k_half:
                            at = slice(d * chans + c * hc, d * chans + (c + 1) * hc)
                            v = lhs(j, k, at)
                            left.append(v.reshape(v.shape[0] * v.shape[1], v.shape[2]))
                            right.append(w_buf[slot, k, di, at, cols])
            q = jnp.dot(jnp.concatenate(left, axis=1), jnp.concatenate(right, axis=0), preferred_element_type=F32)
            total = q if total is None else total + q
        return total

    def frames_of(f0, n):
        return lambda j, k, at: act[j, pl.ds(f0 + k, n), :, at]

    def finish(layer, nslot, i, f0, p, c):
        b = bias[pl.ds(layer, 1), lanes[c]]
        t1 = t2 = None
        for f in range(p.shape[0] // half):
            v = (p[f * half:(f + 1) * half] + b).astype(BF16).astype(F32)
            if isinstance(layer, int):
                vb = v.astype(BF16)
            else:
                res = vid[0, i, f0 + f, :, lanes[c]].astype(F32)
                vb = jnp.where(nslot == 0, res + v, v).astype(BF16)
            vid[nslot, i, f0 + f, :, lanes[c]] = vb
            v = vb.astype(F32)
            t1 = fold(v) if t1 is None else t1 + fold(v)
            t2 = fold(v * v) if t2 is None else t2 + fold(v * v)
            ecol[i, f0 + f, :, lanes[c]] = jnp.where(h == 0, v[half - 1:half], v[0:1])
        s_acc[c, 0] += t1
        s_acc[c, 1] += t2

    def halo_send(slot, row, c):
        return remote(vid.at[slot, row, tail, :, lanes[c]], halo.at[slot, row, :, :, lanes[c]], hs_sem.at[row, c], hr_sem.at[slot, row, c], nxt)

    def edge_send(slot, row, c):
        return remote(ecol.at[row, :, :, lanes[c]], edge.at[slot, 1 - row, pl.ds(2, frames), :, lanes[c]], es_sem.at[row, 0, c],
                      er_sem.at[slot, 1 - row, 0, c], partner)

    def edge_diag(slot, row, c):
        return remote(ecol.at[row, tail, :, lanes[c]], edge.at[slot, 1 - row, pl.ds(0, 2), :, lanes[c]], es_sem.at[row, 1, c],
                      er_sem.at[slot, 1 - row, 1, c], diag)

    def repeat_first(slot, row, cols):
        @pl.when(r == 0)
        def _():
            for f in HALVES:
                halo[slot, row, f, :, cols] = vid[slot, row, 0, :, cols]
                edge[slot, row, f, :, cols] = edge[slot, row, 2, :, cols]

    def half_out(slot, c):
        sums_start(slot, c)
        for row in (OTH, OWN):
            edge_send(slot, row, c).start()

        @pl.when(not_last)
        def _():
            for row in (OTH, OWN):
                edge_diag(slot, row, c).start()
                halo_send(slot, row, c).start()

    def half_in(slot, c, layer):
        for d in sum_sends(slot, c):
            d.wait()
        for row in (OTH, OWN):
            edge_send(slot, row, c).wait()

        @pl.when(not_last)
        def _():
            for row in (OTH, OWN):
                edge_diag(slot, row, c).wait_send()
                halo_send(slot, row, c).wait_send()

        @pl.when(not_first)
        def _():
            for row in (OTH, OWN):
                edge_diag(slot, row, c).wait_recv()
                halo_send(slot, row, c).wait_recv()

        repeat_first(slot, OWN, lanes[c])
        repeat_first(slot, OTH, lanes[c])
        return coefficients(slot, c, layer)

    every = slice(0, chans)
    x_halo = remote(lat.at[tail, 0, my_cols, :], halo.at[0, OWN], hs_sem.at[OWN, 0], hr_sem.at[0, OWN, 0], nxt)
    x_pass = remote(vid.at[0, OTH, tail], halo.at[0, OTH], hs_sem.at[OTH, 0], hr_sem.at[0, OTH, 0], nxt)
    e_part = remote(ecol.at[OWN], edge.at[0, OTH, pl.ds(2, frames)], es_sem.at[OWN, 0, 0], er_sem.at[0, OTH, 0, 0], partner)
    e_nxt = remote(edge.at[0, OWN, pl.ds(frames, 2)], edge.at[0, OWN, pl.ds(0, 2)], es_sem.at[OTH, 1, 0], er_sem.at[0, OWN, 1, 0], nxt)
    e_diag = remote(ecol.at[OWN, tail], edge.at[0, OTH, pl.ds(0, 2)], es_sem.at[OWN, 1, 0], er_sem.at[0, OTH, 1, 0], diag)
    for c in HALVES:
        sums_start(0, c)
    e_part.start()

    @pl.when(not_last)
    def _():
        e_diag.start()
        e_nxt.start()
        x_halo.start()

    for g in (3, 2, 1, 0):
        x_piece(g).start()
    w_copy(1).start()
    load_own.wait()
    for c in small:
        c.wait()
    for c in HALVES:
        for d in sum_sends(0, c):
            d.wait()
    coef = [coefficients(0, c, 0) for c in HALVES]
    for p in range(2, frames + 2):
        for c in HALVES:
            norm(coef[c], 0, OWN, p, c)

    @pl.when(not_last)
    def _():
        x_halo.wait_send()
        e_nxt.wait_send()

    @pl.when(not_first)
    def _():
        x_halo.wait_recv()
        e_nxt.wait_recv()

    repeat_first(0, OWN, every)
    for p in range(2):
        for c in HALVES:
            norm(coef[c], 0, OWN, p, c)
    w_copy(0).wait()

    @pl.loop(0, 4)
    def _(c):
        i = c // 2
        f0 = lax.rem(c, 2) * (frames // 2)
        rows = pl.ds(pl.multiple_of(f0 * half, half), frames // 2 * half)
        acc[i, rows, :] = dots(0, i, (OWN,), frames_of(f0, frames // 2))

    e_part.wait()

    @pl.when(not_last)
    def _():
        e_diag.wait_send()

    @pl.when(not_first)
    def _():
        e_diag.wait_recv()

    def last_k(i, g, c):
        rows = pl.ds(g * per * half, per * half)
        finish(0, 1, i, g * per, acc[i, rows, lanes[c]] + dots(0, i, (OTH,), frames_of(g * per, per), n_half=c), c)

    for g in (3, 2, 1, 0):
        x_piece(g).wait()
        if g == 3:
            x_piece(4).wait()

            @pl.when(not_last)
            def _():
                x_pass.start()
        if g == 0:
            @pl.when(not_last)
            def _():
                x_pass.wait_send()

            @pl.when(not_first)
            def _():
                x_pass.wait_recv()

            repeat_first(0, OTH, every)
        for p in reversed(range(g * per, frames + 2 if g == 3 else (g + 1) * per)):
            for c in HALVES:
                norm(coef[c], 0, OTH, p, c)
        rows = pl.ds(g * per * half, per * half)
        for i in (OTH, OWN):
            if g > 1:
                p = acc[i, rows, :] + dots(0, i, (OTH,), frames_of(g * per, per))
                for c in HALVES:
                    finish(0, 1, i, g * per, p[:, lanes[c]], c)
            else:
                last_k(i, g, 0)
    half_out(1, 0)
    for g in (1, 0):
        for i in (OTH, OWN):
            last_k(i, g, 1)
    half_out(1, 1)

    def strip_send(row, c):
        return remote(vid.at[1, row, :, edge_strip, lanes[c]], ext.at[1 - row, pl.ds(2, frames), :, lanes[c]], ts_sem.at[row, 0, c],
                      tr_sem.at[1 - row, 0, c], partner)

    def strip_pass(row):
        return remote(ext.at[row, pl.ds(frames, 2)], ext.at[row, pl.ds(0, 2)], ts_sem.at[row, 1, 0], tr_sem.at[row, 1, 0], nxt)

    def col2_send(row):
        return remote(ecol2.at[row], edge2.at[1 - row, pl.ds(2, frames)], cs_sem.at[row, 0], cr_sem.at[1 - row, 0], partner)

    def col2_diag(row):
        return remote(ecol2.at[row, tail], edge2.at[1 - row, pl.ds(0, 2)], cs_sem.at[row, 1], cr_sem.at[1 - row, 1], diag)

    def res_send():
        return remote(vid.at[0, OTH, :, edge_strip, :], xres, rs_sem.at[0], rs_sem.at[1], partner)

    def layer_body(layer, carry):
        slot = lax.rem(layer, 2)
        nslot = 1 - slot
        w_copy(layer + 1).start()

        @pl.when(layer == 2)
        def _():
            res_send().start()

        def norms(lo, hi, c):
            for row in (OWN, OTH):
                for p in reversed(range(lo, hi)):
                    norm(coef[c], slot, row, p, c)

        def first_k(i, g):
            acc[i, g * per * half:(g + 1) * per * half, :] = dots(slot, i, (OWN, OTH), frames_of(g * per, per), k_half=0)

        w_copy(layer).wait()
        coef = [half_in(slot, 0, layer)]
        norms(3 * per, frames + 2, 0)
        norms(2 * per, 3 * per, 0)
        first_k(OTH, 3)
        norms(per, 2 * per, 0)
        first_k(OTH, 2)
        norms(0, per, 0)
        first_k(OTH, 1)
        first_k(OTH, 0)
        coef.append(half_in(slot, 1, layer))
        norms(3 * per, frames + 2, 1)
        first_k(OWN, 3)
        norms(2 * per, 3 * per, 1)
        first_k(OWN, 2)
        norms(per, 2 * per, 1)
        first_k(OWN, 1)
        norms(0, per, 1)
        first_k(OWN, 0)
        for c in HALVES:
            for i in (OTH, OWN):
                for g in (3, 2, 1, 0):
                    rows = slice(g * per * half, (g + 1) * per * half)
                    p = dots(slot, i, (OWN, OTH), frames_of(g * per, per), k_half=1, n_half=c)
                    finish(layer, nslot, i, g * per, acc[i, rows, lanes[c]] + p, c)
                if i == OTH and c == 0:
                    @pl.when(layer == 2)
                    def _():
                        strip_send(OTH, 0).start()

            half_out(nslot, c)

            @pl.when(layer == 2)
            def _():
                if c == 1:
                    strip_send(OTH, 1).start()
                strip_send(OWN, c).start()

        return carry

    lax.fori_loop(1, 3, layer_body, 0)

    wide = frames // 4
    pieces_out = (3, 2, 1, 0)

    def out_send(k):
        fs = pl.ds(k * wide, wide)
        dst = out.at[fs, 0, pl.ds(pl.multiple_of(h * (half + strip), strip), part), :]
        return remote(vid.at[0, OTH, fs, part_cols, :], dst, os_sem.at[k], or_sem.at[k], partner)

    def out_local():
        return pltpu.make_async_copy(vid.at[0, OWN], out.at[:, 0, my_cols, :], o_sem.at[0])

    def out_ext():
        dst = out.at[:, 0, pl.ds(pl.multiple_of(half - h * strip, strip), strip), :]
        return pltpu.make_async_copy(xres, dst, o_sem.at[1])

    def norms(lo, hi, c):
        for row in (OWN, OTH):
            for p in reversed(range(lo, hi)):
                norm(coef[c], 1, row, p, c)

    def close(res, p):
        return (res.astype(F32) + (p + bias[3:4, :]).astype(BF16).astype(F32)).astype(BF16)

    def part_dots(k, k_half):
        return dots(1, OTH, (OWN, OTH), lambda j, t, at: act[j, pl.ds(k * wide + t, wide), part_cols, at], k_half)

    def part_chunk(k):
        rows = slice(k * wide * part, (k + 1) * wide * part)
        p = acc[OTH, rows, :] + part_dots(k, 1)
        for f in range(wide):
            fr = k * wide + f
            vid[0, OTH, fr, part_cols, :] = close(vid[0, OTH, fr, part_cols, :], p[f * part:(f + 1) * part])
        out_send(k).start()

    def own_chunk(g):
        p = dots(1, OWN, (OWN, OTH), frames_of(g * per, per))
        for f in range(per):
            vid[0, OWN, g * per + f] = close(vid[0, OWN, g * per + f], p[f * half:(f + 1) * half])

    w_copy(3).wait()
    coef = [half_in(1, 0, 3)]
    def norms_for(k, c):
        norms(k * wide, frames + 2 if k == 3 else (k + 1) * wide, c)

    norms_for(3, 0)
    norms_for(2, 0)
    for k in pieces_out:
        acc[OTH, k * wide * part:(k + 1) * wide * part, :] = part_dots(k, 0)
        if k > 1:
            norms_for(k - 2, 0)
    def columns2(f, carry):
        for row in (OWN, OTH):
            v = vid[1, row, f, strip:half - strip, :].astype(F32)
            ecol2[row, f] = jnp.where(h == 0, v[half - 2 * strip - 1:half - 2 * strip], v[0:1])
        return carry

    lax.fori_loop(0, frames, columns2, 0)
    for row in (OWN, OTH):
        col2_send(row).start()

    @pl.when(not_last)
    def _():
        for row in (OWN, OTH):
            col2_diag(row).start()

    coef.append(half_in(1, 1, 3))
    norms_for(3, 1)
    for k in pieces_out:
        if k > 0:
            norms_for(k - 1, 1)
        part_chunk(k)
    for row in (OWN, OTH):
        col2_send(row).wait()
        for c in HALVES:
            strip_send(row, c).wait()

    @pl.when(not_last)
    def _():
        for row in (OWN, OTH):
            col2_diag(row).wait_send()
            strip_pass(row).start()

    @pl.when(not_first)
    def _():
        for row in (OWN, OTH):
            col2_diag(row).wait_recv()

    @pl.when(r == 0)
    def _():
        for row in (OWN, OTH):
            for f in HALVES:
                ext[row, f] = ext[row, 2]
                edge2[row, f] = edge2[row, 2]

    res_send().wait()
    for row in (OWN, OTH):
        for p in range(2, frames + 2):
            for c in HALVES:
                norm_ext(coef[c], row, p, c)
    for g in (3, 2, 1, 0):
        own_chunk(g)
    out_local().start()

    @pl.when(not_last)
    def _():
        for row in (OWN, OTH):
            strip_pass(row).wait_send()

    @pl.when(not_first)
    def _():
        for row in (OWN, OTH):
            strip_pass(row).wait_recv()

    for row in (OWN, OTH):
        for p in HALVES:
            for c in HALVES:
                norm_ext(coef[c], row, p, c)
    p = dots(1, OWN, (OWN, OTH), lambda j, t, at: xact[j, pl.ds(t, frames), :, at])
    for f in range(frames):
        xres[f] = close(xres[f], p[f * strip:(f + 1) * strip])
    out_ext().start()
    out_local().wait()
    out_ext().wait()
    for k in pieces_out:
        out_send(k).wait()


def solution(mesh):
    n_cp = mesh.shape["cp"]

    def local_decode(lat, conv_w, conv_b, gn_gamma, gn_beta):
        frames, _, width, chans = lat.shape
        half = width // 2
        strip = half // 4
        n_dev = 2 * n_cp
        count = frames * n_cp * 2 * width * (chans // GROUPS)
        dma = pltpu.SemaphoreType.DMA

        def pair(*more):
            return dma((2, *more))

        any_spec = pl.BlockSpec(memory_space=pl.ANY)
        return pl.pallas_call(
            functools.partial(kernel, (n_cp, frames, half, strip, chans, count)),
            out_shape=jax.ShapeDtypeStruct(lat.shape, BF16),
            in_specs=[any_spec] * 5,
            out_specs=any_spec,
            scratch_shapes=[
                pltpu.VMEM(conv_b.shape, F32),
                pltpu.VMEM(gn_gamma.shape, F32),
                pltpu.VMEM(gn_beta.shape, F32),
                pltpu.VMEM((2, 2, frames, half, chans), BF16),
                pltpu.VMEM((2, frames + 2, half, 3 * chans), BF16),
                pltpu.VMEM((2, frames * half, chans), F32),
                pltpu.VMEM((2, 3, 3, 3 * chans, chans), BF16),
                pltpu.VMEM(lat.shape, BF16),
                pltpu.VMEM((2, 2, 2, half, chans), BF16),
                pltpu.VMEM((2, 2, frames + 2, 1, chans), F32),
                pltpu.VMEM((2, frames, 1, chans), F32),
                pltpu.VMEM((2, frames + 2, strip, chans), BF16),
                pltpu.VMEM((2, frames + 2, strip, 3 * chans), BF16),
                pltpu.VMEM((2, frames + 2, 1, chans), F32),
                pltpu.VMEM((2, frames, 1, chans), F32),
                pltpu.VMEM((frames, strip, chans), BF16),
                pltpu.VMEM((2, 2, 8, chans // 2), F32),
                pltpu.VMEM((2, 8, chans // 2), F32),
                pltpu.VMEM((2, 2, chans // 2), F32),
                pltpu.VMEM((2, 2, n_dev, 2, chans // 2), F32),
                dma((8,)),
                pair(),
                dma((5,)),
                dma((5,)),
                pair(2),
                pair(2, 2),
                pair(2, 2),
                pair(2, 2, 2),
                pair(2, 2),
                pair(2, 2),
                pair(2),
                pair(2),
                pair(),
                pair(n_dev),
                pair(2, n_dev),
                pair(),
                dma((4,)),
                dma((4,)),
            ],
            compiler_params=pltpu.CompilerParams(collective_id=0, has_side_effects=True, vmem_limit_bytes=52 * 1024 * 1024),
            name="decode",
        )(*(pltpu.with_memory_space_constraint(a, pltpu.HBM) for a in (lat, conv_w.reshape(4, 3, 3, 3 * chans, chans), conv_b, gn_gamma, gn_beta)))

    spec = P(("dp", "cp"), "hp", None, None)
    return jax.shard_map(local_decode, mesh=mesh, in_specs=(spec, P(), P(), P(), P()), out_specs=spec, check_vma=False)
```
